512 devices in a mesh: dp: 8 (over z_lo), lat: 16 (over y, z_hi, core), lon: 4 (over x).
Axes of the slice: x: 4, y: 4, z: 16 (z_hi: 2, z_lo: 8; z = z_hi * 8 + z_lo), core: 2. Of those that a mesh axis runs over, the one named last changes fastest.
Arguments:
- hidden_in: bfloat16 [8, 256, 512, 128], P('dp', 'lat', 'lon'), may hold values from -6 to 6
- conv_weight: bfloat16 [3, 3, 128, 128], replicated, may hold values from -0.1875 to 0.1875
- conv_bias: float32 [128], replicated, may hold values from -3 to 3
- proj_weight: float32 [128], replicated, may hold values from -5 to 5
- ocean_depth: float32 [256, 512], P('lat', 'lon'), may hold values from 0.5 to 2
- sea_mask: int32 [256, 512], P('lat', 'lon'), may hold values 0 or 1
- step_alpha: float32 [6], replicated, may hold values from 0.04 to 0.07
- step_beta: float32 [6], replicated, may hold values from 0.1 to 0.5
- surface_cotangent: float32 [8, 256, 512], P('dp', 'lat', 'lon'), may hold values from -20 to 20
Outputs:
- grad_hidden: bfloat16 [8, 256, 512, 128], P('dp', 'lat', 'lon')
- grad_weight: float32 [128, 3, 3, 128], P(('lat', 'lon'))
- grad_bias: float32 [128], replicated
- grad_proj: float32 [128], replicated
The draws below stay inside these ranges and needn't reach their ends.
All inputs are finite; a program needn't handle non-finite values. No bound on the sum of `sea_mask` on one device may be relied on, other than what follows from the above.
Results may differ from the reference program's by a relative error of at most 0.01.
Values may be sent and summed in bfloat16 or wider, within the bound.
No kernel may reach another device: no remote copies, remote signals or barrier semaphores. Data moves between devices by JAX's collectives and lax.ppermute only.
A program may use at most 64 MiB of HBM per device.

```python
import math
import jax
import jax.numpy as jnp
from jax import lax

C = 128
ITERS = 6
BATCH = 8
NLAT = 256
NLON = 512


def draw_surface_cotangent(key, part):
    key_noise, key_offset, key_sign = jax.random.split(jax.random.fold_in(key, 17), 3)
    lat_ramp = 1.0 + 2.0 * jnp.arange(NLAT, dtype=jnp.float32) / max(NLAT - 1, 1)
    offset = jax.random.uniform(key_offset, (BATCH, 1, 1), jnp.float32, 0.8, 1.5)
    sample_sign = jnp.where(jax.random.bernoulli(key_sign, 0.5, (BATCH, 1, 1)), 1.0, -1.0)
    slope_part = sample_sign * offset * lat_ramp[None, :, None]
    noise_part = jnp.clip(jax.random.normal(key_noise, (BATCH, NLAT, NLON), jnp.float32), -4.0, 4.0)
    values = noise_part + slope_part
    return values


def with_ends(values, own_key, low, top_value):
    shape = values.shape
    spot = [jax.random.randint(jax.random.fold_in(own_key, axis), (), 0, shape[axis]) for axis in range(len(shape))]
    values = values.at[tuple(spot)].set(low)
    longest = shape.index(max(shape))
    spot[longest] = (spot[longest] + 1) % shape[longest]
    return values.at[tuple(spot)].set(top_value)


def block_levels(stream_key, dims, pieces, low, top_value):
    loudness, own = 1.0, jax.random.fold_in(stream_key, 6)
    for axis_at, blocks in pieces:
        steps = jnp.exp(jax.random.uniform(jax.random.fold_in(own, axis_at), (blocks,), jnp.float32, low / len(pieces), top_value / len(pieces)))
        loudness = loudness * jnp.repeat(steps, dims[axis_at] // blocks).reshape([-1 if axis == axis_at else 1 for axis in range(len(dims))])
    return loudness


def gaussian(stream_key, extent, deviation, limit, cuts=(), held_as=jnp.bfloat16):
    entries = jax.random.normal(stream_key, extent, jnp.float32) * deviation
    if len(cuts) > 0:
        entries = block_levels(stream_key, extent, cuts, -0.22, 0.18) * entries
    return jnp.clip(entries, min=-limit, max=limit).astype(held_as)


def setup_inputs(seed: int = 0) -> dict:
    splits = jax.random.split(jax.random.key(seed), 10)
    hidden_in = gaussian(splits[0], (BATCH, NLAT, NLON, C), 1.0, 6.0, ((0, 8), (1, 16), (2, 4)))
    conv_weight = gaussian(splits[1], (3, 3, C, C), (9 * C) ** -0.5, 0.1875)
    conv_bias = gaussian(splits[2], (C,), 0.5, 3.0, (), jnp.float32)
    proj_weight = gaussian(splits[3], (C,), 1.0, 5.0, (), jnp.float32)
    ocean_depth = jnp.clip(jnp.exp(math.log(2.0) - 1.3862944 * jax.random.uniform(splits[4], (NLAT, NLON), jnp.float32) ** block_levels(splits[4], (NLAT, NLON), ((0, 16), (1, 4)), -0.2, 0.2)), 0.5, 2.0)
    sea_mask = with_ends((jax.random.randint(splits[5], (NLAT, NLON), 0, 5) < 4).astype(jnp.int32), jax.random.fold_in(splits[5], 1), 0, 1)
    step_alpha = jnp.clip(jnp.exp(jax.random.uniform(splits[6], (ITERS,), jnp.float32, math.log(0.04), math.log(0.07))), 0.04, 0.07)
    step_beta = jnp.clip(jax.random.uniform(splits[7], (ITERS,), jnp.float32, 0.1, 0.5), 0.1, 0.5)
    surface_cotangent = draw_surface_cotangent(jax.random.fold_in(splits[9], 71), 0)
    return {"hidden_in": hidden_in, "conv_weight": conv_weight, "conv_bias": conv_bias, "proj_weight": proj_weight, "ocean_depth": ocean_depth, "sea_mask": sea_mask, "step_alpha": step_alpha, "step_beta": step_beta, "surface_cotangent": surface_cotangent}


helm_coef = 0.5

def extend(values, lat_axis):
    lon_axis = lat_axis + 1
    length = values.shape[lon_axis]
    left_col = lax.slice_in_dim(values, length - 1, length, axis=lon_axis)
    right_col = lax.slice_in_dim(values, 0, 1, axis=lon_axis)
    wrapped = jnp.concatenate([left_col, values, right_col], axis=lon_axis)
    widths = [(0, 0)] * wrapped.ndim
    widths[lat_axis] = (1, 1)
    return jnp.pad(wrapped, widths)

def operate(field_ext, mask_ext, depth_ext):
    rows_in = field_ext.shape[-2] - 2
    cols_in = field_ext.shape[-1] - 2
    center = field_ext[..., 1:-1, 1:-1]
    mask_mid = mask_ext[1:-1, 1:-1]
    depth_mid = depth_ext[1:-1, 1:-1]
    result = helm_coef * center
    for row_off, col_off in ((0, 1), (2, 1), (1, 0), (1, 2)):
        beside = field_ext[..., row_off:row_off + rows_in, col_off:col_off + cols_in]
        mask_near = mask_ext[row_off:row_off + rows_in, col_off:col_off + cols_in]
        depth_near = depth_ext[row_off:row_off + rows_in, col_off:col_off + cols_in]
        weight = mask_near * 0.5 * (depth_mid + depth_near)
        result = result + weight * (center - beside)
    return mask_mid * result

def solve_steps(adjoint_start, mask_ext, depth_ext, step_alpha, step_beta):
    solution = jnp.zeros_like(adjoint_start)
    residual = adjoint_start
    direction = adjoint_start
    for turn_index in range(ITERS):
        solution = solution + step_alpha[turn_index] * direction
        if turn_index + 1 < ITERS:
            applied = operate(extend(direction, 1), mask_ext, depth_ext)
            residual = residual - step_alpha[turn_index] * applied
            direction = residual + step_beta[turn_index] * direction
    return solution

def reference(hidden_in, conv_weight, conv_bias, proj_weight, ocean_depth, sea_mask, step_alpha, step_beta, surface_cotangent):
    mask_float = sea_mask.astype(jnp.float32)
    ocean_count = jnp.sum(mask_float)
    sample_mean = lax.optimization_barrier(jnp.sum(mask_float * surface_cotangent, axis=(1, 2))) / ocean_count
    adjoint_start = mask_float * (surface_cotangent - sample_mean[:, None, None])
    forcing_grad = mask_float * solve_steps(adjoint_start, extend(mask_float, 0), extend(ocean_depth, 0), step_alpha, step_beta)
    grad_scale = 1.0 / math.sqrt(BATCH * NLAT * NLON)
    grad_weight = jnp.zeros((C, 3, 3, C), jnp.float32)
    grad_bias = jnp.zeros((C,), jnp.float32)
    grad_proj = jnp.zeros((C,), jnp.float32)
    outputs = []
    for sample in range(BATCH):
        padded = extend(hidden_in[sample], 0)
        shifted = [padded[row_off:row_off + NLAT, col_off:col_off + NLON, :].reshape(NLAT * NLON, C) for row_off in range(3) for col_off in range(3)]
        preact = conv_bias
        for offset in range(9):
            preact = preact + jnp.dot(shifted[offset], conv_weight[offset // 3, offset % 3], preferred_element_type=jnp.float32)
        sigma = jax.nn.sigmoid(preact)
        active = preact * sigma
        slope_act = sigma * (1.0 + preact * (1.0 - sigma))
        force_col = forcing_grad[sample].reshape(NLAT * NLON)[:, None]
        grad_pre = (force_col * proj_weight * slope_act).astype(jnp.bfloat16)
        grad_proj = grad_proj + lax.optimization_barrier(jnp.sum(active * force_col, axis=0))
        grad_bias = grad_bias + lax.optimization_barrier(jnp.sum(grad_pre.astype(jnp.float32), axis=0))
        blocks = [jnp.dot(shifted[offset].T, grad_pre, preferred_element_type=jnp.float32) for offset in range(9)]
        grad_weight = grad_weight + jnp.stack(blocks, axis=1).reshape(C, 3, 3, C)
        grad_ext = extend(grad_pre.reshape(NLAT, NLON, C), 0)
        backed = jnp.zeros((NLAT * NLON, C), jnp.float32)
        for row_off in range(3):
            for col_off in range(3):
                window = grad_ext[2 - row_off:2 - row_off + NLAT, 2 - col_off:2 - col_off + NLON, :].reshape(NLAT * NLON, C)
                backed = backed + jnp.dot(window, conv_weight[row_off, col_off].T, preferred_element_type=jnp.float32)
        outputs.append(backed.reshape(NLAT, NLON, C).astype(jnp.bfloat16))
    return (jnp.stack(outputs), grad_weight * grad_scale, grad_bias * grad_scale, grad_proj * grad_scale)
```

```python
import functools
import math

import jax
import jax.numpy as jnp
from jax import lax
from jax.sharding import Mesh
from jax.sharding import PartitionSpec as P

ITERS = 6
LAT_LON = ("lat_0", "lat_1", "lat_2", "lon")
LAT = ("lat_0", "lat_1", "lat_2")
DP_LAT_LON = ("dp", "lat_0", "lat_1", "lat_2", "lon")


helm_coef = 0.5


def from_everyone(shard, axis):
    peers = lax.axis_size(axis)
    return lax.all_to_all(
        jnp.broadcast_to(shard[None], (peers, *shard.shape)), axis, 0, 0, tiled=True
    )


def over_copies(shard, axis):
    everything = from_everyone(shard, axis)
    return jnp.sum(everything, axis=0)


def packed_total(arrays, axis):
    ends = [0]
    for a in arrays:
        ends.append(ends[-1] + a.size)
    so_far = over_copies(jnp.concatenate([a.ravel() for a in arrays]), axis)
    return tuple((so_far[b:e].reshape(a.shape) for a, b, e in zip(arrays, ends, ends[1:])))


def extended(cells, sides, width, closed):
    for axis, dim in sides:
        count = lax.axis_size(axis)
        ends = count if closed else count - 1
        head = lax.slice_in_dim(cells, 0, width, axis=dim)
        tail = lax.slice_in_dim(cells, cells.shape[dim] - width, cells.shape[dim], axis=dim)
        cells = jnp.concatenate(
            [
                lax.ppermute(tail, axis, [(i, (i + 1) % count) for i in range(ends)]),
                cells,
                lax.ppermute(head, axis, [((i + 1) % count, i) for i in range(ends)]),
            ],
            axis=dim,
        )
    return cells


def in_blocks(shard, dim, peers):
    shape = shard.shape
    blocks = shard.reshape(*shape[:dim], peers, shape[dim] // peers, *shape[dim + 1 :])
    return jnp.moveaxis(blocks, dim, 0)


def sent_and_summed(shard, axis, dim):
    blocks = in_blocks(shard, dim, lax.axis_size(axis))
    arrived = lax.all_to_all(blocks, axis, split_axis=0, concat_axis=0, tiled=True)
    return arrived.astype(jnp.float32).sum(axis=0)


def one_axis_at_a_time(shard, axes):
    return functools.reduce(lax.psum, axes, shard)


def two_pieces(values):
    high = lax.reduce_precision(values, 8, 7)
    return jnp.concatenate([high, values - high]).astype(jnp.bfloat16)


def from_pieces(pieces):
    both = pieces.astype(jnp.float32)
    count = both.shape[-2] // 2
    return both[..., :count, :] + both[..., count:, :]


def all_summed(weight, bias, proj):
    channels = weight.shape[0]
    n_y, n_z, n_c = (lax.axis_size(name) for name in LAT)
    n_x = lax.axis_size("lon")
    share = channels // (n_y * n_z * n_c * n_x)
    rows = share * 9
    parts = weight.reshape(n_y, n_z, n_c, n_x, rows, channels)
    vectors = jnp.stack([bias, proj])
    core = lax.axis_index("lat_2")
    own = jnp.where(core == 0, parts[:, :, 0], parts[:, :, 1])
    other = jnp.where(core == 0, parts[:, :, 1], parts[:, :, 0])
    sent = jnp.concatenate(
        [other.astype(jnp.bfloat16).reshape(-1, channels), two_pieces(vectors)], axis=0
    )
    got = lax.ppermute(sent, "lat_2", [(0, 1), (1, 0)])
    own = own + got[:-4].astype(jnp.float32).reshape(own.shape)
    vectors = vectors + from_pieces(got[-4:])
    by_peer = own.transpose(0, 2, 1, 3, 4).reshape(n_y * n_x, n_z * rows, channels)
    extra = jnp.broadcast_to(two_pieces(vectors)[None], (n_y * n_x, 4, channels))
    sent = jnp.concatenate([by_peer.astype(jnp.bfloat16), extra], axis=1)
    got = lax.all_to_all(sent, ("lat_0", "lon"), 0, 0, tiled=True)
    own = got[:, :-4].astype(jnp.float32).sum(axis=0).reshape(n_z, rows, channels)
    vectors = from_pieces(got[:, -4:]).sum(axis=0)
    n_d = lax.axis_size("dp")
    sent = jnp.concatenate([own, jnp.broadcast_to(vectors[None], (n_z, 2, channels))], axis=1)
    sent = jnp.broadcast_to(sent[:, None], (n_z, n_d, rows + 2, channels))
    sent = sent.reshape(n_z * n_d, rows + 2, channels)
    total = lax.all_to_all(sent, ("lat_1", "dp"), 0, 0, tiled=True).sum(axis=0)
    return total[:rows].reshape(share, 3, 3, channels), total[rows], total[rows + 1]


def operate(field_ext, mask_ext, depth_ext):
    rows_in = field_ext.shape[-2] - 2
    cols_in = field_ext.shape[-1] - 2
    center = field_ext[..., 1:-1, 1:-1]
    mask_mid = mask_ext[1:-1, 1:-1]
    depth_mid = depth_ext[1:-1, 1:-1]
    result = helm_coef * center
    for row_off, col_off in ((0, 1), (2, 1), (1, 0), (1, 2)):
        beside = field_ext[..., row_off : row_off + rows_in, col_off : col_off + cols_in]
        mask_near = mask_ext[row_off : row_off + rows_in, col_off : col_off + cols_in]
        depth_near = depth_ext[row_off : row_off + rows_in, col_off : col_off + cols_in]
        weight = mask_near * 0.5 * (depth_mid + depth_near)
        result = result + weight * (center - beside)
    return mask_mid * result


def solve_steps(adjoint_start, mask_ext, depth_ext, step_alpha, step_beta, widen):
    solution = jnp.zeros_like(adjoint_start)
    residual = adjoint_start
    direction = adjoint_start
    for turn_index in range(ITERS):
        solution = solution + step_alpha[turn_index] * direction
        if turn_index + 1 < ITERS:
            applied = operate(widen(direction), mask_ext, depth_ext)
            residual = residual - step_alpha[turn_index] * applied
            direction = residual + step_beta[turn_index] * direction
    return solution


def pad_zero(field):
    return jnp.pad(field, ((0, 0), (1, 1), (1, 1)))


def shards(
    hidden_in,
    conv_weight,
    conv_bias,
    proj_weight,
    ocean_depth,
    sea_mask,
    step_alpha,
    step_beta,
    surface_cotangent,
):
    samples, lat_rows, lon_cols, channels = hidden_in.shape
    mask_float = sea_mask.astype(jnp.float32)
    counted, summed = packed_total(
        (jnp.sum(mask_float), jnp.sum(mask_float * surface_cotangent, axis=(1, 2))), LAT_LON
    )
    adjoint_start = mask_float * (surface_cotangent - (summed / counted)[:, None, None])
    reach = ITERS - 1
    stacked = jnp.concatenate([adjoint_start, mask_float[None], ocean_depth[None]], axis=0)
    stacked = extended(stacked, ((LAT, 1),), reach, False)
    stacked = extended(stacked, (("lon", 2),), reach, True)
    mask_wide = jnp.pad(stacked[samples], 1)
    depth_wide = jnp.pad(stacked[samples + 1], 1)
    solution = solve_steps(
        stacked[:samples], mask_wide, depth_wide, step_alpha, step_beta, pad_zero
    )
    solution = solution[:, reach : reach + lat_rows, reach : reach + lon_cols]
    forcing_grad = mask_float * solution
    padded = extended(hidden_in, ((LAT, 1),), 1, False)
    padded = extended(padded, (("lon", 2),), 1, True)
    cell_count = samples * lat_rows * lon_cols
    shifted = [
        padded[:, row_off : row_off + lat_rows, col_off : col_off + lon_cols, :].reshape(
            cell_count, channels
        )
        for row_off in range(3)
        for col_off in range(3)
    ]
    preact = conv_bias
    for offset in range(9):
        preact = preact + jnp.dot(
            shifted[offset],
            conv_weight[offset // 3, offset % 3],
            preferred_element_type=jnp.float32,
        )
    sigma = jax.nn.sigmoid(preact)
    active = preact * sigma
    slope_act = sigma * (1.0 + preact * (1.0 - sigma))
    force_col = forcing_grad.reshape(cell_count)[:, None]
    grad_pre = (force_col * proj_weight * slope_act).astype(jnp.bfloat16)
    local_proj = jnp.sum(active * force_col, axis=0)
    local_bias = jnp.sum(grad_pre.astype(jnp.float32), axis=0)
    grad_ext = extended(
        grad_pre.reshape(samples, lat_rows, lon_cols, channels), ((LAT, 1),), 1, False
    )
    grad_ext = extended(grad_ext, (("lon", 2),), 1, True)
    backed = jnp.zeros((cell_count, channels), jnp.float32)
    for row_off in range(3):
        for col_off in range(3):
            window = grad_ext[
                :, 2 - row_off : 2 - row_off + lat_rows, 2 - col_off : 2 - col_off + lon_cols, :
            ].reshape(cell_count, channels)
            backed = backed + lax.dot_general(
                window,
                conv_weight[row_off, col_off],
                (((1,), (1,)), ((), ())),
                preferred_element_type=jnp.float32,
            )
    grad_hidden = backed.reshape(samples, lat_rows, lon_cols, channels).astype(jnp.bfloat16)
    blocks = []
    for shifted_cols in shifted:
        blocks.append(
            lax.dot_general(
                shifted_cols, grad_pre, (((0,), (0,)), ((), ())), preferred_element_type=jnp.float32
            )
        )
    own_weight, total_bias, total_proj = all_summed(
        jnp.stack(blocks, axis=1), local_bias, local_proj
    )
    all_cells = cell_count * lax.axis_size("dp") * lax.axis_size(LAT) * lax.axis_size("lon")
    grad_scale = 1.0 / math.sqrt(all_cells)
    return (grad_hidden, own_weight * grad_scale, total_bias * grad_scale, total_proj * grad_scale)


def solution(mesh):
    split = Mesh(
        mesh.devices.reshape(mesh.shape["dp"], 4, 2, 2, mesh.shape["lon"]),
        ("dp", "lat_0", "lat_1", "lat_2", "lon"),
    )
    placed = (
        P("dp", LAT, "lon", None),
        P(),
        P(),
        P(),
        P(LAT, "lon"),
        P(LAT, "lon"),
        P(),
        P(),
        P("dp", LAT, "lon"),
    )
    return jax.shard_map(
        shards,
        mesh=split,
        in_specs=placed,
        out_specs=(P("dp", LAT, "lon", None), P(LAT_LON, None, None, None), P(), P()),
        check_vma=False,
    )
```

```python
import functools
import math

import jax
import jax.numpy as jnp
from jax import lax
from jax.experimental import pallas as pl
from jax.experimental.pallas import tpu as pltpu
from jax.sharding import Mesh
from jax.sharding import PartitionSpec as P

ITERS = 6
REACH = 6
LAT_LON = ("lat_0", "lat_1", "lat_2", "lon")
LAT = ("lat_0", "lat_1", "lat_2")
WIDE = 144
PACK = 32

helm_coef = 0.5
VMEM = pl.BlockSpec(memory_space=pltpu.VMEM)
SMEM = pl.BlockSpec(memory_space=pltpu.SMEM)


def pieces_of(values, count):
    out = []
    for _ in range(count):
        piece = lax.reduce_precision(values, 8, 7)
        out.append(piece.astype(jnp.bfloat16))
        values = values - piece
    return out


def forward_kernel(
    hidden_ref, edge_ref, ends_ref, fields_ref, weight_ref, bias_ref, alpha_ref, beta_ref,
    ext_ref, preact_ref, force_ref, rhs_ref,
):
    rows = hidden_ref.shape[0]
    ext_ref[0:2] = ends_ref[0:2]
    ext_ref[2 : rows + 2, 0:128] = hidden_ref[...]
    ext_ref[2 : rows + 2, 128:WIDE] = edge_ref[...]
    ext_ref[rows + 2 : rows + 4] = ends_ref[2:4]
    for a in range(3):
        for c in range(3):
            rhs_ref[a * 128 : a * 128 + 128, c * 128 : c * 128 + 128] = weight_ref[a, c]

    total = [
        fields_ref[0, k].astype(jnp.float32)
        + fields_ref[1, k].astype(jnp.float32)
        + fields_ref[2, k].astype(jnp.float32)
        for k in range(2)
    ]
    start, wet_depth = total
    mask = jnp.where(wet_depth > 0.0, 1.0, 0.0)
    lane = lax.broadcasted_iota(jnp.int32, (2 * PACK, 128), 1)

    def other_half(field):
        parts = [field[k * PACK : (k + 1) * PACK] for k in range(field.shape[0] // PACK)]
        swapped = []
        for k in range(0, len(parts), 2):
            swapped += [parts[k + 1], parts[k]]
        return jnp.concatenate(swapped, axis=0)

    def beside(field):
        count = field.shape[0]
        lanes = lane if count == 2 * PACK else jnp.concatenate([lane, lane], axis=0)
        up = pltpu.roll(field, 1, 0)
        down = pltpu.roll(field, count - 1, 0)
        from_left = pltpu.roll(field, 1, 1)
        from_left = jnp.where(lanes == 0, other_half(from_left), from_left)
        from_right = pltpu.roll(field, 127, 1)
        from_right = jnp.where(lanes == 127, other_half(from_right), from_right)
        return up, down, from_left, from_right

    weights = [
        0.5 * (near_mask * wet_depth + mask * near_depth)
        for near_mask, near_depth in zip(beside(mask), beside(wet_depth))
    ]
    diagonal = helm_coef * mask + weights[0] + weights[1] + weights[2] + weights[3]
    weights = [jnp.concatenate([w, w], axis=0) for w in weights]
    diagonal = jnp.concatenate([diagonal, diagonal], axis=0)
    residual = jnp.concatenate([start, mask], axis=0)
    direction = residual
    result = jnp.zeros_like(residual)
    for k in range(ITERS):
        result = result + alpha_ref[k] * direction
        if k + 1 < ITERS:
            applied = diagonal * direction
            for w, near in zip(weights, beside(direction)):
                applied = applied - w * near
            residual = residual - alpha_ref[k] * applied
            direction = residual + beta_ref[k] * direction
    result = result * jnp.concatenate([mask, mask], axis=0)
    force_ref[...] = result.T

    group = 6
    bias = bias_ref[...]
    for g in range(0, rows + 2, group):
        lhs = jnp.concatenate(
            [ext_ref[g + a : g + a + group].reshape(group * WIDE, 128) for a in range(3)], axis=1
        )
        out = jnp.dot(lhs, rhs_ref[...], preferred_element_type=jnp.float32)
        for j in range(group):
            part = out[j * WIDE : (j + 1) * WIDE]
            preact_ref[g + j] = (
                pltpu.roll(part[:, 0:128], 1, 0)
                + part[:, 128:256]
                + pltpu.roll(part[:, 256:384], WIDE - 1, 0)
                + bias
            )


def backward_kernel(
    mean_ref, preact_ref, force_ref, ext_ref, proj_ref,
    grad_ref, weight_ref, vectors_ref, moved_ref,
):
    rows = grad_ref.shape[0] - 2
    force = force_ref[...]
    force = force - mean_ref[0] * pltpu.roll(force, 64, 1)
    proj = proj_ref[...]
    sum_bias = jnp.zeros((8, 128), jnp.float32)
    sum_proj = jnp.zeros((8, 128), jnp.float32)
    for g in range(rows + 2):
        at = g + REACH - 1
        column = jnp.concatenate(
            [
                force[:, at : at + 1],
                force[0:8, PACK + at : PACK + at + 1],
                force[120:128, PACK + at : PACK + at + 1],
            ],
            axis=0,
        )
        column = jnp.broadcast_to(column, (WIDE, 128))
        preact = preact_ref[g]
        sigma = jax.nn.sigmoid(preact)
        active = preact * sigma
        slope_act = sigma * (1.0 + preact * (1.0 - sigma))
        grad = (column * proj * slope_act).astype(jnp.bfloat16)
        grad_ref[g] = grad
        if 1 <= g <= rows:
            own = grad.astype(jnp.float32)[0:128]
            for k in range(16):
                sum_bias = sum_bias + own[k * 8 : k * 8 + 8]
                sum_proj = sum_proj + (active * column)[k * 8 : k * 8 + 8]
            own = jnp.concatenate([own, jnp.zeros((WIDE - 128, 128), jnp.float32)], axis=0)
            moved_ref[g - 1, :, 0:128] = pltpu.roll(own, WIDE - 1, 0).astype(jnp.bfloat16)
            moved_ref[g - 1, :, 128:256] = own.astype(jnp.bfloat16)
            moved_ref[g - 1, :, 256:384] = pltpu.roll(own, 1, 0).astype(jnp.bfloat16)
    vectors_ref[0:1] = jnp.sum(sum_bias, axis=0, keepdims=True)
    vectors_ref[1:2] = jnp.sum(sum_proj, axis=0, keepdims=True)
    moved = moved_ref[...].reshape(rows * WIDE, 384)
    for a in range(3):
        cells = ext_ref[a + 1 : a + 1 + rows].reshape(rows * WIDE, 128)
        out = lax.dot_general(
            cells, moved, (((0,), (0,)), ((), ())), preferred_element_type=jnp.float32
        )
        for c in range(3):
            weight_ref[a * 3 + c] = out[:, c * 128 : c * 128 + 128]


def input_kernel(grad_ref, weight_ref, out_ref, rhs_ref):
    rows = out_ref.shape[0]
    for a in range(3):
        for c in range(3):
            rhs_ref[c * 128 : c * 128 + 128, a * 128 : a * 128 + 128] = weight_ref[a, c]
    group = 4
    for y in range(0, rows, group):
        lhs = jnp.concatenate(
            [
                grad_ref[y - a + 2 : y - a + 2 + group].reshape(group * WIDE, 128)
                for a in range(3)
            ],
            axis=1,
        )
        out = lax.dot_general(
            lhs, rhs_ref[...], (((1,), (1,)), ((), ())), preferred_element_type=jnp.float32
        )
        for j in range(group):
            part = out[j * WIDE : (j + 1) * WIDE]
            total = (
                pltpu.roll(part[:, 0:128], WIDE - 1, 0)
                + part[:, 128:256]
                + pltpu.roll(part[:, 256:384], 1, 0)
            )
            out_ref[y + j] = total[0:128].astype(jnp.bfloat16)


def call(kernel, shapes, scratch, in_specs, args, name):
    return pl.pallas_call(
        kernel,
        out_shape=shapes,
        in_specs=in_specs,
        out_specs=jax.tree.map(lambda _: VMEM, shapes),
        scratch_shapes=scratch,
        compiler_params=pltpu.CompilerParams(vmem_limit_bytes=40 * 1024 * 1024),
        name=name,
    )(*args)


def gathered_edges(hidden, fields):
    count = lax.axis_size("lon")
    me = lax.axis_index("lon")
    rows = hidden.shape[0]
    head = hidden[:, 0:2].reshape(1, 2 * rows, 128)
    tail = hidden[:, 126:128].reshape(1, 2 * rows, 128)
    peer = lax.broadcasted_iota(jnp.int32, (count, 1, 1), 0)
    columns = jnp.where(peer == (me + 1) % count, tail, head)
    flat = jnp.broadcast_to(fields.reshape(1, -1, 128), (count, 6 * rows, 128))
    sent = jnp.concatenate([columns, flat], axis=1)
    got = lax.all_to_all(sent, "lon", 0, 0, tiled=True)
    left = lax.dynamic_index_in_dim(got, (me + count - 1) % count, 0, keepdims=False)
    right = lax.dynamic_index_in_dim(got, (me + 1) % count, 0, keepdims=False)
    shape = (rows, 2, 128)
    edge = jnp.concatenate(
        [
            right[: 2 * rows].reshape(shape),
            jnp.zeros((rows, WIDE - 132, 128), jnp.bfloat16),
            left[: 2 * rows].reshape(shape),
        ],
        axis=1,
    )
    lane = lax.broadcasted_iota(jnp.int32, (1, 1, 128), 2)
    shape = (6, rows, 128)
    second = jnp.where(
        lane < 64, right[2 * rows :].reshape(shape), left[2 * rows :].reshape(shape)
    )
    every = got[:, 2 * rows :].reshape(count, 2, 3, rows, 128).astype(jnp.float32).sum(axis=2)
    summed = jnp.sum(every[:, 0])
    counted = jnp.sum(jnp.where(every[:, 1] > 0.0, 1.0, 0.0))
    return edge, second, summed, counted


def two_pieces(values):
    return jnp.concatenate(pieces_of(values, 2))


def from_pieces(pieces):
    both = pieces.astype(jnp.float32)
    count = both.shape[-2] // 2
    return both[..., :count, :] + both[..., count:, :]


def all_summed(weight, vectors):
    channels = weight.shape[1]
    n_y, n_z, n_c = (lax.axis_size(name) for name in LAT)
    n_x = lax.axis_size("lon")
    n_d = lax.axis_size("dp")
    share = channels // (n_y * n_z * n_c * n_x)
    parts = weight.reshape(9, n_y, n_z, n_c, n_x * share, channels)
    core = lax.axis_index("lat_2")
    own = jnp.where(core == 0, parts[:, :, :, 0], parts[:, :, :, 1])
    other = jnp.where(core == 0, parts[:, :, :, 1], parts[:, :, :, 0])
    sent = jnp.concatenate(
        [other.astype(jnp.bfloat16).reshape(-1, channels), two_pieces(vectors)], axis=0
    )
    got = lax.ppermute(sent, "lat_2", [(0, 1), (1, 0)])
    own = own + got[:-4].astype(jnp.float32).reshape(own.shape)
    vectors = vectors + from_pieces(got[-4:])
    rows = share * 9
    own = own.astype(jnp.bfloat16).reshape(9, n_y, n_z, n_x, share, channels)
    by_peer = own.transpose(1, 3, 2, 0, 4, 5).reshape(n_y * n_x, n_z * rows, channels)
    extra = jnp.broadcast_to(two_pieces(vectors)[None], (n_y * n_x, 4, channels))
    sent = jnp.concatenate([by_peer, extra], axis=1)
    got = lax.all_to_all(sent, ("lat_0", "lon"), 0, 0, tiled=True)
    own = got[:, :-4].astype(jnp.float32).sum(axis=0).reshape(n_z, rows, channels)
    vectors = from_pieces(got[:, -4:]).sum(axis=0)
    sent = jnp.concatenate([own, jnp.broadcast_to(vectors[None], (n_z, 2, channels))], axis=1)
    sent = jnp.broadcast_to(sent[:, None], (n_z, n_d, rows + 2, channels))
    sent = sent.reshape(n_z * n_d, rows + 2, channels)
    total = lax.all_to_all(sent, ("lat_1", "dp"), 0, 0, tiled=True).sum(axis=0)
    own = total[:rows].reshape(3, 3, share, channels).transpose(2, 0, 1, 3)
    return own, total[rows], total[rows + 1]


def shards(
    hidden_in, conv_weight, conv_bias, proj_weight, ocean_depth, sea_mask,
    step_alpha, step_beta, surface_cotangent,
):
    rows = hidden_in.shape[1]
    hidden = hidden_in[0]
    mask = sea_mask.astype(jnp.float32)
    fields = jnp.stack(
        pieces_of(mask * surface_cotangent[0], 3) + pieces_of(mask * ocean_depth, 3)
    )
    edge, second, summed, counted = gathered_edges(hidden, fields)
    fields = jnp.concatenate([fields[:, None], second[:, None]], axis=1)

    def outgoing(at, field_at):
        cells = jnp.concatenate([hidden[at : at + 2], edge[at : at + 2]], axis=1)
        near = fields[:, :, field_at : field_at + REACH]
        return cells.reshape(2 * WIDE, 128), near.reshape(12 * REACH, 128)

    n_lat = lax.axis_size(LAT)
    lat = lax.axis_index(LAT)
    upper = lax.axis_index("lat_2") == 0
    up, down = outgoing(0, 0), outgoing(rows - 2, rows - REACH)
    sums = jnp.broadcast_to(
        jnp.stack(pieces_of(summed, 3) + pieces_of(counted, 3))[:, None], (6, 128)
    )
    cross = jnp.concatenate([jnp.where(upper, u, d) for u, d in zip(up, down)] + [sums])
    pair = jnp.concatenate([jnp.where(upper, d, u) for u, d in zip(up, down)])
    odd = [(i, (i + 1) % n_lat) for i in range(1, n_lat, 2)]
    cross = lax.ppermute(cross, LAT, odd + [(j, i) for i, j in odd])
    pair = lax.ppermute(pair, "lat_2", [(0, 1), (1, 0)])
    got = cross[-6:, 0].astype(jnp.float32)
    sums = jnp.stack([summed + got[0] + got[1] + got[2], counted + got[3] + got[4] + got[5]])
    others = lax.axis_size(("lat_0", "lat_2"))
    sums = lax.all_to_all(
        jnp.broadcast_to(sums[None, :, None], (others, 2, 128)), ("lat_0", "lat_2"), 0, 0, tiled=True
    )
    sums = jnp.sum(sums[:, :, 0], axis=0)
    mean = (sums[0] / sums[1])[None]

    cross = cross[:-6]
    zero = jnp.zeros((), jnp.bfloat16)
    above = jnp.where(lat == 0, zero, jnp.where(upper, cross, pair))
    below = jnp.where(lat == n_lat - 1, zero, jnp.where(upper, pair, cross))
    split_at = 2 * WIDE
    ends = jnp.concatenate([above[:split_at], below[:split_at]]).reshape(4, WIDE, 128)
    shape = (6, 2, REACH, 128)
    fields = jnp.concatenate(
        [
            above[split_at:].reshape(shape),
            fields,
            below[split_at:].reshape(shape),
            jnp.zeros((6, 2, PACK - rows - 2 * REACH, 128), jnp.bfloat16),
        ],
        axis=2,
    )
    fields = fields.reshape(2, 3, 2 * PACK, 128).transpose(1, 0, 2, 3)

    ext, preact, force = call(
        forward_kernel,
        (
            jax.ShapeDtypeStruct((rows + 4, WIDE, 128), jnp.bfloat16),
            jax.ShapeDtypeStruct((rows + 2, WIDE, 128), jnp.float32),
            jax.ShapeDtypeStruct((128, 128), jnp.float32),
        ),
        [pltpu.VMEM((384, 384), jnp.bfloat16)],
        [VMEM] * 6 + [SMEM] * 2,
        (hidden, edge, ends, fields, conv_weight, conv_bias[None], step_alpha, step_beta),
        "forward",
    )
    grad, weight, vectors = call(
        backward_kernel,
        (
            jax.ShapeDtypeStruct((rows + 2, WIDE, 128), jnp.bfloat16),
            jax.ShapeDtypeStruct((9, 128, 128), jnp.float32),
            jax.ShapeDtypeStruct((2, 128), jnp.float32),
        ),
        [pltpu.VMEM((rows, WIDE, 384), jnp.bfloat16)],
        [SMEM] + [VMEM] * 4,
        (mean, preact, force, ext, proj_weight[None]),
        "backward",
    )
    grad_hidden = call(
        input_kernel,
        jax.ShapeDtypeStruct((rows, 128, 128), jnp.bfloat16),
        [pltpu.VMEM((384, 384), jnp.bfloat16)],
        [VMEM] * 2,
        (grad, conv_weight),
        "input_grad",
    )
    own_weight, total_bias, total_proj = all_summed(weight, vectors)
    cells = rows * 128 * lax.axis_size("dp") * n_lat * lax.axis_size("lon")
    grad_scale = 1.0 / math.sqrt(cells)
    return (
        grad_hidden[None],
        own_weight * grad_scale,
        total_bias * grad_scale,
        total_proj * grad_scale,
    )


def solution(mesh):
    split = Mesh(
        mesh.devices.reshape(mesh.shape["dp"], 4, 2, 2, mesh.shape["lon"]),
        ("dp", "lat_0", "lat_1", "lat_2", "lon"),
    )
    placed = (
        P("dp", LAT, "lon", None),
        P(),
        P(),
        P(),
        P(LAT, "lon"),
        P(LAT, "lon"),
        P(),
        P(),
        P("dp", LAT, "lon"),
    )
    return jax.shard_map(
        shards,
        mesh=split,
        in_specs=placed,
        out_specs=(P("dp", LAT, "lon", None), P(LAT_LON, None, None, None), P(), P()),
        check_vma=False,
    )
```

```python
import functools
import math

import jax
import jax.numpy as jnp
from jax import lax
from jax.experimental import pallas as pl
from jax.experimental.pallas import tpu as pltpu
from jax.sharding import Mesh
from jax.sharding import PartitionSpec as P

ITERS = 6
LAT_LON = ("lat_0", "lat_1", "lat_2", "lon")
LAT = ("lat_0", "lat_1", "lat_2")
WIDE = 144
PACK = 32
PLANES = 5
SENT = 64 + PLANES * PACK

helm_coef = 0.5
VMEM = pl.BlockSpec(memory_space=pltpu.VMEM)
SMEM = pl.BlockSpec(memory_space=pltpu.SMEM)


def rounded(values):
    return values.astype(jnp.bfloat16).astype(jnp.float32)


def pieces_of(values, count):
    out = []
    for _ in range(count):
        piece = rounded(values)
        out.append(piece)
        values = values - piece
    return out


def full(value):
    return jnp.full((1, 128), value, jnp.float32)


def first_kernel(
    at_ref, hidden_ref, cot_ref, mask_ref, depth_ref, cross_ref, pair_ref, planes_ref, sums_ref
):
    rows = hidden_ref.shape[0]
    upper = at_ref[0] == 0
    mask = mask_ref[...].astype(jnp.float32)
    wet = mask * cot_ref[0]
    planes = pieces_of(wet, 3) + pieces_of(mask * depth_ref[...], 2)
    summed, counted = jnp.sum(wet), jnp.sum(mask)
    sums_ref[0:1] = full(summed)
    sums_ref[1:2] = full(counted)
    sums = pieces_of(full(summed), 3) + pieces_of(full(counted), 3)
    sums = jnp.concatenate(sums + [jnp.zeros((2, 128), jnp.float32)], axis=0)
    for k in range(PLANES):
        planes_ref[k] = planes[k]
    for ref, top in ((cross_ref, upper), (pair_ref, jnp.logical_not(upper))):
        start = jnp.where(top, 0, rows - 2)
        ref[0:256] = hidden_ref[pl.ds(start, 2)].reshape(256, 128)
        near = [jnp.where(top, p[0:8], p[rows - 8 : rows]) for p in planes] + [sums]
        for k in range(0, 6, 2):
            tile = jnp.concatenate(near[k : k + 2], axis=0)
            ref[256 + k * 8 : 272 + k * 8] = tile.astype(jnp.bfloat16)


def second_kernel(
    at_ref, hidden_ref, planes_ref, sums_ref, cross_ref, pair_ref,
    ends_ref, fields_ref, sent_ref, total_ref,
):
    rows = hidden_ref.shape[0]
    upper = at_ref[0] == 0
    keep_above = jnp.where(at_ref[1] == 0, 0.0, 1.0)
    keep_below = jnp.where(at_ref[2] == 0, 0.0, 1.0)
    zero = jnp.zeros((), jnp.bfloat16)
    for k in range(2):
        cross = cross_ref[k * 128 : k * 128 + 128]
        pair = pair_ref[k * 128 : k * 128 + 128]
        ends_ref[k] = jnp.where(keep_above > 0.0, jnp.where(upper, cross, pair), zero)
        ends_ref[k + 2] = jnp.where(keep_below > 0.0, jnp.where(upper, pair, cross), zero)
    cross = cross_ref[256:304].astype(jnp.float32)
    pair = pair_ref[256:304].astype(jnp.float32)
    got = cross[40:48]
    summed = sums_ref[0:1] + got[0:1] + got[1:2] + got[2:3]
    counted = sums_ref[1:2] + got[3:4] + got[4:5] + got[5:6]
    lane = lax.broadcasted_iota(jnp.int32, (1, 128), 1)
    total = jnp.where(lane < 64, summed, counted)
    total_ref[...] = jnp.broadcast_to(total[None], total_ref.shape)
    above = jnp.where(upper, cross, pair) * keep_above
    below = jnp.where(upper, pair, cross) * keep_below
    fields = []
    for k in range(PLANES):
        at = k * 8
        fields.append(
            jnp.concatenate([above[at : at + 8], planes_ref[k], below[at : at + 8]], axis=0)
        )
    fields_ref[0] = fields[0] + fields[1] + fields[2]
    fields_ref[1] = fields[3] + fields[4]
    place = lax.broadcasted_iota(jnp.int32, (8, 128), 0)
    columns = [[jnp.zeros((8, 128), jnp.float32) for _ in range(4)] for _ in range(4)]
    for r in range(rows + 4):
        if r < 2:
            source = ends_ref.at[r]
        elif r < rows + 2:
            source = hidden_ref.at[r - 2]
        else:
            source = ends_ref.at[r - rows]
        head = source[0:16].astype(jnp.float32)
        tail = source[112:128].astype(jnp.float32)
        for k, row in enumerate((head[0:1], head[1:2], tail[14:15], tail[15:16])):
            columns[k][r // 8] = jnp.where(place == r % 8, row, columns[k][r // 8])
    columns = [jnp.concatenate(tiles, axis=0) for tiles in columns]
    fields = [f.astype(jnp.bfloat16) for f in fields]
    for peer in range(sent_ref.shape[0]):
        to_right = at_ref[4] == peer
        for k in range(2):
            chosen = jnp.where(to_right, columns[2 + k], columns[k])
            sent_ref[peer, k * 32 : k * 32 + 32] = chosen.astype(jnp.bfloat16)
        for k in range(PLANES):
            sent_ref[peer, 64 + k * PACK : 64 + k * PACK + PACK] = fields[k]


def forward_kernel(
    at_ref, hidden_ref, ends_ref, fields_ref, got_ref, weight_ref, bias_ref, alpha_ref, beta_ref,
    ext_ref, preact_ref, force_ref, rhs_ref,
):
    rows = hidden_ref.shape[0]
    left, right = at_ref[3], at_ref[4]
    ext_ref[0:2, 0:128] = ends_ref[0:2]
    ext_ref[2 : rows + 2, 0:128] = hidden_ref[...]
    ext_ref[rows + 2 : rows + 4, 0:128] = ends_ref[2:4]
    columns = got_ref[right, 0:64].astype(jnp.float32), got_ref[left, 0:64].astype(jnp.float32)
    place = lax.broadcasted_iota(jnp.int32, (WIDE - 128, 128), 0)
    for r in range(rows + 4):
        tile = jnp.zeros((WIDE - 128, 128), jnp.float32)
        for side, base in enumerate((0, WIDE - 130)):
            for k in range(2):
                row = columns[side][k * 32 + r : k * 32 + r + 1]
                tile = jnp.where(place == base + k, row, tile)
        ext_ref[r, 128:WIDE] = tile.astype(jnp.bfloat16)
    for a in range(3):
        for c in range(3):
            rhs_ref[a * 128 : a * 128 + 128, c * 128 : c * 128 + 128] = weight_ref[a, c]

    lane = lax.broadcasted_iota(jnp.int32, (2 * PACK, 128), 1)
    second = jnp.where(
        jnp.concatenate([lane] * 3, axis=0)[: PLANES * PACK] < 64,
        got_ref[right, 64:SENT].astype(jnp.float32),
        got_ref[left, 64:SENT].astype(jnp.float32),
    )
    second = [second[k * PACK : k * PACK + PACK] for k in range(PLANES)]
    start = jnp.concatenate([fields_ref[0], second[0] + second[1] + second[2]], axis=0)
    wet_depth = jnp.concatenate([fields_ref[1], second[3] + second[4]], axis=0)
    mask = jnp.where(wet_depth > 0.0, 1.0, 0.0)

    def other_half(field):
        parts = [field[k * PACK : (k + 1) * PACK] for k in range(field.shape[0] // PACK)]
        swapped = []
        for k in range(0, len(parts), 2):
            swapped += [parts[k + 1], parts[k]]
        return jnp.concatenate(swapped, axis=0)

    def beside(field):
        count = field.shape[0]
        lanes = lane if count == 2 * PACK else jnp.concatenate([lane, lane], axis=0)
        up = pltpu.roll(field, 1, 0)
        down = pltpu.roll(field, count - 1, 0)
        from_left = pltpu.roll(field, 1, 1)
        from_left = jnp.where(lanes == 0, other_half(from_left), from_left)
        from_right = pltpu.roll(field, 127, 1)
        from_right = jnp.where(lanes == 127, other_half(from_right), from_right)
        return up, down, from_left, from_right

    weights = [
        0.5 * (near_mask * wet_depth + mask * near_depth)
        for near_mask, near_depth in zip(beside(mask), beside(wet_depth))
    ]
    diagonal = helm_coef * mask + weights[0] + weights[1] + weights[2] + weights[3]
    weights = [jnp.concatenate([w, w], axis=0) for w in weights]
    diagonal = jnp.concatenate([diagonal, diagonal], axis=0)
    residual = jnp.concatenate([start, mask], axis=0)
    direction = residual
    result = jnp.zeros_like(residual)
    for k in range(ITERS):
        result = result + alpha_ref[k] * direction
        if k + 1 < ITERS:
            applied = diagonal * direction
            for w, near in zip(weights, beside(direction)):
                applied = applied - w * near
            residual = residual - alpha_ref[k] * applied
            direction = residual + beta_ref[k] * direction
    result = result * jnp.concatenate([mask, mask], axis=0)
    force_ref[...] = result.T

    group = 6
    bias = bias_ref[...]
    for g in range(0, rows + 2, group):
        lhs = jnp.concatenate(
            [ext_ref[g + a : g + a + group].reshape(group * WIDE, 128) for a in range(3)], axis=1
        )
        out = jnp.dot(lhs, rhs_ref[...], preferred_element_type=jnp.float32)
        for j in range(group):
            part = out[j * WIDE : (j + 1) * WIDE]
            preact_ref[g + j] = (
                pltpu.roll(part[:, 0:128], 1, 0)
                + part[:, 128:256]
                + pltpu.roll(part[:, 256:384], WIDE - 1, 0)
                + bias
            )


def backward_kernel(
    total_ref, preact_ref, force_ref, ext_ref, proj_ref,
    grad_ref, sent_ref, moved_ref, weight_ref,
):
    rows = grad_ref.shape[0] - 2
    total = jnp.sum(total_ref[...], axis=0)
    mean = jnp.broadcast_to(total[:, 0:1], (1, 128)) / jnp.broadcast_to(total[:, 127:128], (1, 128))
    force = force_ref[...]
    force = force - mean * pltpu.roll(force, 64, 1)
    proj = proj_ref[...]
    sum_bias = jnp.zeros((8, 128), jnp.float32)
    sum_proj = jnp.zeros((8, 128), jnp.float32)
    for g in range(rows + 2):
        at = g + 7
        column = jnp.concatenate(
            [
                force[:, at : at + 1],
                force[0:8, PACK + at : PACK + at + 1],
                force[120:128, PACK + at : PACK + at + 1],
            ],
            axis=0,
        )
        column = jnp.broadcast_to(column, (WIDE, 128))
        preact = preact_ref[g]
        sigma = jax.nn.sigmoid(preact)
        active = preact * sigma
        slope_act = sigma * (1.0 + preact * (1.0 - sigma))
        grad = (column * proj * slope_act).astype(jnp.bfloat16)
        grad_ref[g] = grad
        if 1 <= g <= rows:
            own = grad.astype(jnp.float32)[0:128]
            for k in range(16):
                sum_bias = sum_bias + own[k * 8 : k * 8 + 8]
                sum_proj = sum_proj + (active * column)[k * 8 : k * 8 + 8]
            own = jnp.concatenate([own, jnp.zeros((WIDE - 128, 128), jnp.float32)], axis=0)
            moved_ref[g - 1, :, 0:128] = pltpu.roll(own, WIDE - 1, 0).astype(jnp.bfloat16)
            moved_ref[g - 1, :, 128:256] = own.astype(jnp.bfloat16)
            moved_ref[g - 1, :, 256:384] = pltpu.roll(own, 1, 0).astype(jnp.bfloat16)
    moved = moved_ref[...].reshape(rows * WIDE, 384)
    for a in range(3):
        cells = ext_ref[a + 1 : a + 1 + rows].reshape(rows * WIDE, 128)
        out = lax.dot_general(
            cells, moved, (((0,), (0,)), ((), ())), preferred_element_type=jnp.float32
        )
        for c in range(3):
            weight_ref[a * 3 + c] = out[:, c * 128 : c * 128 + 128]
    vectors = jnp.concatenate(
        [jnp.sum(sum_bias, axis=0, keepdims=True), jnp.sum(sum_proj, axis=0, keepdims=True)], axis=0
    )
    vectors = jnp.concatenate(pieces_of(vectors, 2) + [jnp.zeros((4, 128), jnp.float32)], axis=0)
    vectors = pltpu.roll(vectors, 4, 0)
    place = lax.broadcasted_iota(jnp.int32, (8, 128), 0) // 2

    def one_pair(at, carry):
        y, c = at // 2, at % 2
        for x in range(4):
            tiles = []
            for t in range(5):
                tile = vectors
                for j in range(4):
                    slot = 4 * t + j
                    if slot >= 18:
                        continue
                    z, k = slot // 9, slot % 9
                    start = pl.multiple_of(((y * 2 + z) * 2 + c) * 8, 8)
                    piece = weight_ref[k, pl.ds(start, 8)]
                    if j != x:
                        piece = pltpu.roll(piece, (2 * j - 2 * x) % 8, 0)
                    tile = jnp.where(place == j, piece, tile)
                tiles.append(tile)
            sent_ref[at * 4 + x] = jnp.concatenate(tiles, axis=0).astype(jnp.bfloat16)
        return carry

    lax.fori_loop(0, 8, one_pair, 0)


def middle_kernel(got_ref, sent_ref):
    total = jnp.sum(got_ref[...].astype(jnp.float32), axis=0)
    vectors = total[36:38] + total[38:40]
    vectors = jnp.concatenate(pieces_of(vectors, 2) + [jnp.zeros((2, 128), jnp.float32)], axis=0)
    peers = sent_ref.shape[0] // 2
    for z in range(2):
        block = jnp.concatenate([total[z * 18 : z * 18 + 18], vectors], axis=0)
        block = block.astype(jnp.bfloat16)
        for d in range(peers):
            sent_ref[z * peers + d] = block


def last_kernel(scale, got_ref, weight_ref, bias_ref, proj_ref):
    total = jnp.sum(got_ref[...].astype(jnp.float32), axis=0) * scale
    for k in range(9):
        for e in range(2):
            weight_ref[e, k // 3, k % 3 : k % 3 + 1] = total[k * 2 + e : k * 2 + e + 1]
    bias_ref[...] = total[18:19] + total[20:21]
    proj_ref[...] = total[19:20] + total[21:22]


def input_kernel(grad_ref, weight_ref, out_ref, rhs_ref):
    rows = out_ref.shape[0]
    for a in range(3):
        for c in range(3):
            rhs_ref[c * 128 : c * 128 + 128, a * 128 : a * 128 + 128] = weight_ref[a, c]
    group = 4
    for y in range(0, rows, group):
        lhs = jnp.concatenate(
            [
                grad_ref[y - a + 2 : y - a + 2 + group].reshape(group * WIDE, 128)
                for a in range(3)
            ],
            axis=1,
        )
        out = lax.dot_general(
            lhs, rhs_ref[...], (((1,), (1,)), ((), ())), preferred_element_type=jnp.float32
        )
        for j in range(group):
            part = out[j * WIDE : (j + 1) * WIDE]
            total = (
                pltpu.roll(part[:, 0:128], WIDE - 1, 0)
                + part[:, 128:256]
                + pltpu.roll(part[:, 256:384], 1, 0)
            )
            out_ref[y + j] = total[0:128].astype(jnp.bfloat16)


def call(kernel, shapes, scratch, in_specs, args, name):
    return pl.pallas_call(
        kernel,
        out_shape=shapes,
        in_specs=in_specs,
        out_specs=jax.tree.map(lambda _: VMEM, shapes),
        scratch_shapes=scratch,
        compiler_params=pltpu.CompilerParams(vmem_limit_bytes=40 * 1024 * 1024),
        name=name,
    )(*args)


def shape(dims, dtype):
    return jax.ShapeDtypeStruct(dims, dtype)


def shards(
    hidden_in, conv_weight, conv_bias, proj_weight, ocean_depth, sea_mask,
    step_alpha, step_beta, surface_cotangent,
):
    wide, narrow = jnp.float32, jnp.bfloat16
    rows = hidden_in.shape[1]
    hidden = hidden_in[0]
    n_x = lax.axis_size("lon")
    n_lat = lax.axis_size(LAT)
    n_all = lax.axis_size(("lat_0", "lat_2", "lon"))
    n_z = lax.axis_size(("lat_1", "dp"))
    lat, x = lax.axis_index(LAT), lax.axis_index("lon")
    at = jnp.stack(
        [lat % 2, lat, n_lat - 1 - lat, (x + n_x - 1) % n_x, (x + 1) % n_x]
    ).astype(jnp.int32)
    cross, pair, planes, sums = call(
        first_kernel,
        (
            shape((304, 128), narrow),
            shape((304, 128), narrow),
            shape((PLANES, rows, 128), wide),
            shape((2, 128), wide),
        ),
        [],
        [SMEM] + [VMEM] * 4,
        (at, hidden, surface_cotangent, sea_mask, ocean_depth),
        "first",
    )
    odd = [(i, (i + 1) % n_lat) for i in range(1, n_lat, 2)]
    cross = lax.ppermute(cross, LAT, odd + [(j, i) for i, j in odd])
    pair = lax.ppermute(pair, "lat_2", [(0, 1), (1, 0)])
    ends, fields, sent, total = call(
        second_kernel,
        (
            shape((4, 128, 128), narrow),
            shape((2, PACK, 128), wide),
            shape((n_x, SENT, 128), narrow),
            shape((n_all, 1, 128), wide),
        ),
        [],
        [SMEM] + [VMEM] * 5,
        (at, hidden, planes, sums, cross, pair),
        "second",
    )
    got = lax.all_to_all(sent, "lon", 0, 0, tiled=True)
    total = lax.all_to_all(total, ("lat_0", "lat_2", "lon"), 0, 0, tiled=True)
    ext, preact, force = call(
        forward_kernel,
        (
            shape((rows + 4, WIDE, 128), narrow),
            shape((rows + 2, WIDE, 128), wide),
            shape((128, 128), wide),
        ),
        [pltpu.VMEM((384, 384), narrow)],
        [SMEM] + [VMEM] * 6 + [SMEM] * 2,
        (at, hidden, ends, fields, got, conv_weight, conv_bias[None], step_alpha, step_beta),
        "forward",
    )
    grad, sent = call(
        backward_kernel,
        (shape((rows + 2, WIDE, 128), narrow), shape((n_all, 40, 128), narrow)),
        [pltpu.VMEM((rows, WIDE, 384), narrow), pltpu.VMEM((9, 128, 128), wide)],
        [VMEM] * 5,
        (total, preact, force, ext, proj_weight[None]),
        "backward",
    )
    got = lax.all_to_all(sent, ("lat_0", "lat_2", "lon"), 0, 0, tiled=True)
    sent = call(middle_kernel, shape((n_z, 24, 128), narrow), [], [VMEM], (got,), "middle")
    got = lax.all_to_all(sent, ("lat_1", "dp"), 0, 0, tiled=True)
    grad_hidden = call(
        input_kernel,
        shape((rows, 128, 128), narrow),
        [pltpu.VMEM((384, 384), narrow)],
        [VMEM] * 2,
        (grad, conv_weight),
        "input_grad",
    )
    cells = rows * 128 * lax.axis_size("dp") * n_lat * n_x
    own_weight, total_bias, total_proj = call(
        functools.partial(last_kernel, 1.0 / math.sqrt(cells)),
        (shape((2, 3, 3, 128), wide), shape((1, 128), wide), shape((1, 128), wide)),
        [],
        [VMEM],
        (got,),
        "last",
    )
    return grad_hidden[None], own_weight, total_bias[0], total_proj[0]


def solution(mesh):
    split = Mesh(
        mesh.devices.reshape(mesh.shape["dp"], 4, 2, 2, mesh.shape["lon"]),
        ("dp", "lat_0", "lat_1", "lat_2", "lon"),
    )
    placed = (
        P("dp", LAT, "lon", None),
        P(),
        P(),
        P(),
        P(LAT, "lon"),
        P(LAT, "lon"),
        P(),
        P(),
        P("dp", LAT, "lon"),
    )
    return jax.shard_map(
        shards,
        mesh=split,
        in_specs=placed,
        out_specs=(P("dp", LAT, "lon", None), P(LAT_LON, None, None, None), P(), P()),
        check_vma=False,
    )
```

```python
import functools
import math

import jax
import jax.numpy as jnp
from jax import lax
from jax.experimental import pallas as pl
from jax.experimental.pallas import tpu as pltpu
from jax.sharding import Mesh
from jax.sharding import PartitionSpec as P

ITERS = 6
LAT_LON = ("lat_0", "lat_1", "lat_2", "lon")
LAT = ("lat_0", "lat_1", "lat_2")
WIDE = 144
PACK = 32
PLANES = 5
SENT = 64 + PACK + 16

helm_coef = 0.5
VMEM = pl.BlockSpec(memory_space=pltpu.VMEM)
SMEM = pl.BlockSpec(memory_space=pltpu.SMEM)
HBM = pl.BlockSpec(memory_space=pltpu.HBM)


def rounded(values):
    return values.astype(jnp.bfloat16).astype(jnp.float32)


def pieces_of(values, count):
    out = []
    for _ in range(count):
        piece = rounded(values)
        out.append(piece)
        values = values - piece
    return out


def full(value):
    return jnp.full((1, 128), value, jnp.float32)


def first_kernel(
    at_ref, hidden_ref, cot_hbm, mask_hbm, depth_hbm,
    cross_ref, pair_ref, planes_ref, sums_ref,
    cot_ref, mask_ref, depth_ref, sems,
):
    rows = mask_ref.shape[0]
    upper = at_ref[0] == 0
    last = (rows - 2) * 128
    starts = (jnp.where(upper, 0, last), jnp.where(upper, last, 0))
    copies = [
        pltpu.make_async_copy(cot_hbm.at[0], cot_ref, sems.at[0]),
        pltpu.make_async_copy(mask_hbm, mask_ref, sems.at[1]),
        pltpu.make_async_copy(depth_hbm, depth_ref, sems.at[2]),
    ]
    for k, ref in enumerate((cross_ref, pair_ref)):
        start = pl.multiple_of(starts[k], 128)
        copies.append(
            pltpu.make_async_copy(
                hidden_ref.at[pl.ds(start, 256)], ref.at[pl.ds(0, 256)], sems.at[3 + k]
            )
        )
    for copy in copies:
        copy.start()
    for copy in copies[:3]:
        copy.wait()
    mask = mask_ref[...].astype(jnp.float32)
    wet = mask * cot_ref[...]
    planes = pieces_of(wet, 3) + pieces_of(mask * depth_ref[...], 2)
    lane = lax.broadcasted_iota(jnp.int32, (1, 128), 1)
    sums = jnp.where(lane < 64, full(jnp.sum(wet)), full(jnp.sum(mask)))
    sums_ref[...] = jnp.broadcast_to(sums[None], sums_ref.shape)
    for k in range(PLANES):
        planes_ref[k] = planes[k]
    planes = planes + [planes[0]]
    for ref, top in ((cross_ref, upper), (pair_ref, jnp.logical_not(upper))):
        near = [jnp.where(top, p[0:8], p[rows - 8 : rows]) for p in planes]
        for k in range(0, 6, 2):
            tile = jnp.concatenate(near[k : k + 2], axis=0)
            ref[256 + k * 8 : 272 + k * 8] = tile.astype(jnp.bfloat16)
    for copy in copies[3:]:
        copy.wait()


def second_kernel(
    at_ref, hidden_ref, planes_ref, sums_ref, cross_ref, pair_ref,
    ends_ref, fields_ref, sent_ref,
):
    rows = hidden_ref.shape[0]
    upper = at_ref[0] == 0
    keep_above = jnp.where(at_ref[1] == 0, 0.0, 1.0)
    keep_below = jnp.where(at_ref[2] == 0, 0.0, 1.0)
    zero = jnp.zeros((), jnp.bfloat16)
    for k in range(2):
        cross = cross_ref[k * 128 : k * 128 + 128]
        pair = pair_ref[k * 128 : k * 128 + 128]
        ends_ref[k] = jnp.where(keep_above > 0.0, jnp.where(upper, cross, pair), zero)
        ends_ref[k + 2] = jnp.where(keep_below > 0.0, jnp.where(upper, pair, cross), zero)
    cross = cross_ref[256:304].astype(jnp.float32)
    pair = pair_ref[256:304].astype(jnp.float32)
    total = jnp.sum(sums_ref[...], axis=0)
    summed = jnp.broadcast_to(total[:, 0:1], (1, 128))
    counted = jnp.broadcast_to(total[:, 127:128], (1, 128))
    sums = pieces_of(summed, 3) + pieces_of(counted, 3)
    sums = jnp.concatenate(sums + [jnp.zeros((10, 128), jnp.float32)], axis=0)
    above = jnp.where(upper, cross, pair) * keep_above
    below = jnp.where(upper, pair, cross) * keep_below
    fields = []
    for k in range(PLANES):
        at = k * 8
        fields.append(
            jnp.concatenate([above[at : at + 8], planes_ref[k], below[at : at + 8]], axis=0)
        )
    fields_ref[0] = fields[0] + fields[1] + fields[2]
    fields_ref[1] = fields[3] + fields[4]
    place = lax.broadcasted_iota(jnp.int32, (8, 128), 0)
    columns = [[jnp.zeros((8, 128), jnp.float32) for _ in range(4)] for _ in range(4)]
    for r in range(rows + 4):
        if r < 2:
            source = ends_ref.at[r]
        elif r < rows + 2:
            source = hidden_ref.at[r - 2]
        else:
            source = ends_ref.at[r - rows]
        head = source[0:16].astype(jnp.float32)
        tail = source[112:128].astype(jnp.float32)
        for k, row in enumerate((head[0:1], head[1:2], tail[14:15], tail[15:16])):
            columns[k][r // 8] = jnp.where(place == r % 8, row, columns[k][r // 8])
    columns = [jnp.concatenate(tiles, axis=0) for tiles in columns]
    lane = lax.broadcasted_iota(jnp.int32, (PACK, 128), 1) // 8
    heads = tails = jnp.zeros((PACK, 128), jnp.float32)
    for k in range(PLANES):
        head = fields[k] if k == 0 else pltpu.roll(fields[k], 8 * k, 1)
        heads = jnp.where(lane == k, head, heads)
        tails = jnp.where(lane == k, pltpu.roll(fields[k], 8 * k + 8, 1), tails)
    heads = jnp.concatenate(columns[0:2] + [heads, sums], axis=0)
    tails = jnp.concatenate(columns[2:4] + [tails, sums], axis=0)
    for peer in range(sent_ref.shape[0]):
        sent_ref[peer] = jnp.where(at_ref[4] == peer, tails, heads).astype(jnp.bfloat16)


def main_kernel(
    at_ref, hidden_ref, ends_ref, fields_ref, got_ref, weight_ref, bias_ref, proj_ref,
    alpha_ref, beta_ref,
    grad_hbm, sent_ref,
    ext_ref, preact_ref, rhs_ref, grad_ref, moved_ref, total_ref, sem,
):
    rows = hidden_ref.shape[0]
    left, right = at_ref[3], at_ref[4]
    ext_ref[0:2, 0:128] = ends_ref[0:2]
    ext_ref[2 : rows + 2, 0:128] = hidden_ref[...]
    ext_ref[rows + 2 : rows + 4, 0:128] = ends_ref[2:4]
    columns = got_ref[right, 0:64].astype(jnp.float32), got_ref[left, 0:64].astype(jnp.float32)
    place = lax.broadcasted_iota(jnp.int32, (WIDE - 128, 128), 0)
    for r in range(rows + 4):
        tile = jnp.zeros((WIDE - 128, 128), jnp.float32)
        for side, base in enumerate((0, WIDE - 130)):
            for k in range(2):
                row = columns[side][k * 32 + r : k * 32 + r + 1]
                tile = jnp.where(place == base + k, row, tile)
        ext_ref[r, 128:WIDE] = tile.astype(jnp.bfloat16)
    for a in range(3):
        for c in range(3):
            rhs_ref[a * 128 : a * 128 + 128, c * 128 : c * 128 + 128] = weight_ref[a, c]

    lane = lax.broadcasted_iota(jnp.int32, (2 * PACK, 128), 1)
    from_left = got_ref[left, 64 : 64 + PACK].astype(jnp.float32)
    from_right = got_ref[right, 64 : 64 + PACK].astype(jnp.float32)
    second = []
    for k in range(PLANES):
        beyond = from_right if k == 0 else pltpu.roll(from_right, 128 - 8 * k, 1)
        before = pltpu.roll(from_left, 120 - 8 * k, 1)
        near = lane[:PACK]
        second.append(jnp.where(near < 8, beyond, jnp.where(near >= 120, before, 0.0)))
    start = jnp.concatenate([fields_ref[0], second[0] + second[1] + second[2]], axis=0)
    wet_depth = jnp.concatenate([fields_ref[1], second[3] + second[4]], axis=0)
    mask = jnp.where(wet_depth > 0.0, 1.0, 0.0)

    def other_half(field):
        parts = [field[k * PACK : (k + 1) * PACK] for k in range(field.shape[0] // PACK)]
        swapped = []
        for k in range(0, len(parts), 2):
            swapped += [parts[k + 1], parts[k]]
        return jnp.concatenate(swapped, axis=0)

    def beside(field):
        count = field.shape[0]
        lanes = lane if count == 2 * PACK else jnp.concatenate([lane, lane], axis=0)
        up = pltpu.roll(field, 1, 0)
        down = pltpu.roll(field, count - 1, 0)
        from_left = pltpu.roll(field, 1, 1)
        from_left = jnp.where(lanes == 0, other_half(from_left), from_left)
        from_right = pltpu.roll(field, 127, 1)
        from_right = jnp.where(lanes == 127, other_half(from_right), from_right)
        return up, down, from_left, from_right

    weights = [
        0.5 * (near_mask * wet_depth + mask * near_depth)
        for near_mask, near_depth in zip(beside(mask), beside(wet_depth))
    ]
    diagonal = helm_coef * mask + weights[0] + weights[1] + weights[2] + weights[3]
    weights = [jnp.concatenate([w, w], axis=0) for w in weights]
    diagonal = jnp.concatenate([diagonal, diagonal], axis=0)
    residual = jnp.concatenate([start, mask], axis=0)
    direction = residual
    result = jnp.zeros_like(residual)
    for k in range(ITERS):
        result = result + alpha_ref[k] * direction
        if k + 1 < ITERS:
            applied = diagonal * direction
            for w, near in zip(weights, beside(direction)):
                applied = applied - w * near
            residual = residual - alpha_ref[k] * applied
            direction = residual + beta_ref[k] * direction
    result = result * jnp.concatenate([mask, mask], axis=0)
    sums = got_ref[:, 64 + PACK : SENT].astype(jnp.float32)
    sums = jnp.sum(sums, axis=0)
    mean = (sums[0:1] + sums[1:2] + sums[2:3]) / (sums[3:4] + sums[4:5] + sums[5:6])
    force = result.T
    force = force - mean * pltpu.roll(force, 64, 1)

    group = 6
    bias = bias_ref[...]
    for g in range(0, rows + 2, group):
        lhs = jnp.concatenate(
            [ext_ref[g + a : g + a + group].reshape(group * WIDE, 128) for a in range(3)], axis=1
        )
        out = jnp.dot(lhs, rhs_ref[...], preferred_element_type=jnp.float32)
        for j in range(group):
            part = out[j * WIDE : (j + 1) * WIDE]
            preact_ref[g + j] = (
                pltpu.roll(part[:, 0:128], 1, 0)
                + part[:, 128:256]
                + pltpu.roll(part[:, 256:384], WIDE - 1, 0)
                + bias
            )

    proj = proj_ref[...]
    sum_bias = jnp.zeros((8, 128), jnp.float32)
    sum_proj = jnp.zeros((8, 128), jnp.float32)
    for g in range(rows + 2):
        at = g + 7
        column = jnp.concatenate(
            [
                force[:, at : at + 1],
                force[0:8, PACK + at : PACK + at + 1],
                force[120:128, PACK + at : PACK + at + 1],
            ],
            axis=0,
        )
        column = jnp.broadcast_to(column, (WIDE, 128))
        preact = preact_ref[g]
        sigma = jax.nn.sigmoid(preact)
        active = preact * sigma
        slope_act = sigma * (1.0 + preact * (1.0 - sigma))
        grad = (column * proj * slope_act).astype(jnp.bfloat16)
        grad_ref[g] = grad
        if 1 <= g <= rows:
            own = grad.astype(jnp.float32)[0:128]
            for k in range(16):
                sum_bias = sum_bias + own[k * 8 : k * 8 + 8]
                sum_proj = sum_proj + (active * column)[k * 8 : k * 8 + 8]
            own = jnp.concatenate([own, jnp.zeros((WIDE - 128, 128), jnp.float32)], axis=0)
            moved_ref[g - 1, :, 0:128] = pltpu.roll(own, WIDE - 1, 0).astype(jnp.bfloat16)
            moved_ref[g - 1, :, 128:256] = own.astype(jnp.bfloat16)
            moved_ref[g - 1, :, 256:384] = pltpu.roll(own, 1, 0).astype(jnp.bfloat16)
    copy = pltpu.make_async_copy(grad_ref, grad_hbm, sem)
    copy.start()
    moved = moved_ref[...].reshape(rows * WIDE, 384)
    for a in range(3):
        cells = ext_ref[a + 1 : a + 1 + rows].reshape(rows * WIDE, 128)
        out = lax.dot_general(
            cells, moved, (((0,), (0,)), ((), ())), preferred_element_type=jnp.float32
        )
        for c in range(3):
            total_ref[a * 3 + c] = out[:, c * 128 : c * 128 + 128]
    vectors = jnp.concatenate(
        [jnp.sum(sum_bias, axis=0, keepdims=True), jnp.sum(sum_proj, axis=0, keepdims=True)], axis=0
    )
    vectors = jnp.concatenate(pieces_of(vectors, 2) + [jnp.zeros((4, 128), jnp.float32)], axis=0)
    vectors = pltpu.roll(vectors, 4, 0)
    place = lax.broadcasted_iota(jnp.int32, (8, 128), 0) // 2

    def one_pair(at, carry):
        y, c = at // 2, at % 2
        for x in range(4):
            tiles = []
            for t in range(5):
                tile = vectors
                for j in range(4):
                    slot = 4 * t + j
                    if slot >= 18:
                        continue
                    z, k = slot // 9, slot % 9
                    start = pl.multiple_of(((y * 2 + z) * 2 + c) * 8, 8)
                    piece = total_ref[k, pl.ds(start, 8)]
                    if j != x:
                        piece = pltpu.roll(piece, (2 * j - 2 * x) % 8, 0)
                    tile = jnp.where(place == j, piece, tile)
                tiles.append(tile)
            sent_ref[at * 4 + x] = jnp.concatenate(tiles, axis=0).astype(jnp.bfloat16)
        return carry

    lax.fori_loop(0, 8, one_pair, 0)
    copy.wait()


def middle_kernel(got_ref, sent_ref):
    total = jnp.sum(got_ref[...].astype(jnp.float32), axis=0)
    vectors = total[36:38] + total[38:40]
    vectors = jnp.concatenate(pieces_of(vectors, 2) + [jnp.zeros((2, 128), jnp.float32)], axis=0)
    peers = sent_ref.shape[0] // 2
    for z in range(2):
        block = jnp.concatenate([total[z * 18 : z * 18 + 18], vectors], axis=0)
        block = block.astype(jnp.bfloat16)
        for d in range(peers):
            sent_ref[z * peers + d] = block


def last_kernel(scale, got_ref, weight_ref, bias_ref, proj_ref):
    total = jnp.sum(got_ref[...].astype(jnp.float32), axis=0) * scale
    for k in range(9):
        weight_ref[k // 3, k % 3] = total[k * 2 : k * 2 + 2]
    bias_ref[...] = total[18:19] + total[20:21]
    proj_ref[...] = total[19:20] + total[21:22]


def input_kernel(grad_ref, weight_ref, out_ref, rhs_ref):
    rows = out_ref.shape[0]
    for a in range(3):
        for c in range(3):
            rhs_ref[c * 128 : c * 128 + 128, a * 128 : a * 128 + 128] = weight_ref[a, c]
    group = 4
    for y in range(0, rows, group):
        lhs = jnp.concatenate(
            [
                grad_ref[y - a + 2 : y - a + 2 + group].reshape(group * WIDE, 128)
                for a in range(3)
            ],
            axis=1,
        )
        out = lax.dot_general(
            lhs, rhs_ref[...], (((1,), (1,)), ((), ())), preferred_element_type=jnp.float32
        )
        for j in range(group):
            part = out[j * WIDE : (j + 1) * WIDE]
            total = (
                pltpu.roll(part[:, 0:128], WIDE - 1, 0)
                + part[:, 128:256]
                + pltpu.roll(part[:, 256:384], 1, 0)
            )
            out_ref[y + j] = total[0:128].astype(jnp.bfloat16)


def call(kernel, shapes, scratch, in_specs, args, out_specs=None):
    return pl.pallas_call(
        kernel,
        out_shape=shapes,
        in_specs=in_specs,
        out_specs=jax.tree.map(lambda _: VMEM, shapes) if out_specs is None else out_specs,
        scratch_shapes=scratch,
        compiler_params=pltpu.CompilerParams(vmem_limit_bytes=40 * 1024 * 1024),
    )(*args)


def shape(dims, dtype):
    return jax.ShapeDtypeStruct(dims, dtype)


def shards(
    hidden_in, conv_weight, conv_bias, proj_weight, ocean_depth, sea_mask,
    step_alpha, step_beta, surface_cotangent,
):
    wide, narrow = jnp.float32, jnp.bfloat16
    rows = hidden_in.shape[1]
    hidden = hidden_in[0]
    n_x = lax.axis_size("lon")
    n_lat = lax.axis_size(LAT)
    n_all = lax.axis_size(("lat_0", "lat_2", "lon"))
    n_z = lax.axis_size(("lat_1", "dp"))
    lat, x = lax.axis_index(LAT), lax.axis_index("lon")
    at = jnp.stack(
        [lat % 2, lat, n_lat - 1 - lat, (x + n_x - 1) % n_x, (x + 1) % n_x]
    ).astype(jnp.int32)
    cross, pair, planes, sums = call(
        first_kernel,
        (
            shape((304, 128), narrow),
            shape((304, 128), narrow),
            shape((PLANES, rows, 128), wide),
            shape((n_lat, 1, 128), wide),
        ),
        [
            pltpu.VMEM((rows, 128), wide),
            pltpu.VMEM((rows, 128), jnp.int32),
            pltpu.VMEM((rows, 128), wide),
            pltpu.SemaphoreType.DMA((5,)),
        ],
        [SMEM] + [HBM] * 4,
        (at, hidden.reshape(rows * 128, 128), surface_cotangent, sea_mask, ocean_depth),
    )
    odd = [(i, (i + 1) % n_lat) for i in range(1, n_lat, 2)]
    cross = lax.ppermute(cross, LAT, odd + [(j, i) for i, j in odd])
    pair = lax.ppermute(pair, "lat_2", [(0, 1), (1, 0)])
    sums, pair = lax.optimization_barrier((sums, pair))
    sums = lax.all_to_all(sums, LAT, 0, 0, tiled=True)
    ends, fields, sent = call(
        second_kernel,
        (
            shape((4, 128, 128), narrow),
            shape((2, PACK, 128), wide),
            shape((n_x, SENT, 128), narrow),
        ),
        [],
        [SMEM] + [VMEM] * 5,
        (at, hidden, planes, sums, cross, pair),
    )
    got = lax.all_to_all(sent, "lon", 0, 0, tiled=True)
    grad, sent = call(
        main_kernel,
        (shape((rows + 2, WIDE, 128), narrow), shape((n_all, 40, 128), narrow)),
        [
            pltpu.VMEM((rows + 4, WIDE, 128), narrow),
            pltpu.VMEM((rows + 2, WIDE, 128), wide),
            pltpu.VMEM((384, 384), narrow),
            pltpu.VMEM((rows + 2, WIDE, 128), narrow),
            pltpu.VMEM((rows, WIDE, 384), narrow),
            pltpu.VMEM((9, 128, 128), wide),
            pltpu.SemaphoreType.DMA,
        ],
        [SMEM] + [VMEM] * 7 + [SMEM] * 2,
        (
            at, hidden, ends, fields, got, conv_weight, conv_bias[None], proj_weight[None],
            step_alpha, step_beta,
        ),
        (HBM, VMEM),
    )
    got = lax.all_to_all(sent, ("lat_0", "lat_2", "lon"), 0, 0, tiled=True)
    sent = call(middle_kernel, shape((n_z, 24, 128), narrow), [], [VMEM], (got,))
    got = lax.all_to_all(sent, ("lat_1", "dp"), 0, 0, tiled=True)
    grad_hidden = call(
        input_kernel,
        shape((rows, 128, 128), narrow),
        [pltpu.VMEM((384, 384), narrow)],
        [VMEM] * 2,
        (grad, conv_weight),
    )
    cells = rows * 128 * lax.axis_size("dp") * n_lat * n_x
    own_weight, total_bias, total_proj = call(
        functools.partial(last_kernel, 1.0 / math.sqrt(cells)),
        (shape((3, 3, 2, 128), wide), shape((1, 128), wide), shape((1, 128), wide)),
        [],
        [VMEM],
        (got,),
    )
    return grad_hidden[None], own_weight.transpose(2, 0, 1, 3), total_bias[0], total_proj[0]


def solution(mesh):
    split = Mesh(
        mesh.devices.reshape(mesh.shape["dp"], 4, 2, 2, mesh.shape["lon"]),
        ("dp", "lat_0", "lat_1", "lat_2", "lon"),
    )
    placed = (
        P("dp", LAT, "lon", None),
        P(),
        P(),
        P(),
        P(LAT, "lon"),
        P(LAT, "lon"),
        P(),
        P(),
        P("dp", LAT, "lon"),
    )
    return jax.shard_map(
        shards,
        mesh=split,
        in_specs=placed,
        out_specs=(P("dp", LAT, "lon", None), P(LAT_LON, None, None, None), P(), P()),
        check_vma=False,
    )
```

```python
import functools
import math

import jax
import jax.numpy as jnp
from jax import lax
from jax.experimental import pallas as pl
from jax.experimental.pallas import tpu as pltpu
from jax.sharding import Mesh
from jax.sharding import PartitionSpec as P

ITERS = 6
LAT_LON = ("lat_0", "lat_1", "lat_2", "lon")
LAT = ("lat_0", "lat_1", "lat_2")
WIDE = 144
PACK = 32
PLANES = 5
NEAR = 48

helm_coef = 0.5
VMEM = pl.BlockSpec(memory_space=pltpu.VMEM)
SMEM = pl.BlockSpec(memory_space=pltpu.SMEM)
HBM = pl.BlockSpec(memory_space=pltpu.HBM)


def rounded(values):
    return values.astype(jnp.bfloat16).astype(jnp.float32)


def pieces_of(values, count):
    out = []
    for _ in range(count):
        piece = rounded(values)
        out.append(piece)
        values = values - piece
    return out


def full(value):
    return jnp.full((1, 128), value, jnp.float32)


def packed(planes, shift):
    rows = planes[0].shape[0]
    lane = lax.broadcasted_iota(jnp.int32, (rows, 128), 1) // 8
    out = jnp.zeros((rows, 128), jnp.float32)
    for k, plane in enumerate(planes):
        by = (8 * k + shift) % 128
        out = jnp.where(lane == k, pltpu.roll(plane, by, 1) if by else plane, out)
    return out


def first_kernel(
    at_ref, hidden_ref, cot_ref, mask_ref, depth_ref,
    cross_ref, pair_ref, head_ref, tail_ref, near_ref, planes_ref, sums_ref,
):
    rows = hidden_ref.shape[0]
    upper = at_ref[0] == 0
    mask = mask_ref[...].astype(jnp.float32)
    wet = mask * cot_ref[0]
    planes = pieces_of(wet, 3) + pieces_of(mask * depth_ref[...], 2)
    summed, counted = full(jnp.sum(wet)), full(jnp.sum(mask))
    sums_ref[0:1] = summed
    sums_ref[1:2] = counted
    sums = pieces_of(summed, 3) + pieces_of(counted, 3)
    sums = jnp.concatenate(sums + [jnp.zeros((2, 128), jnp.float32)], axis=0)
    for k in range(PLANES):
        planes_ref[k] = planes[k]
    for ref, top in ((cross_ref, upper), (pair_ref, jnp.logical_not(upper))):
        start = jnp.where(top, 0, rows - 2)
        ref[0:256] = hidden_ref[pl.ds(start, 2)].reshape(256, 128)
        near = [jnp.where(top, p[0:8], p[rows - 8 : rows]) for p in planes] + [sums]
        for k in range(0, 6, 2):
            tile = jnp.concatenate(near[k : k + 2], axis=0)
            ref[256 + k * 8 : 272 + k * 8] = tile.astype(jnp.bfloat16)
    place = lax.broadcasted_iota(jnp.int32, (8, 128), 0)
    columns = [[jnp.zeros((8, 128), jnp.float32) for _ in range(2)] for _ in range(4)]
    for r in range(rows):
        head = hidden_ref[r, 0:16].astype(jnp.float32)
        tail = hidden_ref[r, 112:128].astype(jnp.float32)
        for k, row in enumerate((head[0:1], head[1:2], tail[14:15], tail[15:16])):
            columns[k][r // 8] = jnp.where(place == r % 8, row, columns[k][r // 8])
    ends = []
    for side, ref in ((0, head_ref), (1, tail_ref)):
        fields = packed(planes, 0 if side == 0 else 8)
        pair = columns[2 * side : 2 * side + 2]
        whole = jnp.concatenate([pair[0][0], pair[0][1], pair[1][0], pair[1][1], fields], axis=0)
        ends.append(whole)
        corner = jnp.zeros((8, 128), jnp.float32)
        for r in range(2):
            for k in range(2):
                row = jnp.where(upper, pair[k][0][r : r + 1], pair[k][1][6 + r : 7 + r])
                corner = jnp.where(place == 2 * r + k, row, corner)
        facing = jnp.where(upper, fields[0:8], fields[rows - 8 : rows])
        ref[...] = jnp.concatenate([corner, facing], axis=0).astype(jnp.bfloat16)
    n_x = near_ref.shape[0] // 2
    for peer in range(n_x):
        chosen = jnp.where(at_ref[4] == peer, ends[1], ends[0]).astype(jnp.bfloat16)
        near_ref[peer] = chosen
        near_ref[n_x + peer] = chosen


def sums_kernel(sums_ref, cross_ref, total_ref):
    got = cross_ref[288:304].astype(jnp.float32)[8:16]
    summed = sums_ref[0:1] + got[0:1] + got[1:2] + got[2:3]
    counted = sums_ref[1:2] + got[3:4] + got[4:5] + got[5:6]
    lane = lax.broadcasted_iota(jnp.int32, (1, 128), 1)
    total = jnp.where(lane < 64, summed, counted)
    total_ref[...] = jnp.broadcast_to(total[None], total_ref.shape)


def forward_kernel(
    at_ref, hidden_ref, planes_ref, cross_ref, pair_ref, head_ref, tail_ref, near_ref,
    weight_ref, bias_ref, alpha_ref, beta_ref,
    ext_ref, preact_ref, force_ref, rhs_ref,
):
    rows = hidden_ref.shape[0]
    n_x = near_ref.shape[0] // 2
    core, left, right = at_ref[0], at_ref[3], at_ref[4]
    upper = core == 0
    keep_above = jnp.where(at_ref[1] == 0, 0.0, 1.0)
    keep_below = jnp.where(at_ref[2] == 0, 0.0, 1.0)
    zero = jnp.zeros((), jnp.bfloat16)
    for k in range(2):
        cross = cross_ref[k * 128 : k * 128 + 128]
        pair = pair_ref[k * 128 : k * 128 + 128]
        ext_ref[k, 0:128] = jnp.where(keep_above > 0.0, jnp.where(upper, cross, pair), zero)
        ext_ref[k + rows + 2, 0:128] = jnp.where(
            keep_below > 0.0, jnp.where(upper, pair, cross), zero
        )
    ext_ref[2 : rows + 2, 0:128] = hidden_ref[...]

    place = lax.broadcasted_iota(jnp.int32, (WIDE - 128, 128), 0)
    tiles = [jnp.zeros((WIDE - 128, 128), jnp.float32) for _ in range(rows + 4)]
    second = []
    for side, base, corner_ref in ((right, 0, head_ref), (left, WIDE - 130, tail_ref)):
        own = near_ref[core * n_x + side].astype(jnp.float32)
        other = near_ref[(1 - core) * n_x + side].astype(jnp.float32)
        corner = corner_ref[...].astype(jnp.float32)
        for k in range(2):
            for r in range(rows + 4):
                if r < 2:
                    mate = other[k * 16 + rows - 2 + r : k * 16 + rows - 1 + r]
                    row = jnp.where(upper, corner[2 * r + k : 2 * r + k + 1], mate) * keep_above
                elif r < rows + 2:
                    row = own[k * 16 + r - 2 : k * 16 + r - 1]
                else:
                    j = r - rows - 2
                    mate = other[k * 16 + j : k * 16 + j + 1]
                    row = jnp.where(upper, mate, corner[2 * j + k : 2 * j + k + 1]) * keep_below
                tiles[r] = jnp.where(place == base + k, row, tiles[r])
        above = jnp.where(upper, corner[8:16], other[40:48]) * keep_above
        below = jnp.where(upper, other[32:40], corner[8:16]) * keep_below
        second.append(jnp.concatenate([above, own[32:48], below], axis=0))
    for r in range(rows + 4):
        ext_ref[r, 128:WIDE] = tiles[r].astype(jnp.bfloat16)
    from_right, from_left = second
    cross = cross_ref[256:304].astype(jnp.float32)
    pair = pair_ref[256:304].astype(jnp.float32)
    above = jnp.where(upper, cross, pair) * keep_above
    below = jnp.where(upper, pair, cross) * keep_below
    lane = lax.broadcasted_iota(jnp.int32, (2 * PACK, 128), 1)
    planes = []
    for k in range(PLANES):
        beyond = from_right if k == 0 else pltpu.roll(from_right, 128 - 8 * k, 1)
        before = pltpu.roll(from_left, 120 - 8 * k, 1)
        near = lane[:PACK]
        at = k * 8
        planes.append(
            jnp.concatenate(
                [
                    above[at : at + 8],
                    planes_ref[k],
                    below[at : at + 8],
                    jnp.where(near < 8, beyond, jnp.where(near >= 120, before, 0.0)),
                ],
                axis=0,
            )
        )
    start = planes[0] + planes[1] + planes[2]
    wet_depth = planes[3] + planes[4]
    for a in range(3):
        for c in range(3):
            rhs_ref[a * 128 : a * 128 + 128, c * 128 : c * 128 + 128] = weight_ref[a, c]

    mask = jnp.where(wet_depth > 0.0, 1.0, 0.0)

    def other_half(field):
        parts = [field[k * PACK : (k + 1) * PACK] for k in range(field.shape[0] // PACK)]
        swapped = []
        for k in range(0, len(parts), 2):
            swapped += [parts[k + 1], parts[k]]
        return jnp.concatenate(swapped, axis=0)

    def beside(field):
        count = field.shape[0]
        lanes = lane if count == 2 * PACK else jnp.concatenate([lane, lane], axis=0)
        up = pltpu.roll(field, 1, 0)
        down = pltpu.roll(field, count - 1, 0)
        from_left = pltpu.roll(field, 1, 1)
        from_left = jnp.where(lanes == 0, other_half(from_left), from_left)
        from_right = pltpu.roll(field, 127, 1)
        from_right = jnp.where(lanes == 127, other_half(from_right), from_right)
        return up, down, from_left, from_right

    weights = [
        0.5 * (near_mask * wet_depth + mask * near_depth)
        for near_mask, near_depth in zip(beside(mask), beside(wet_depth))
    ]
    diagonal = helm_coef * mask + weights[0] + weights[1] + weights[2] + weights[3]
    weights = [jnp.concatenate([w, w], axis=0) for w in weights]
    diagonal = jnp.concatenate([diagonal, diagonal], axis=0)
    residual = jnp.concatenate([start, mask], axis=0)
    direction = residual
    result = jnp.zeros_like(residual)
    for k in range(ITERS):
        result = result + alpha_ref[k] * direction
        if k + 1 < ITERS:
            applied = diagonal * direction
            for w, near in zip(weights, beside(direction)):
                applied = applied - w * near
            residual = residual - alpha_ref[k] * applied
            direction = residual + beta_ref[k] * direction
    result = result * jnp.concatenate([mask, mask], axis=0)
    force_ref[...] = result.T

    group = 6
    bias = bias_ref[...]
    for g in range(0, rows + 2, group):
        lhs = jnp.concatenate(
            [ext_ref[g + a : g + a + group].reshape(group * WIDE, 128) for a in range(3)], axis=1
        )
        out = jnp.dot(lhs, rhs_ref[...], preferred_element_type=jnp.float32)
        for j in range(group):
            part = out[j * WIDE : (j + 1) * WIDE]
            preact_ref[g + j] = (
                pltpu.roll(part[:, 0:128], 1, 0)
                + part[:, 128:256]
                + pltpu.roll(part[:, 256:384], WIDE - 1, 0)
                + bias
            )


def backward_kernel(
    total_ref, preact_ref, force_ref, ext_ref, proj_ref,
    grad_hbm, sent_ref,
    grad_ref, moved_ref, weight_ref, sem,
):
    rows = grad_ref.shape[0] - 2
    total = jnp.sum(total_ref[...], axis=0)
    mean = jnp.broadcast_to(total[:, 0:1], (1, 128)) / jnp.broadcast_to(total[:, 127:128], (1, 128))
    force = force_ref[...]
    force = force - mean * pltpu.roll(force, 64, 1)
    proj = proj_ref[...]
    sum_bias = jnp.zeros((8, 128), jnp.float32)
    sum_proj = jnp.zeros((8, 128), jnp.float32)
    for g in range(rows + 2):
        at = g + 7
        column = jnp.concatenate(
            [
                force[:, at : at + 1],
                force[0:8, PACK + at : PACK + at + 1],
                force[120:128, PACK + at : PACK + at + 1],
            ],
            axis=0,
        )
        column = jnp.broadcast_to(column, (WIDE, 128))
        preact = preact_ref[g]
        sigma = jax.nn.sigmoid(preact)
        active = preact * sigma
        slope_act = sigma * (1.0 + preact * (1.0 - sigma))
        grad = (column * proj * slope_act).astype(jnp.bfloat16)
        grad_ref[g] = grad
        if 1 <= g <= rows:
            own = grad.astype(jnp.float32)[0:128]
            for k in range(16):
                sum_bias = sum_bias + own[k * 8 : k * 8 + 8]
                sum_proj = sum_proj + (active * column)[k * 8 : k * 8 + 8]
            own = jnp.concatenate([own, jnp.zeros((WIDE - 128, 128), jnp.float32)], axis=0)
            moved_ref[g - 1, :, 0:128] = pltpu.roll(own, WIDE - 1, 0).astype(jnp.bfloat16)
            moved_ref[g - 1, :, 128:256] = own.astype(jnp.bfloat16)
            moved_ref[g - 1, :, 256:384] = pltpu.roll(own, 1, 0).astype(jnp.bfloat16)
    copy = pltpu.make_async_copy(grad_ref, grad_hbm, sem)
    copy.start()
    moved = moved_ref[...].reshape(rows * WIDE, 384)
    for a in range(3):
        cells = ext_ref[a + 1 : a + 1 + rows].reshape(rows * WIDE, 128)
        out = lax.dot_general(
            cells, moved, (((0,), (0,)), ((), ())), preferred_element_type=jnp.float32
        )
        for c in range(3):
            weight_ref[a * 3 + c] = out[:, c * 128 : c * 128 + 128]
    vectors = jnp.concatenate(
        [jnp.sum(sum_bias, axis=0, keepdims=True), jnp.sum(sum_proj, axis=0, keepdims=True)], axis=0
    )
    vectors = jnp.concatenate(pieces_of(vectors, 2) + [jnp.zeros((4, 128), jnp.float32)], axis=0)
    vectors = pltpu.roll(vectors, 4, 0)
    place = lax.broadcasted_iota(jnp.int32, (8, 128), 0) // 2

    def one_pair(at, carry):
        y, c = at // 2, at % 2
        for x in range(4):
            tiles = []
            for t in range(5):
                tile = vectors
                for j in range(4):
                    slot = 4 * t + j
                    if slot >= 18:
                        continue
                    z, k = slot // 9, slot % 9
                    start = pl.multiple_of(((y * 2 + z) * 2 + c) * 8, 8)
                    piece = weight_ref[k, pl.ds(start, 8)]
                    if j != x:
                        piece = pltpu.roll(piece, (2 * j - 2 * x) % 8, 0)
                    tile = jnp.where(place == j, piece, tile)
                tiles.append(tile)
            sent_ref[at * 4 + x] = jnp.concatenate(tiles, axis=0).astype(jnp.bfloat16)
        return carry

    lax.fori_loop(0, 8, one_pair, 0)
    copy.wait()


def middle_kernel(got_ref, sent_ref):
    total = jnp.sum(got_ref[...].astype(jnp.float32), axis=0)
    vectors = total[36:38] + total[38:40]
    vectors = jnp.concatenate(pieces_of(vectors, 2) + [jnp.zeros((2, 128), jnp.float32)], axis=0)
    peers = sent_ref.shape[0] // 2
    for z in range(2):
        block = jnp.concatenate([total[z * 18 : z * 18 + 18], vectors], axis=0)
        block = block.astype(jnp.bfloat16)
        for d in range(peers):
            sent_ref[z * peers + d] = block


def last_kernel(scale, got_ref, weight_ref, bias_ref, proj_ref):
    total = jnp.sum(got_ref[...].astype(jnp.float32), axis=0) * scale
    for k in range(9):
        weight_ref[k // 3, k % 3] = total[k * 2 : k * 2 + 2]
    bias_ref[...] = total[18:19] + total[20:21]
    proj_ref[...] = total[19:20] + total[21:22]


def input_kernel(grad_ref, weight_ref, out_ref, rhs_ref):
    rows = out_ref.shape[0]
    for a in range(3):
        for c in range(3):
            rhs_ref[c * 128 : c * 128 + 128, a * 128 : a * 128 + 128] = weight_ref[a, c]
    group = 4
    for y in range(0, rows, group):
        lhs = jnp.concatenate(
            [
                grad_ref[y - a + 2 : y - a + 2 + group].reshape(group * WIDE, 128)
                for a in range(3)
            ],
            axis=1,
        )
        out = lax.dot_general(
            lhs, rhs_ref[...], (((1,), (1,)), ((), ())), preferred_element_type=jnp.float32
        )
        for j in range(group):
            part = out[j * WIDE : (j + 1) * WIDE]
            total = (
                pltpu.roll(part[:, 0:128], WIDE - 1, 0)
                + part[:, 128:256]
                + pltpu.roll(part[:, 256:384], 1, 0)
            )
            out_ref[y + j] = total[0:128].astype(jnp.bfloat16)


def call(kernel, shapes, scratch, in_specs, args, out_specs=None):
    return pl.pallas_call(
        kernel,
        out_shape=shapes,
        in_specs=in_specs,
        out_specs=jax.tree.map(lambda _: VMEM, shapes) if out_specs is None else out_specs,
        scratch_shapes=scratch,
        compiler_params=pltpu.CompilerParams(vmem_limit_bytes=40 * 1024 * 1024),
    )(*args)


def shape(dims, dtype):
    return jax.ShapeDtypeStruct(dims, dtype)


def shards(
    hidden_in, conv_weight, conv_bias, proj_weight, ocean_depth, sea_mask,
    step_alpha, step_beta, surface_cotangent,
):
    wide, narrow = jnp.float32, jnp.bfloat16
    rows = hidden_in.shape[1]
    hidden = hidden_in[0]
    n_x = lax.axis_size("lon")
    n_lat = lax.axis_size(LAT)
    n_all = lax.axis_size(("lat_0", "lat_2", "lon"))
    n_z = lax.axis_size(("lat_1", "dp"))
    lat, me = lax.axis_index(LAT), lax.axis_index("lon")
    at = jnp.stack(
        [lat % 2, lat, n_lat - 1 - lat, (me + n_x - 1) % n_x, (me + 1) % n_x]
    ).astype(jnp.int32)
    cross, pair, head, tail, near, planes, sums = call(
        first_kernel,
        (
            shape((304, 128), narrow),
            shape((304, 128), narrow),
            shape((16, 128), narrow),
            shape((16, 128), narrow),
            shape((2 * n_x, NEAR, 128), narrow),
            shape((PLANES, rows, 128), wide),
            shape((2, 128), wide),
        ),
        [],
        [SMEM] + [VMEM] * 4,
        (at, hidden, surface_cotangent, sea_mask, ocean_depth),
    )
    odd = [(i, (i + 1) % n_lat) for i in range(1, n_lat, 2)]
    odd = odd + [(j, i) for i, j in odd]

    def corner(step):
        return [(i * n_x + x, j * n_x + (x + step) % n_x) for i, j in odd for x in range(n_x)]

    cross = lax.ppermute(cross, LAT, odd)
    head = lax.ppermute(head, LAT_LON, corner(n_x - 1))
    tail = lax.ppermute(tail, LAT_LON, corner(1))
    pair = lax.ppermute(pair, "lat_2", [(0, 1), (1, 0)])
    near = lax.all_to_all(near, ("lat_2", "lon"), 0, 0, tiled=True)
    total = call(sums_kernel, shape((n_all, 1, 128), wide), [], [VMEM] * 2, (sums, cross))
    total = lax.all_to_all(total, ("lat_0", "lat_2", "lon"), 0, 0, tiled=True)
    ext, preact, force = call(
        forward_kernel,
        (
            shape((rows + 4, WIDE, 128), narrow),
            shape((rows + 2, WIDE, 128), wide),
            shape((128, 128), wide),
        ),
        [pltpu.VMEM((384, 384), narrow)],
        [SMEM] + [VMEM] * 9 + [SMEM] * 2,
        (
            at, hidden, planes, cross, pair, head, tail, near, conv_weight,
            conv_bias[None], step_alpha, step_beta,
        ),
    )
    grad, sent = call(
        backward_kernel,
        (shape((rows + 2, WIDE, 128), narrow), shape((n_all, 40, 128), narrow)),
        [
            pltpu.VMEM((rows + 2, WIDE, 128), narrow),
            pltpu.VMEM((rows, WIDE, 384), narrow),
            pltpu.VMEM((9, 128, 128), wide),
            pltpu.SemaphoreType.DMA,
        ],
        [VMEM] * 5,
        (total, preact, force, ext, proj_weight[None]),
        (HBM, VMEM),
    )
    got = lax.all_to_all(sent, ("lat_0", "lat_2", "lon"), 0, 0, tiled=True)
    sent = call(middle_kernel, shape((n_z, 24, 128), narrow), [], [VMEM], (got,))
    got = lax.all_to_all(sent, ("lat_1", "dp"), 0, 0, tiled=True)
    grad_hidden = call(
        input_kernel,
        shape((rows, 128, 128), narrow),
        [pltpu.VMEM((384, 384), narrow)],
        [VMEM] * 2,
        (grad, conv_weight),
    )
    cells = rows * 128 * lax.axis_size("dp") * n_lat * n_x
    own_weight, total_bias, total_proj = call(
        functools.partial(last_kernel, 1.0 / math.sqrt(cells)),
        (shape((3, 3, 2, 128), wide), shape((1, 128), wide), shape((1, 128), wide)),
        [],
        [VMEM],
        (got,),
    )
    return grad_hidden[None], own_weight.transpose(2, 0, 1, 3), total_bias[0], total_proj[0]


def solution(mesh):
    split = Mesh(
        mesh.devices.reshape(mesh.shape["dp"], 4, 2, 2, mesh.shape["lon"]),
        ("dp", "lat_0", "lat_1", "lat_2", "lon"),
    )
    placed = (
        P("dp", LAT, "lon", None),
        P(),
        P(),
        P(),
        P(LAT, "lon"),
        P(LAT, "lon"),
        P(),
        P(),
        P("dp", LAT, "lon"),
    )
    return jax.shard_map(
        shards,
        mesh=split,
        in_specs=placed,
        out_specs=(P("dp", LAT, "lon", None), P(LAT_LON, None, None, None), P(), P()),
        check_vma=False,
    )
```

```python
import functools
import math

import jax
import jax.numpy as jnp
from jax import lax
from jax.experimental import pallas as pl
from jax.experimental.pallas import tpu as pltpu
from jax.sharding import Mesh
from jax.sharding import PartitionSpec as P

ITERS = 6
LAT_LON = ("lat_0", "lat_1", "lat_2", "lon")
LAT = ("lat_0", "lat_1", "lat_2")
WIDE = 144
PACK = 32
PLANES = 5
NEAR = 48

helm_coef = 0.5
VMEM = pl.BlockSpec(memory_space=pltpu.VMEM)
SMEM = pl.BlockSpec(memory_space=pltpu.SMEM)
HBM = pl.BlockSpec(memory_space=pltpu.HBM)


def rounded(values):
    return values.astype(jnp.bfloat16).astype(jnp.float32)


def pieces_of(values, count):
    out = []
    for _ in range(count):
        piece = rounded(values)
        out.append(piece)
        values = values - piece
    return out


def full(value):
    return jnp.full((1, 128), value, jnp.float32)


def packed(planes, shift):
    rows = planes[0].shape[0]
    lane = lax.broadcasted_iota(jnp.int32, (rows, 128), 1) // 8
    out = jnp.zeros((rows, 128), jnp.float32)
    for k, plane in enumerate(planes):
        by = (8 * k + shift) % 128
        out = jnp.where(lane == k, pltpu.roll(plane, by, 1) if by else plane, out)
    return out


def edge_columns(load, rows):
    place = lax.broadcasted_iota(jnp.int32, (8, 128), 0)
    columns = [[jnp.zeros((8, 128), jnp.float32) for _ in range(rows // 8)] for _ in range(4)]
    for r in range(rows):
        head = load(r, 0).astype(jnp.float32)
        tail = load(r, 112).astype(jnp.float32)
        for k, row in enumerate((head[0:1], head[1:2], tail[14:15], tail[15:16])):
            columns[k][r // 8] = jnp.where(place == r % 8, row, columns[k][r // 8])
    return columns


def first_kernel(
    at_ref, hidden_ref, fields_ref, cross_ref, pair_ref, near_ref, planes_ref, sums_ref
):
    rows = hidden_ref.shape[0]
    upper = at_ref[0] == 0
    wet, wet_depth = fields_ref[0], fields_ref[1]
    planes = pieces_of(wet, 3) + pieces_of(wet_depth, 2)
    summed = full(jnp.sum(wet))
    counted = full(jnp.sum(jnp.where(wet_depth > 0.0, 1.0, 0.0)))
    sums_ref[0:1] = summed
    sums_ref[1:2] = counted
    sums = pieces_of(summed, 3) + pieces_of(counted, 3)
    sums = jnp.concatenate(sums + [jnp.zeros((2, 128), jnp.float32)], axis=0)
    for k in range(PLANES):
        planes_ref[k] = planes[k]
    for ref, top in ((cross_ref, upper), (pair_ref, jnp.logical_not(upper))):
        start = jnp.where(top, 0, rows - 2)
        ref[0:256] = hidden_ref[pl.ds(start, 2)].reshape(256, 128)
        near = [jnp.where(top, p[0:8], p[rows - 8 : rows]) for p in planes] + [sums]
        for k in range(0, 6, 2):
            tile = jnp.concatenate(near[k : k + 2], axis=0)
            ref[256 + k * 8 : 272 + k * 8] = tile.astype(jnp.bfloat16)
    columns = edge_columns(lambda r, at: hidden_ref[r, at : at + 16], rows)
    head = jnp.concatenate(columns[0] + columns[1] + [packed(planes, 0)], axis=0)
    tail = jnp.concatenate(columns[2] + columns[3] + [packed(planes, 8)], axis=0)
    n_x = near_ref.shape[0] // 2
    for peer in range(n_x):
        chosen = jnp.where(at_ref[4] == peer, tail, head).astype(jnp.bfloat16)
        near_ref[peer] = chosen
        near_ref[n_x + peer] = chosen


def second_kernel(at_ref, sums_ref, cross_ref, sent_ref):
    tiles = [cross_ref[256 + k * 16 : 272 + k * 16].astype(jnp.float32) for k in range(3)]
    planes = [tiles[k // 2][k % 2 * 8 : k % 2 * 8 + 8] for k in range(PLANES)]
    got = tiles[2][8:16]
    summed = sums_ref[0:1] + got[0:1] + got[1:2] + got[2:3]
    counted = sums_ref[1:2] + got[3:4] + got[4:5] + got[5:6]
    sums = pieces_of(summed, 3) + pieces_of(counted, 3)
    sums = jnp.concatenate(sums + [jnp.zeros((2, 128), jnp.float32)], axis=0)
    place = lax.broadcasted_iota(jnp.int32, (8, 128), 0)
    blocks = []
    for side in range(2):
        corner = jnp.zeros((8, 128), jnp.float32)
        for r in range(2):
            start = r * 128 + 112 * side
            tile = cross_ref[start : start + 16].astype(jnp.float32)
            for k in range(2):
                at = 14 * side + k
                corner = jnp.where(place == 2 * r + k, tile[at : at + 1], corner)
        block = jnp.concatenate([corner, packed(planes, 8 * side), sums], axis=0)
        blocks.append(block)
    n_x = 4
    for peer in range(n_x):
        chosen = jnp.where(at_ref[4] == peer, blocks[1], blocks[0]).astype(jnp.bfloat16)
        for group in range(sent_ref.shape[0] // n_x):
            sent_ref[group * n_x + peer] = chosen


def sides_of(at_ref):
    return (
        at_ref[0] == 0,
        jnp.where(at_ref[1] == 0, 0.0, 1.0),
        jnp.where(at_ref[2] == 0, 0.0, 1.0),
    )


def fill(rhs_ref, weight_ref):
    for a in range(3):
        for c in range(3):
            rhs_ref[a * 128 : a * 128 + 128, c * 128 : c * 128 + 128] = weight_ref[a, c]


def convolved(ext_ref, rhs_ref, bias, start, group):
    lhs = jnp.concatenate(
        [ext_ref[pl.ds(start + a, group)].reshape(group * WIDE, 128) for a in range(3)], axis=1
    )
    out = jnp.dot(lhs, rhs_ref[...], preferred_element_type=jnp.float32)
    rows = []
    for j in range(group):
        part = out[j * WIDE : (j + 1) * WIDE]
        rows.append(
            pltpu.roll(part[:, 0:128], 1, 0)
            + part[:, 128:256]
            + pltpu.roll(part[:, 256:384], WIDE - 1, 0)
            + bias
        )
    return rows


def forward_kernel(
    at_ref, hidden_ref, cross_ref, pair_ref, near_ref, weight_ref, bias_ref, proj_ref,
    alpha_ref, beta_ref,
    ext_ref, preact_ref, params_ref, rhs_ref,
):
    rows = hidden_ref.shape[0]
    n_x = near_ref.shape[0] // 2
    core, left, right = at_ref[0], at_ref[3], at_ref[4]
    upper, keep_above, keep_below = sides_of(at_ref)
    zero = jnp.zeros((), jnp.bfloat16)
    for k in range(2):
        cross = cross_ref[k * 128 : k * 128 + 128]
        pair = pair_ref[k * 128 : k * 128 + 128]
        ext_ref[k, 0:128] = jnp.where(keep_above > 0.0, jnp.where(upper, cross, pair), zero)
        ext_ref[k + rows + 2, 0:128] = jnp.where(
            keep_below > 0.0, jnp.where(upper, pair, cross), zero
        )
    ext_ref[2 : rows + 2, 0:128] = hidden_ref[...]
    place = lax.broadcasted_iota(jnp.int32, (WIDE - 128, 128), 0)
    tiles = [jnp.zeros((WIDE - 128, 128), jnp.float32) for _ in range(rows + 4)]
    for side, base in ((right, 0), (left, WIDE - 130)):
        own = near_ref[core * n_x + side].astype(jnp.float32)
        other = near_ref[(1 - core) * n_x + side].astype(jnp.float32)
        for k in range(2):
            for r in range(rows + 4):
                at = r - 2
                source = own
                if r < 2:
                    source, at = other, rows - 2 + r
                elif r >= rows + 2:
                    source, at = other, r - rows - 2
                row = source[k * 16 + at : k * 16 + at + 1]
                tiles[r] = jnp.where(place == base + k, row, tiles[r])
    for r in range(rows + 4):
        ext_ref[r, 128:WIDE] = tiles[r].astype(jnp.bfloat16)
    fill(rhs_ref, weight_ref)
    bias = bias_ref[...]
    params_ref[0:1] = bias
    params_ref[1:2] = proj_ref[...]
    for k in range(ITERS):
        params_ref[2 + k : 3 + k] = full(alpha_ref[k])
        params_ref[8 + k : 9 + k] = full(beta_ref[k])
    group = 6
    for g in range(0, rows + 2, group):
        for j, row in enumerate(convolved(ext_ref, rhs_ref, bias, g, group)):
            preact_ref[g + j] = row


def backward_kernel(
    at_ref, planes_ref, cross_ref, pair_ref, near_ref, got_ref, kernel_ref, params_ref,
    preact_ref, early_ref,
    grad_hbm, sent_ref, ext_ref,
    grad_ref, moved_ref, weight_ref, rhs_ref, sem,
):
    rows = grad_ref.shape[0] - 2
    n_x = near_ref.shape[0] // 2
    core, left, right = at_ref[0], at_ref[3], at_ref[4]
    upper, keep_above, keep_below = sides_of(at_ref)
    keep_cross = jnp.where(upper, keep_above, keep_below)
    place = lax.broadcasted_iota(jnp.int32, (WIDE - 128, 128), 0)
    tiles = [jnp.zeros((WIDE - 128, 128), jnp.float32) for _ in range(2)]
    second = []
    for side, base in ((right, 0), (left, WIDE - 130)):
        own = near_ref[core * n_x + side, 32:48].astype(jnp.float32)
        other = near_ref[(1 - core) * n_x + side, 32:48].astype(jnp.float32)
        corner = got_ref[at_ref[5] * n_x + side].astype(jnp.float32)[0:16] * keep_cross
        for r in range(2):
            for k in range(2):
                row = corner[2 * r + k : 2 * r + k + 1]
                tiles[r] = jnp.where(place == base + k, row, tiles[r])
        above = jnp.where(upper, corner[8:16], other[8:16] * keep_above)
        below = jnp.where(upper, other[0:8] * keep_below, corner[8:16])
        second.append(jnp.concatenate([above, own, below], axis=0))
    from_right, from_left = second
    crossed = jnp.where(upper, 0, rows + 2)
    paired = rows + 2 - crossed
    for r in range(2):
        ext_ref[crossed + r, 128:WIDE] = tiles[r].astype(jnp.bfloat16)
        keep = jnp.where(upper, keep_below, keep_above) > 0.0
        mate = ext_ref[paired + r, 128:WIDE]
        ext_ref[paired + r, 128:WIDE] = jnp.where(keep, mate, jnp.zeros((), jnp.bfloat16))
    fill(rhs_ref, kernel_ref)
    again = jnp.where(upper, 0, rows)
    fixed = convolved(ext_ref, rhs_ref, params_ref[0:1], again, 2)
    cross = cross_ref[256:304].astype(jnp.float32)
    pair = pair_ref[256:304].astype(jnp.float32)
    above = jnp.where(upper, cross, pair) * keep_above
    below = jnp.where(upper, pair, cross) * keep_below
    lane = lax.broadcasted_iota(jnp.int32, (2 * PACK, 128), 1)
    planes = []
    for k in range(PLANES):
        beyond = from_right if k == 0 else pltpu.roll(from_right, 128 - 8 * k, 1)
        before = pltpu.roll(from_left, 120 - 8 * k, 1)
        near = lane[:PACK]
        at = k * 8
        planes.append(
            jnp.concatenate(
                [
                    above[at : at + 8],
                    planes_ref[k],
                    below[at : at + 8],
                    jnp.where(near < 8, beyond, jnp.where(near >= 120, before, 0.0)),
                ],
                axis=0,
            )
        )
    start = planes[0] + planes[1] + planes[2]
    wet_depth = planes[3] + planes[4]
    mask = jnp.where(wet_depth > 0.0, 1.0, 0.0)

    def other_half(field):
        parts = [field[k * PACK : (k + 1) * PACK] for k in range(field.shape[0] // PACK)]
        swapped = []
        for k in range(0, len(parts), 2):
            swapped += [parts[k + 1], parts[k]]
        return jnp.concatenate(swapped, axis=0)

    def beside(field):
        count = field.shape[0]
        lanes = lane if count == 2 * PACK else jnp.concatenate([lane, lane], axis=0)
        up = pltpu.roll(field, 1, 0)
        down = pltpu.roll(field, count - 1, 0)
        from_left = pltpu.roll(field, 1, 1)
        from_left = jnp.where(lanes == 0, other_half(from_left), from_left)
        from_right = pltpu.roll(field, 127, 1)
        from_right = jnp.where(lanes == 127, other_half(from_right), from_right)
        return up, down, from_left, from_right

    weights = [
        0.5 * (near_mask * wet_depth + mask * near_depth)
        for near_mask, near_depth in zip(beside(mask), beside(wet_depth))
    ]
    diagonal = helm_coef * mask + weights[0] + weights[1] + weights[2] + weights[3]
    weights = [jnp.concatenate([w, w], axis=0) for w in weights]
    diagonal = jnp.concatenate([diagonal, diagonal], axis=0)
    residual = jnp.concatenate([start, mask], axis=0)
    direction = residual
    result = jnp.zeros_like(residual)
    for k in range(ITERS):
        result = result + params_ref[2 + k : 3 + k] * direction
        if k + 1 < ITERS:
            applied = diagonal * direction
            for w, near in zip(weights, beside(direction)):
                applied = applied - w * near
            residual = residual - params_ref[2 + k : 3 + k] * applied
            direction = residual + params_ref[8 + k : 9 + k] * direction
    result = result * jnp.concatenate([mask, mask], axis=0)
    sums = jnp.sum(got_ref[:, 16:24].astype(jnp.float32), axis=0)
    mean = (sums[0:1] + sums[1:2] + sums[2:3]) / (sums[3:4] + sums[4:5] + sums[5:6])
    force = result.T
    force = force - mean * pltpu.roll(force, 64, 1)
    proj = params_ref[1:2]
    sum_bias = jnp.zeros((8, 128), jnp.float32)
    sum_proj = jnp.zeros((8, 128), jnp.float32)
    for g in range(rows + 2):
        at = g + 7
        column = jnp.concatenate(
            [
                force[:, at : at + 1],
                force[0:8, PACK + at : PACK + at + 1],
                force[120:128, PACK + at : PACK + at + 1],
            ],
            axis=0,
        )
        column = jnp.broadcast_to(column, (WIDE, 128))
        preact = preact_ref[g]
        if g < 2:
            preact = jnp.where(upper, fixed[g], preact)
        elif g >= rows:
            preact = jnp.where(upper, preact, fixed[g - rows])
        sigma = jax.nn.sigmoid(preact)
        active = preact * sigma
        slope_act = sigma * (1.0 + preact * (1.0 - sigma))
        grad = (column * proj * slope_act).astype(jnp.bfloat16)
        grad_ref[g] = grad
        if 1 <= g <= rows:
            own = grad.astype(jnp.float32)[0:128]
            for k in range(16):
                sum_bias = sum_bias + own[k * 8 : k * 8 + 8]
                sum_proj = sum_proj + (active * column)[k * 8 : k * 8 + 8]
            own = jnp.concatenate([own, jnp.zeros((WIDE - 128, 128), jnp.float32)], axis=0)
            moved_ref[g - 1, :, 0:128] = pltpu.roll(own, WIDE - 1, 0).astype(jnp.bfloat16)
            moved_ref[g - 1, :, 128:256] = own.astype(jnp.bfloat16)
            moved_ref[g - 1, :, 256:384] = pltpu.roll(own, 1, 0).astype(jnp.bfloat16)
    copy = pltpu.make_async_copy(grad_ref, grad_hbm, sem)
    copy.start()
    moved = moved_ref[...].reshape(rows * WIDE, 384)
    for a in range(3):
        cells = ext_ref[a + 1 : a + 1 + rows].reshape(rows * WIDE, 128)
        out = lax.dot_general(
            cells, moved, (((0,), (0,)), ((), ())), preferred_element_type=jnp.float32
        )
        for c in range(3):
            weight_ref[a * 3 + c] = out[:, c * 128 : c * 128 + 128]
    vectors = jnp.concatenate(
        [jnp.sum(sum_bias, axis=0, keepdims=True), jnp.sum(sum_proj, axis=0, keepdims=True)], axis=0
    )
    vectors = jnp.concatenate(pieces_of(vectors, 2) + [jnp.zeros((4, 128), jnp.float32)], axis=0)
    vectors = pltpu.roll(vectors, 4, 0)
    place = lax.broadcasted_iota(jnp.int32, (8, 128), 0) // 2

    def one_pair(at, carry):
        y, c = at // 2, at % 2
        for x in range(4):
            tiles = []
            for t in range(5):
                tile = vectors
                for j in range(4):
                    slot = 4 * t + j
                    if slot >= 18:
                        continue
                    z, k = slot // 9, slot % 9
                    start = pl.multiple_of(((y * 2 + z) * 2 + c) * 8, 8)
                    piece = weight_ref[k, pl.ds(start, 8)]
                    if j != x:
                        piece = pltpu.roll(piece, (2 * j - 2 * x) % 8, 0)
                    tile = jnp.where(place == j, piece, tile)
                tiles.append(tile)
            sent_ref[at * 4 + x] = jnp.concatenate(tiles, axis=0).astype(jnp.bfloat16)
        return carry

    lax.fori_loop(0, 8, one_pair, 0)
    copy.wait()


def middle_kernel(got_ref, sent_ref):
    total = jnp.sum(got_ref[...].astype(jnp.float32), axis=0)
    vectors = total[36:38] + total[38:40]
    vectors = jnp.concatenate(pieces_of(vectors, 2) + [jnp.zeros((2, 128), jnp.float32)], axis=0)
    peers = sent_ref.shape[0] // 2
    for z in range(2):
        block = jnp.concatenate([total[z * 18 : z * 18 + 18], vectors], axis=0)
        block = block.astype(jnp.bfloat16)
        for d in range(peers):
            sent_ref[z * peers + d] = block


def last_kernel(scale, got_ref, weight_ref, bias_ref, proj_ref):
    total = jnp.sum(got_ref[...].astype(jnp.float32), axis=0) * scale
    for k in range(9):
        weight_ref[k // 3, k % 3] = total[k * 2 : k * 2 + 2]
    bias_ref[...] = total[18:19] + total[20:21]
    proj_ref[...] = total[19:20] + total[21:22]


def input_kernel(grad_ref, weight_ref, out_ref, rhs_ref):
    rows = out_ref.shape[0]
    for a in range(3):
        for c in range(3):
            rhs_ref[c * 128 : c * 128 + 128, a * 128 : a * 128 + 128] = weight_ref[a, c]
    group = 4
    for y in range(0, rows, group):
        lhs = jnp.concatenate(
            [
                grad_ref[y - a + 2 : y - a + 2 + group].reshape(group * WIDE, 128)
                for a in range(3)
            ],
            axis=1,
        )
        out = lax.dot_general(
            lhs, rhs_ref[...], (((1,), (1,)), ((), ())), preferred_element_type=jnp.float32
        )
        for j in range(group):
            part = out[j * WIDE : (j + 1) * WIDE]
            total = (
                pltpu.roll(part[:, 0:128], WIDE - 1, 0)
                + part[:, 128:256]
                + pltpu.roll(part[:, 256:384], 1, 0)
            )
            out_ref[y + j] = total[0:128].astype(jnp.bfloat16)


def call(kernel, shapes, scratch, in_specs, args, out_specs=None, aliases={}):
    return pl.pallas_call(
        kernel,
        out_shape=shapes,
        in_specs=in_specs,
        out_specs=jax.tree.map(lambda _: VMEM, shapes) if out_specs is None else out_specs,
        scratch_shapes=scratch,
        input_output_aliases=aliases,
        compiler_params=pltpu.CompilerParams(vmem_limit_bytes=40 * 1024 * 1024),
    )(*args)


def shape(dims, dtype):
    return jax.ShapeDtypeStruct(dims, dtype)


def shards(
    hidden_in, conv_weight, conv_bias, proj_weight, ocean_depth, sea_mask,
    step_alpha, step_beta, surface_cotangent,
):
    wide, narrow = jnp.float32, jnp.bfloat16
    rows = hidden_in.shape[1]
    hidden = hidden_in[0]
    n_x = lax.axis_size("lon")
    n_lat = lax.axis_size(LAT)
    n_all = lax.axis_size(("lat_0", "lat_2", "lon"))
    n_z = lax.axis_size(("lat_1", "dp"))
    lat, me = lax.axis_index(LAT), lax.axis_index("lon")
    row_group = lax.axis_index(("lat_0", "lat_2"))
    at = jnp.stack(
        [lat % 2, lat, n_lat - 1 - lat, (me + n_x - 1) % n_x, (me + 1) % n_x, row_group]
    ).astype(jnp.int32)
    mask = sea_mask.astype(wide)
    fields = jnp.stack([mask * surface_cotangent[0], mask * ocean_depth])
    cross, pair, near, planes, sums = call(
        first_kernel,
        (
            shape((304, 128), narrow),
            shape((304, 128), narrow),
            shape((2 * n_x, NEAR, 128), narrow),
            shape((PLANES, rows, 128), wide),
            shape((2, 128), wide),
        ),
        [],
        [SMEM] + [VMEM] * 2,
        (at, hidden, fields),
    )
    odd = [(i, (i + 1) % n_lat) for i in range(1, n_lat, 2)]
    odd = odd + [(j, i) for i, j in odd]
    cross = lax.ppermute(cross, LAT, odd)
    pair = lax.ppermute(pair, "lat_2", [(0, 1), (1, 0)])
    near = lax.all_to_all(near, ("lat_2", "lon"), 0, 0, tiled=True)
    sent = call(
        second_kernel, shape((n_all, 24, 128), narrow), [], [SMEM] + [VMEM] * 2, (at, sums, cross)
    )
    got = lax.all_to_all(sent, ("lat_0", "lat_2", "lon"), 0, 0, tiled=True)
    early, preact, params = call(
        forward_kernel,
        (
            shape((rows + 4, WIDE, 128), narrow),
            shape((rows + 2, WIDE, 128), wide),
            shape((16, 128), wide),
        ),
        [pltpu.VMEM((384, 384), narrow)],
        [SMEM] + [VMEM] * 7 + [SMEM] * 2,
        (
            at, hidden, cross, pair, near, conv_weight, conv_bias[None],
            proj_weight[None], step_alpha, step_beta,
        ),
    )
    grad, sent, _ = call(
        backward_kernel,
        (
            shape((rows + 2, WIDE, 128), narrow),
            shape((n_all, 40, 128), narrow),
            shape((rows + 4, WIDE, 128), narrow),
        ),
        [
            pltpu.VMEM((rows + 2, WIDE, 128), narrow),
            pltpu.VMEM((rows, WIDE, 384), narrow),
            pltpu.VMEM((9, 128, 128), wide),
            pltpu.VMEM((384, 384), narrow),
            pltpu.SemaphoreType.DMA,
        ],
        [SMEM] + [VMEM] * 9,
        (at, planes, cross, pair, near, got, conv_weight, params, preact, early),
        (HBM, VMEM, VMEM),
        {9: 2},
    )
    got = lax.all_to_all(sent, ("lat_0", "lat_2", "lon"), 0, 0, tiled=True)
    sent = call(middle_kernel, shape((n_z, 24, 128), narrow), [], [VMEM], (got,))
    got = lax.all_to_all(sent, ("lat_1", "dp"), 0, 0, tiled=True)
    grad_hidden = call(
        input_kernel,
        shape((rows, 128, 128), narrow),
        [pltpu.VMEM((384, 384), narrow)],
        [VMEM] * 2,
        (grad, conv_weight),
    )
    cells = rows * 128 * lax.axis_size("dp") * n_lat * n_x
    own_weight, total_bias, total_proj = call(
        functools.partial(last_kernel, 1.0 / math.sqrt(cells)),
        (shape((3, 3, 2, 128), wide), shape((1, 128), wide), shape((1, 128), wide)),
        [],
        [VMEM],
        (got,),
    )
    return grad_hidden[None], own_weight.transpose(2, 0, 1, 3), total_bias[0], total_proj[0]


def solution(mesh):
    split = Mesh(
        mesh.devices.reshape(mesh.shape["dp"], 4, 2, 2, mesh.shape["lon"]),
        ("dp", "lat_0", "lat_1", "lat_2", "lon"),
    )
    placed = (
        P("dp", LAT, "lon", None),
        P(),
        P(),
        P(),
        P(LAT, "lon"),
        P(LAT, "lon"),
        P(),
        P(),
        P("dp", LAT, "lon"),
    )
    return jax.shard_map(
        shards,
        mesh=split,
        in_specs=placed,
        out_specs=(P("dp", LAT, "lon", None), P(LAT_LON, None, None, None), P(), P()),
        check_vma=False,
    )
```

```python
import functools
import math

import jax
import jax.numpy as jnp
from jax import lax
from jax.experimental import pallas as pl
from jax.experimental.pallas import tpu as pltpu
from jax.sharding import Mesh
from jax.sharding import PartitionSpec as P

ITERS = 6
LAT_LON = ("lat_0", "lat_1", "lat_2", "lon")
LAT = ("lat_0", "lat_1", "lat_2")
WIDE = 144
PACK = 32
PLANES = 5
NEAR = 48

helm_coef = 0.5
VMEM = pl.BlockSpec(memory_space=pltpu.VMEM)
SMEM = pl.BlockSpec(memory_space=pltpu.SMEM)
HBM = pl.BlockSpec(memory_space=pltpu.HBM)


def rounded(values):
    return values.astype(jnp.bfloat16).astype(jnp.float32)


def pieces_of(values, count):
    out = []
    for _ in range(count):
        piece = rounded(values)
        out.append(piece)
        values = values - piece
    return out


def full(value):
    return jnp.full((1, 128), value, jnp.float32)


def packed(planes, shift):
    rows = planes[0].shape[0]
    lane = lax.broadcasted_iota(jnp.int32, (rows, 128), 1) // 8
    out = jnp.zeros((rows, 128), jnp.float32)
    for k, plane in enumerate(planes):
        by = (8 * k + shift) % 128
        out = jnp.where(lane == k, pltpu.roll(plane, by, 1) if by else plane, out)
    return out


def edge_columns(load, rows):
    place = lax.broadcasted_iota(jnp.int32, (8, 128), 0)
    columns = [[jnp.zeros((8, 128), jnp.float32) for _ in range(rows // 8)] for _ in range(4)]
    for r in range(rows):
        head = load(r, 0).astype(jnp.float32)
        tail = load(r, 112).astype(jnp.float32)
        for k, row in enumerate((head[0:1], head[1:2], tail[14:15], tail[15:16])):
            columns[k][r // 8] = jnp.where(place == r % 8, row, columns[k][r // 8])
    return columns


def unpacked(beyond, before, k):
    near = lax.broadcasted_iota(jnp.int32, beyond.shape, 1)
    if k:
        beyond = pltpu.roll(beyond, 128 - 8 * k, 1)
    before = pltpu.roll(before, 120 - 8 * k, 1)
    return jnp.where(near < 8, beyond, jnp.where(near >= 120, before, 0.0))


def first_kernel(
    at_ref, hidden_ref, fields_ref, cross_ref, pair_ref, near_ref, planes_ref, sums_ref
):
    rows = hidden_ref.shape[0]
    upper = at_ref[0] == 0
    wet, wet_depth = fields_ref[0], fields_ref[1]
    planes = pieces_of(wet, 3) + pieces_of(wet_depth, 2)
    summed = full(jnp.sum(wet))
    counted = full(jnp.sum(jnp.where(wet_depth > 0.0, 1.0, 0.0)))
    sums_ref[0:1] = summed
    sums_ref[1:2] = counted
    sums = pieces_of(summed, 3) + pieces_of(counted, 3)
    sums = jnp.concatenate(sums + [jnp.zeros((2, 128), jnp.float32)], axis=0)
    for k in range(PLANES):
        planes_ref[k] = planes[k]
    for ref, top in ((cross_ref, upper), (pair_ref, jnp.logical_not(upper))):
        start = jnp.where(top, 0, rows - 2)
        ref[0:256] = hidden_ref[pl.ds(start, 2)].reshape(256, 128)
        near = [jnp.where(top, p[0:8], p[rows - 8 : rows]) for p in planes] + [sums]
        for k in range(0, 6, 2):
            tile = jnp.concatenate(near[k : k + 2], axis=0)
            ref[256 + k * 8 : 272 + k * 8] = tile.astype(jnp.bfloat16)
    columns = edge_columns(lambda r, at: hidden_ref[r, at : at + 16], rows)
    head = jnp.concatenate(columns[0] + columns[1] + [packed(planes, 0)], axis=0)
    tail = jnp.concatenate(columns[2] + columns[3] + [packed(planes, 8)], axis=0)
    n_x = near_ref.shape[0] // 2
    for peer in range(n_x):
        chosen = jnp.where(at_ref[4] == peer, tail, head).astype(jnp.bfloat16)
        near_ref[peer] = chosen
        near_ref[n_x + peer] = chosen


def second_kernel(at_ref, sums_ref, cross_ref, sent_ref):
    tiles = [cross_ref[256 + k * 16 : 272 + k * 16].astype(jnp.float32) for k in range(3)]
    planes = [tiles[k // 2][k % 2 * 8 : k % 2 * 8 + 8] for k in range(PLANES)]
    got = tiles[2][8:16]
    summed = sums_ref[0:1] + got[0:1] + got[1:2] + got[2:3]
    counted = sums_ref[1:2] + got[3:4] + got[4:5] + got[5:6]
    lane = lax.broadcasted_iota(jnp.int32, (1, 128), 1)
    sums = pieces_of(jnp.where(lane < 64, summed, counted), 3)
    place = lax.broadcasted_iota(jnp.int32, (8, 128), 0)
    blocks = []
    for side in range(2):
        corner = jnp.zeros((8, 128), jnp.float32)
        for r in range(2):
            start = r * 128 + 112 * side
            tile = cross_ref[start : start + 16].astype(jnp.float32)
            for k in range(2):
                at = 14 * side + k
                corner = jnp.where(place == 2 * r + k, tile[at : at + 1], corner)
        for k in range(3):
            corner = jnp.where(place == 4 + k, sums[k], corner)
        blocks.append(jnp.concatenate([corner, packed(planes, 8 * side)], axis=0))
    n_x = 4
    for peer in range(n_x):
        chosen = jnp.where(at_ref[4] == peer, blocks[1], blocks[0]).astype(jnp.bfloat16)
        for group in range(sent_ref.shape[0] // n_x):
            sent_ref[group * n_x + peer] = chosen


def sides_of(at_ref):
    return (
        at_ref[0] == 0,
        jnp.where(at_ref[1] == 0, 0.0, 1.0),
        jnp.where(at_ref[2] == 0, 0.0, 1.0),
    )


def fill(rhs_ref, weight_ref):
    for a in range(3):
        for c in range(3):
            rhs_ref[a * 128 : a * 128 + 128, c * 128 : c * 128 + 128] = weight_ref[a, c]


def convolved(ext_ref, rhs_ref, bias, start, group):
    lhs = jnp.concatenate(
        [ext_ref[pl.ds(start + a, group)].reshape(group * WIDE, 128) for a in range(3)], axis=1
    )
    out = jnp.dot(lhs, rhs_ref[...], preferred_element_type=jnp.float32)
    rows = []
    for j in range(group):
        part = out[j * WIDE : (j + 1) * WIDE]
        rows.append(
            pltpu.roll(part[:, 0:128], 1, 0)
            + part[:, 128:256]
            + pltpu.roll(part[:, 256:384], WIDE - 1, 0)
            + bias
        )
    return rows


def forward_kernel(
    at_ref, hidden_ref, planes_ref, cross_ref, pair_ref, near_ref, weight_ref, bias_ref, proj_ref,
    alpha_ref, beta_ref,
    ext_ref, preact_ref, side_ref, rhs_ref,
):
    rows = hidden_ref.shape[0]
    n_x = near_ref.shape[0] // 2
    core, left, right = at_ref[0], at_ref[3], at_ref[4]
    upper, keep_above, keep_below = sides_of(at_ref)
    zero = jnp.zeros((), jnp.bfloat16)
    for k in range(2):
        cross = cross_ref[k * 128 : k * 128 + 128]
        pair = pair_ref[k * 128 : k * 128 + 128]
        ext_ref[k, 0:128] = jnp.where(keep_above > 0.0, jnp.where(upper, cross, pair), zero)
        ext_ref[k + rows + 2, 0:128] = jnp.where(
            keep_below > 0.0, jnp.where(upper, pair, cross), zero
        )
    ext_ref[2 : rows + 2, 0:128] = hidden_ref[...]
    place = lax.broadcasted_iota(jnp.int32, (WIDE - 128, 128), 0)
    tiles = [jnp.zeros((WIDE - 128, 128), jnp.float32) for _ in range(rows + 4)]
    second = []
    for side, base in ((right, 0), (left, WIDE - 130)):
        own = near_ref[core * n_x + side].astype(jnp.float32)
        other = near_ref[(1 - core) * n_x + side].astype(jnp.float32)
        for k in range(2):
            for r in range(rows + 4):
                at = r - 2
                if r < 2:
                    at = k * 16 + rows - 2 + r
                    row = other[at : at + 1] * keep_above
                elif r >= rows + 2:
                    at = k * 16 + r - rows - 2
                    row = other[at : at + 1] * keep_below
                else:
                    row = own[k * 16 + at : k * 16 + at + 1]
                tiles[r] = jnp.where(place == base + k, row, tiles[r])
        above = jnp.where(upper, 0.0, other[40:48] * keep_above)
        below = jnp.where(upper, other[32:40] * keep_below, 0.0)
        second.append(jnp.concatenate([above, own[32:48], below], axis=0))
    for r in range(rows + 4):
        ext_ref[r, 128:WIDE] = tiles[r].astype(jnp.bfloat16)
    cross = cross_ref[256:304].astype(jnp.float32)
    pair = pair_ref[256:304].astype(jnp.float32)
    above = jnp.where(upper, cross, pair) * keep_above
    below = jnp.where(upper, pair, cross) * keep_below
    planes = []
    for k in range(PLANES):
        at = k * 8
        tile = unpacked(second[0], second[1], k)
        planes.append(
            jnp.concatenate(
                [above[at : at + 8], planes_ref[k], below[at : at + 8], tile], axis=0
            )
        )
    side_ref[0 : 2 * PACK] = planes[0] + planes[1] + planes[2]
    side_ref[2 * PACK : 4 * PACK] = planes[3] + planes[4]
    fill(rhs_ref, weight_ref)
    bias = bias_ref[...]
    steps = [full(ref[k]) for ref in (alpha_ref, beta_ref) for k in range(ITERS)]
    params = [bias, proj_ref[...], *steps, full(0.0), full(0.0)]
    side_ref[4 * PACK : 4 * PACK + 16] = jnp.concatenate(params, axis=0)
    group = 4
    shift = jnp.where(upper, 2, 0)
    for g in range(0, rows, group):
        for j, row in enumerate(convolved(ext_ref, rhs_ref, bias, g + shift, group)):
            preact_ref[g + j] = row


def backward_kernel(
    at_ref, got_ref, kernel_ref, side_ref, preact_ref, early_ref,
    grad_hbm, sent_ref, ext_ref,
    grad_ref, moved_ref, weight_ref, rhs_ref, sem,
):
    rows = grad_ref.shape[0] - 2
    n_x = 4
    fields = side_ref[0 : 4 * PACK]
    fields = (fields[0 : 2 * PACK], fields[2 * PACK : 4 * PACK])
    params = side_ref[4 * PACK : 4 * PACK + 16]
    left, right = at_ref[3], at_ref[4]
    upper, keep_above, keep_below = sides_of(at_ref)
    keep_cross = jnp.where(upper, keep_above, keep_below)
    place = lax.broadcasted_iota(jnp.int32, (WIDE - 128, 128), 0)
    tiles = [jnp.zeros((WIDE - 128, 128), jnp.float32) for _ in range(2)]
    second = []
    for side, base in ((right, 0), (left, WIDE - 130)):
        corner = got_ref[at_ref[5] * n_x + side].astype(jnp.float32) * keep_cross
        for r in range(2):
            for k in range(2):
                row = corner[2 * r + k : 2 * r + k + 1]
                tiles[r] = jnp.where(place == base + k, row, tiles[r])
        second.append(corner[8:16])
    crossed = jnp.where(upper, 0, rows + 2)
    for r in range(2):
        ext_ref[crossed + r, 128:WIDE] = tiles[r].astype(jnp.bfloat16)
    fill(rhs_ref, kernel_ref)
    again = jnp.where(upper, 0, rows)
    fixed = convolved(ext_ref, rhs_ref, params[0:1], again, 2)
    corner = [unpacked(second[0], second[1], k) for k in range(PLANES)]
    corner = (corner[0] + corner[1] + corner[2], corner[3] + corner[4])
    start, wet_depth = [
        jnp.concatenate(
            [
                fields[k][0:PACK],
                fields[k][PACK : PACK + 8] + jnp.where(upper, corner[k], 0.0),
                fields[k][PACK + 8 : 2 * PACK - 8],
                fields[k][2 * PACK - 8 : 2 * PACK] + jnp.where(upper, 0.0, corner[k]),
            ],
            axis=0,
        )
        for k in range(2)
    ]
    lane = lax.broadcasted_iota(jnp.int32, (2 * PACK, 128), 1)
    mask = jnp.where(wet_depth > 0.0, 1.0, 0.0)

    def other_half(field):
        parts = [field[k * PACK : (k + 1) * PACK] for k in range(field.shape[0] // PACK)]
        swapped = []
        for k in range(0, len(parts), 2):
            swapped += [parts[k + 1], parts[k]]
        return jnp.concatenate(swapped, axis=0)

    def beside(field):
        count = field.shape[0]
        lanes = lane if count == 2 * PACK else jnp.concatenate([lane, lane], axis=0)
        up = pltpu.roll(field, 1, 0)
        down = pltpu.roll(field, count - 1, 0)
        from_left = pltpu.roll(field, 1, 1)
        from_left = jnp.where(lanes == 0, other_half(from_left), from_left)
        from_right = pltpu.roll(field, 127, 1)
        from_right = jnp.where(lanes == 127, other_half(from_right), from_right)
        return up, down, from_left, from_right

    weights = [
        0.5 * (near_mask * wet_depth + mask * near_depth)
        for near_mask, near_depth in zip(beside(mask), beside(wet_depth))
    ]
    diagonal = helm_coef * mask + weights[0] + weights[1] + weights[2] + weights[3]
    weights = [jnp.concatenate([w, w], axis=0) for w in weights]
    diagonal = jnp.concatenate([diagonal, diagonal], axis=0)
    residual = jnp.concatenate([start, mask], axis=0)
    direction = residual
    result = jnp.zeros_like(residual)
    for k in range(ITERS):
        result = result + params[2 + k : 3 + k] * direction
        if k + 1 < ITERS:
            applied = diagonal * direction
            for w, near in zip(weights, beside(direction)):
                applied = applied - w * near
            residual = residual - params[2 + k : 3 + k] * applied
            direction = residual + params[8 + k : 9 + k] * direction
    result = result * jnp.concatenate([mask, mask], axis=0)
    sums = jnp.sum(got_ref[...].astype(jnp.float32)[:, 0:8], axis=0)
    sums = sums[4:5] + sums[5:6] + sums[6:7]
    mean = jnp.broadcast_to(sums[:, 0:1], (1, 128)) / jnp.broadcast_to(sums[:, 127:128], (1, 128))
    force = result.T
    force = force - mean * pltpu.roll(force, 64, 1)
    proj = params[1:2]
    shift = jnp.where(upper, 2, 0)
    sum_bias = jnp.zeros((8, 128), jnp.float32)
    sum_proj = jnp.zeros((8, 128), jnp.float32)
    for g in range(rows + 2):
        at = g + 7
        column = jnp.concatenate(
            [
                force[:, at : at + 1],
                force[0:8, PACK + at : PACK + at + 1],
                force[120:128, PACK + at : PACK + at + 1],
            ],
            axis=0,
        )
        column = jnp.broadcast_to(column, (WIDE, 128))
        if g < 2:
            preact = jnp.where(upper, fixed[g], preact_ref[g])
        elif g >= rows:
            preact = jnp.where(upper, preact_ref[g - 2], fixed[g - rows])
        else:
            preact = preact_ref[g - shift]
        sigma = jax.nn.sigmoid(preact)
        active = preact * sigma
        slope_act = sigma * (1.0 + preact * (1.0 - sigma))
        grad = (column * proj * slope_act).astype(jnp.bfloat16)
        grad_ref[g] = grad
        if 1 <= g <= rows:
            own = grad.astype(jnp.float32)[0:128]
            for k in range(16):
                sum_bias = sum_bias + own[k * 8 : k * 8 + 8]
                sum_proj = sum_proj + (active * column)[k * 8 : k * 8 + 8]
            own = jnp.concatenate([own, jnp.zeros((WIDE - 128, 128), jnp.float32)], axis=0)
            moved_ref[g - 1, :, 0:128] = pltpu.roll(own, WIDE - 1, 0).astype(jnp.bfloat16)
            moved_ref[g - 1, :, 128:256] = own.astype(jnp.bfloat16)
            moved_ref[g - 1, :, 256:384] = pltpu.roll(own, 1, 0).astype(jnp.bfloat16)
    copy = pltpu.make_async_copy(grad_ref, grad_hbm, sem)
    copy.start()
    to = lax.broadcasted_iota(jnp.int32, (128, 128), 0)
    of = lax.broadcasted_iota(jnp.int32, (128, 128), 1)
    source = (
        to // 32 * 32 + to // 2 % 2 * 16 + to // 16 % 2 * 8 + to // 4 % 4 * 2 + to % 2
    )
    order = jnp.where(of == source, 1.0, 0.0).astype(jnp.bfloat16)
    moved = moved_ref[...].reshape(rows * WIDE, 384)
    for a in range(3):
        cells = ext_ref[a + 1 : a + 1 + rows].reshape(rows * WIDE, 128)
        out = lax.dot_general(
            cells, moved, (((0,), (0,)), ((), ())), preferred_element_type=jnp.float32
        )
        out = jnp.dot(
            order, out.astype(jnp.bfloat16), preferred_element_type=jnp.float32
        )
        for c in range(3):
            weight_ref[a * 3 + c] = out[:, c * 128 : c * 128 + 128]
    vectors = jnp.concatenate(
        [jnp.sum(sum_bias, axis=0, keepdims=True), jnp.sum(sum_proj, axis=0, keepdims=True)], axis=0
    )
    vectors = jnp.concatenate(pieces_of(vectors, 2) + [jnp.zeros((4, 128), jnp.float32)], axis=0)
    vectors = pltpu.roll(vectors, 4, 0)
    low = lax.broadcasted_iota(jnp.int32, (8, 128), 0) < 4

    def one_pair(t, carry):
        start = pl.multiple_of(t * 8, 8)
        blocks = ([], [])
        for k in range(0, 9, 2):
            one = weight_ref[k, pl.ds(start, 8)]
            two = weight_ref[k + 1, pl.ds(start, 8)] if k < 8 else vectors
            two_low = pltpu.roll(two, 4, 0) if k < 8 else vectors
            blocks[0].append(jnp.where(low, one, two_low))
            blocks[1].append(jnp.where(low, pltpu.roll(one, 4, 0), two))
        for x in range(2):
            sent_ref[t * 2 + x] = jnp.concatenate(blocks[x], axis=0).astype(jnp.bfloat16)
        return carry

    lax.fori_loop(0, 16, one_pair, 0)
    copy.wait()


def middle_kernel(got_ref, sent_ref):
    total = jnp.sum(got_ref[...].astype(jnp.float32), axis=0)
    vectors = total[36:38] + total[38:40]
    vectors = jnp.concatenate(pieces_of(vectors, 2) + [jnp.zeros((2, 128), jnp.float32)], axis=0)
    peers = sent_ref.shape[0] // 2
    for z in range(2):
        block = [total[4 * k + 2 * z : 4 * k + 2 * z + 2] for k in range(9)]
        block = jnp.concatenate(block + [vectors], axis=0)
        block = block.astype(jnp.bfloat16)
        for d in range(peers):
            sent_ref[z * peers + d] = block


def last_kernel(scale, got_ref, weight_ref, bias_ref, proj_ref):
    total = jnp.sum(got_ref[...].astype(jnp.float32), axis=0) * scale
    for k in range(9):
        weight_ref[k // 3, k % 3] = total[k * 2 : k * 2 + 2]
    bias_ref[...] = total[18:19] + total[20:21]
    proj_ref[...] = total[19:20] + total[21:22]


def input_kernel(grad_ref, weight_ref, out_ref, rhs_ref):
    rows = out_ref.shape[0]
    for a in range(3):
        for c in range(3):
            rhs_ref[c * 128 : c * 128 + 128, a * 128 : a * 128 + 128] = weight_ref[a, c]
    group = 4
    for y in range(0, rows, group):
        lhs = jnp.concatenate(
            [
                grad_ref[y - a + 2 : y - a + 2 + group].reshape(group * WIDE, 128)
                for a in range(3)
            ],
            axis=1,
        )
        out = lax.dot_general(
            lhs, rhs_ref[...], (((1,), (1,)), ((), ())), preferred_element_type=jnp.float32
        )
        for j in range(group):
            part = out[j * WIDE : (j + 1) * WIDE]
            total = (
                pltpu.roll(part[:, 0:128], WIDE - 1, 0)
                + part[:, 128:256]
                + pltpu.roll(part[:, 256:384], 1, 0)
            )
            out_ref[y + j] = total[0:128].astype(jnp.bfloat16)


def call(kernel, shapes, scratch, in_specs, args, out_specs=None, aliases={}):
    return pl.pallas_call(
        kernel,
        out_shape=shapes,
        in_specs=in_specs,
        out_specs=jax.tree.map(lambda _: VMEM, shapes) if out_specs is None else out_specs,
        scratch_shapes=scratch,
        input_output_aliases=aliases,
        compiler_params=pltpu.CompilerParams(vmem_limit_bytes=40 * 1024 * 1024),
    )(*args)


def shape(dims, dtype):
    return jax.ShapeDtypeStruct(dims, dtype)


def shards(
    hidden_in, conv_weight, conv_bias, proj_weight, ocean_depth, sea_mask,
    step_alpha, step_beta, surface_cotangent,
):
    wide, narrow = jnp.float32, jnp.bfloat16
    rows = hidden_in.shape[1]
    hidden = hidden_in[0]
    n_x = lax.axis_size("lon")
    n_lat = lax.axis_size(LAT)
    n_all = lax.axis_size(("lat_0", "lat_2", "lon"))
    n_z = lax.axis_size(("lat_1", "dp"))
    lat, me = lax.axis_index(LAT), lax.axis_index("lon")
    row_group = lax.axis_index(("lat_0", "lat_2"))
    at = jnp.stack(
        [lat % 2, lat, n_lat - 1 - lat, (me + n_x - 1) % n_x, (me + 1) % n_x, row_group]
    ).astype(jnp.int32)
    mask = sea_mask.astype(wide)
    fields = jnp.stack([mask * surface_cotangent[0], mask * ocean_depth])
    cross, pair, near, planes, sums = call(
        first_kernel,
        (
            shape((304, 128), narrow),
            shape((304, 128), narrow),
            shape((2 * n_x, NEAR, 128), narrow),
            shape((PLANES, rows, 128), wide),
            shape((2, 128), wide),
        ),
        [],
        [SMEM] + [VMEM] * 2,
        (at, hidden, fields),
    )
    odd = [(i, (i + 1) % n_lat) for i in range(1, n_lat, 2)]
    odd = odd + [(j, i) for i, j in odd]
    cross = lax.ppermute(cross, LAT, odd)
    pair = lax.ppermute(pair, "lat_2", [(0, 1), (1, 0)])
    near = lax.all_to_all(near, ("lat_2", "lon"), 0, 0, tiled=True)
    sent = call(
        second_kernel, shape((n_all, 16, 128), narrow), [], [SMEM] + [VMEM] * 2, (at, sums, cross)
    )
    got = lax.all_to_all(sent, ("lat_0", "lat_2", "lon"), 0, 0, tiled=True)
    early, preact, side = call(
        forward_kernel,
        (
            shape((rows + 4, WIDE, 128), narrow),
            shape((rows, WIDE, 128), wide),
            shape((4 * PACK + 16, 128), wide),
        ),
        [pltpu.VMEM((384, 384), narrow)],
        [SMEM] + [VMEM] * 8 + [SMEM] * 2,
        (
            at, hidden, planes, cross, pair, near, conv_weight, conv_bias[None],
            proj_weight[None], step_alpha, step_beta,
        ),
    )
    grad, sent, _ = call(
        backward_kernel,
        (
            shape((rows + 2, WIDE, 128), narrow),
            shape((n_all, 40, 128), narrow),
            shape((rows + 4, WIDE, 128), narrow),
        ),
        [
            pltpu.VMEM((rows + 2, WIDE, 128), narrow),
            pltpu.VMEM((rows, WIDE, 384), narrow),
            pltpu.VMEM((9, 128, 128), wide),
            pltpu.VMEM((384, 384), narrow),
            pltpu.SemaphoreType.DMA,
        ],
        [SMEM] + [VMEM] * 5,
        (at, got, conv_weight, side, preact, early),
        (HBM, VMEM, VMEM),
        {5: 2},
    )
    got = lax.all_to_all(sent, ("lat_0", "lat_2", "lon"), 0, 0, tiled=True)
    sent = call(middle_kernel, shape((n_z, 24, 128), narrow), [], [VMEM], (got,))
    got = lax.all_to_all(sent, ("lat_1", "dp"), 0, 0, tiled=True)
    grad_hidden = call(
        input_kernel,
        shape((rows, 128, 128), narrow),
        [pltpu.VMEM((384, 384), narrow)],
        [VMEM] * 2,
        (grad, conv_weight),
    )
    cells = rows * 128 * lax.axis_size("dp") * n_lat * n_x
    own_weight, total_bias, total_proj = call(
        functools.partial(last_kernel, 1.0 / math.sqrt(cells)),
        (shape((3, 3, 2, 128), wide), shape((1, 128), wide), shape((1, 128), wide)),
        [],
        [VMEM],
        (got,),
    )
    return grad_hidden[None], own_weight.transpose(2, 0, 1, 3), total_bias[0], total_proj[0]


def solution(mesh):
    split = Mesh(
        mesh.devices.reshape(mesh.shape["dp"], 4, 2, 2, mesh.shape["lon"]),
        ("dp", "lat_0", "lat_1", "lat_2", "lon"),
    )
    placed = (
        P("dp", LAT, "lon", None),
        P(),
        P(),
        P(),
        P(LAT, "lon"),
        P(LAT, "lon"),
        P(),
        P(),
        P("dp", LAT, "lon"),
    )
    return jax.shard_map(
        shards,
        mesh=split,
        in_specs=placed,
        out_specs=(P("dp", LAT, "lon", None), P(LAT_LON, None, None, None), P(), P()),
        check_vma=False,
    )
```

```python
import functools
import math

import jax
import jax.numpy as jnp
from jax import lax
from jax.experimental import pallas as pl
from jax.experimental.pallas import tpu as pltpu
from jax.sharding import Mesh
from jax.sharding import PartitionSpec as P

ITERS = 6
LAT_LON = ("lat_0", "lat_1", "lat_2", "lon")
LAT = ("lat_0", "lat_1", "lat_2")
WIDE = 144
CHUNK = 48
PACK = 32
PLANES = 5
NEAR = 48

helm_coef = 0.5
VMEM = pl.BlockSpec(memory_space=pltpu.VMEM)
SMEM = pl.BlockSpec(memory_space=pltpu.SMEM)
HBM = pl.BlockSpec(memory_space=pltpu.HBM)


def rounded(values):
    return values.astype(jnp.bfloat16).astype(jnp.float32)


def pieces_of(values, count):
    out = []
    for _ in range(count):
        piece = rounded(values)
        out.append(piece)
        values = values - piece
    return out


def full(value):
    return jnp.full((1, 128), value, jnp.float32)


def packed(planes, shift):
    rows = planes[0].shape[0]
    lane = lax.broadcasted_iota(jnp.int32, (rows, 128), 1) // 8
    out = jnp.zeros((rows, 128), jnp.float32)
    for k, plane in enumerate(planes):
        by = (8 * k + shift) % 128
        out = jnp.where(lane == k, pltpu.roll(plane, by, 1) if by else plane, out)
    return out


def edge_columns(load, rows):
    place = lax.broadcasted_iota(jnp.int32, (8, 128), 0)
    columns = [[jnp.zeros((8, 128), jnp.float32) for _ in range(rows // 8)] for _ in range(4)]
    for r in range(rows):
        head = load(r, 0).astype(jnp.float32)
        tail = load(r, 112).astype(jnp.float32)
        for k, row in enumerate((head[0:1], head[1:2], tail[14:15], tail[15:16])):
            columns[k][r // 8] = jnp.where(place == r % 8, row, columns[k][r // 8])
    return columns


def unpacked(beyond, before, k):
    near = lax.broadcasted_iota(jnp.int32, beyond.shape, 1)
    if k:
        beyond = pltpu.roll(beyond, 128 - 8 * k, 1)
    before = pltpu.roll(before, 120 - 8 * k, 1)
    return jnp.where(near < 8, beyond, jnp.where(near >= 120, before, 0.0))


def first_kernel(
    at_ref, hidden_ref, fields_ref, cross_ref, pair_ref, near_ref, planes_ref, sums_ref
):
    rows = hidden_ref.shape[0]
    upper = at_ref[0] == 0
    wet, wet_depth = fields_ref[0], fields_ref[1]
    planes = pieces_of(wet, 3) + pieces_of(wet_depth, 2)
    summed = full(jnp.sum(wet))
    counted = full(jnp.sum(jnp.where(wet_depth > 0.0, 1.0, 0.0)))
    sums_ref[0:1] = summed
    sums_ref[1:2] = counted
    sums = pieces_of(summed, 3) + pieces_of(counted, 3)
    sums = jnp.concatenate(sums + [jnp.zeros((2, 128), jnp.float32)], axis=0)
    for k in range(PLANES):
        planes_ref[k] = planes[k]
    for ref, top in ((cross_ref, upper), (pair_ref, jnp.logical_not(upper))):
        start = jnp.where(top, 0, rows - 2)
        ref[0:256] = hidden_ref[pl.ds(start, 2)].reshape(256, 128)
        near = [jnp.where(top, p[0:8], p[rows - 8 : rows]) for p in planes] + [sums]
        for k in range(0, 6, 2):
            tile = jnp.concatenate(near[k : k + 2], axis=0)
            ref[256 + k * 8 : 272 + k * 8] = tile.astype(jnp.bfloat16)
    columns = edge_columns(lambda r, at: hidden_ref[r, at : at + 16], rows)
    head = jnp.concatenate(columns[0] + columns[1] + [packed(planes, 0)], axis=0)
    tail = jnp.concatenate(columns[2] + columns[3] + [packed(planes, 8)], axis=0)
    n_x = near_ref.shape[0] // 2
    for peer in range(n_x):
        chosen = jnp.where(at_ref[4] == peer, tail, head).astype(jnp.bfloat16)
        near_ref[peer] = chosen
        near_ref[n_x + peer] = chosen


def second_kernel(at_ref, sums_ref, cross_ref, sent_ref):
    tiles = [cross_ref[256 + k * 16 : 272 + k * 16].astype(jnp.float32) for k in range(3)]
    planes = [tiles[k // 2][k % 2 * 8 : k % 2 * 8 + 8] for k in range(PLANES)]
    got = tiles[2][8:16]
    summed = sums_ref[0:1] + got[0:1] + got[1:2] + got[2:3]
    counted = sums_ref[1:2] + got[3:4] + got[4:5] + got[5:6]
    lane = lax.broadcasted_iota(jnp.int32, (1, 128), 1)
    sums = pieces_of(jnp.where(lane < 64, summed, counted), 3)
    place = lax.broadcasted_iota(jnp.int32, (8, 128), 0)
    blocks = []
    for side in range(2):
        corner = jnp.zeros((8, 128), jnp.float32)
        for r in range(2):
            start = r * 128 + 112 * side
            tile = cross_ref[start : start + 16].astype(jnp.float32)
            for k in range(2):
                at = 14 * side + k
                corner = jnp.where(place == 2 * r + k, tile[at : at + 1], corner)
        for k in range(3):
            corner = jnp.where(place == 4 + k, sums[k], corner)
        blocks.append(jnp.concatenate([corner, packed(planes, 8 * side)], axis=0))
    n_x = 4
    for peer in range(n_x):
        chosen = jnp.where(at_ref[4] == peer, blocks[1], blocks[0]).astype(jnp.bfloat16)
        for group in range(sent_ref.shape[0] // n_x):
            sent_ref[group * n_x + peer] = chosen


def sides_of(at_ref):
    return (
        at_ref[0] == 0,
        jnp.where(at_ref[1] == 0, 0.0, 1.0),
        jnp.where(at_ref[2] == 0, 0.0, 1.0),
    )


def fill(rhs_ref, weight_ref):
    for a in range(3):
        for c in range(3):
            rhs_ref[a * 128 : a * 128 + 128, c * 128 : c * 128 + 128] = weight_ref[a, c]


def convolved(ext_ref, rhs_ref, bias, start, group):
    lhs = jnp.concatenate(
        [ext_ref[pl.ds(start + a, group)].reshape(group * WIDE, 128) for a in range(3)], axis=1
    )
    out = jnp.dot(lhs, rhs_ref[...], preferred_element_type=jnp.float32)
    rows = []
    for j in range(group):
        part = out[j * WIDE : (j + 1) * WIDE]
        rows.append(
            pltpu.roll(part[:, 0:128], 1, 0)
            + part[:, 128:256]
            + pltpu.roll(part[:, 256:384], WIDE - 1, 0)
            + bias
        )
    return rows


def forward_kernel(
    at_ref, hidden_ref, planes_ref, cross_ref, pair_ref, near_ref, weight_ref, bias_ref, proj_ref,
    alpha_ref, beta_ref,
    ext_ref, preact_ref, side_ref, rhs_ref,
):
    rows = hidden_ref.shape[0]
    n_x = near_ref.shape[0] // 2
    core, left, right = at_ref[0], at_ref[3], at_ref[4]
    upper, keep_above, keep_below = sides_of(at_ref)
    zero = jnp.zeros((), jnp.bfloat16)
    for k in range(2):
        cross = cross_ref[k * 128 : k * 128 + 128]
        pair = pair_ref[k * 128 : k * 128 + 128]
        ext_ref[k, 0:128] = jnp.where(keep_above > 0.0, jnp.where(upper, cross, pair), zero)
        ext_ref[k + rows + 2, 0:128] = jnp.where(
            keep_below > 0.0, jnp.where(upper, pair, cross), zero
        )
    ext_ref[2 : rows + 2, 0:128] = hidden_ref[...]
    place = lax.broadcasted_iota(jnp.int32, (WIDE - 128, 128), 0)
    tiles = [jnp.zeros((WIDE - 128, 128), jnp.float32) for _ in range(rows + 4)]
    second = []
    for side, base in ((right, 0), (left, WIDE - 130)):
        own = near_ref[core * n_x + side].astype(jnp.float32)
        other = near_ref[(1 - core) * n_x + side].astype(jnp.float32)
        for k in range(2):
            for r in range(rows + 4):
                at = r - 2
                if r < 2:
                    at = k * 16 + rows - 2 + r
                    row = other[at : at + 1] * keep_above
                elif r >= rows + 2:
                    at = k * 16 + r - rows - 2
                    row = other[at : at + 1] * keep_below
                else:
                    row = own[k * 16 + at : k * 16 + at + 1]
                tiles[r] = jnp.where(place == base + k, row, tiles[r])
        above = jnp.where(upper, 0.0, other[40:48] * keep_above)
        below = jnp.where(upper, other[32:40] * keep_below, 0.0)
        second.append(jnp.concatenate([above, own[32:48], below], axis=0))
    for r in range(rows + 4):
        ext_ref[r, 128:WIDE] = tiles[r].astype(jnp.bfloat16)
    cross = cross_ref[256:304].astype(jnp.float32)
    pair = pair_ref[256:304].astype(jnp.float32)
    above = jnp.where(upper, cross, pair) * keep_above
    below = jnp.where(upper, pair, cross) * keep_below
    planes = []
    for k in range(PLANES):
        at = k * 8
        tile = unpacked(second[0], second[1], k)
        planes.append(
            jnp.concatenate(
                [above[at : at + 8], planes_ref[k], below[at : at + 8], tile], axis=0
            )
        )
    side_ref[0 : 2 * PACK] = planes[0] + planes[1] + planes[2]
    side_ref[2 * PACK : 4 * PACK] = planes[3] + planes[4]
    fill(rhs_ref, weight_ref)
    bias = bias_ref[...]
    steps = [full(ref[k]) for ref in (alpha_ref, beta_ref) for k in range(ITERS)]
    params = [bias, proj_ref[...], *steps, full(0.0), full(0.0)]
    side_ref[4 * PACK : 4 * PACK + 16] = jnp.concatenate(params, axis=0)
    group = 4
    shift = jnp.where(upper, 2, 0)
    for g in range(0, rows, group):
        for j, row in enumerate(convolved(ext_ref, rhs_ref, bias, g + shift, group)):
            preact_ref[g + j] = 0.5 * row


def backward_kernel(
    at_ref, got_ref, kernel_ref, side_ref, preact_ref, early_ref,
    grad_hbm, sent_ref, ext_ref,
    grad_ref, moved_ref, weight_ref, rhs_ref, fixed_ref, sem,
):
    rows = grad_ref.shape[0] - 2
    n_x = 4
    fields = side_ref[0 : 4 * PACK]
    fields = (fields[0 : 2 * PACK], fields[2 * PACK : 4 * PACK])
    params = side_ref[4 * PACK : 4 * PACK + 16]
    left, right = at_ref[3], at_ref[4]
    upper, keep_above, keep_below = sides_of(at_ref)
    keep_cross = jnp.where(upper, keep_above, keep_below)
    place = lax.broadcasted_iota(jnp.int32, (WIDE - 128, 128), 0)
    tiles = [jnp.zeros((WIDE - 128, 128), jnp.float32) for _ in range(2)]
    second = []
    for side, base in ((right, 0), (left, WIDE - 130)):
        corner = got_ref[at_ref[5] * n_x + side].astype(jnp.float32) * keep_cross
        for r in range(2):
            for k in range(2):
                row = corner[2 * r + k : 2 * r + k + 1]
                tiles[r] = jnp.where(place == base + k, row, tiles[r])
        second.append(corner[8:16])
    crossed = jnp.where(upper, 0, rows + 2)
    for r in range(2):
        ext_ref[crossed + r, 128:WIDE] = tiles[r].astype(jnp.bfloat16)
    fill(rhs_ref, kernel_ref)
    again = jnp.where(upper, 0, rows)
    for g, row in enumerate(convolved(ext_ref, rhs_ref, params[0:1], again, 2)):
        fixed_ref[g] = 0.5 * row
    corner = [unpacked(second[0], second[1], k) for k in range(PLANES)]
    corner = (corner[0] + corner[1] + corner[2], corner[3] + corner[4])
    start, wet_depth = [
        jnp.concatenate(
            [
                fields[k][0:PACK],
                fields[k][PACK : PACK + 8] + jnp.where(upper, corner[k], 0.0),
                fields[k][PACK + 8 : 2 * PACK - 8],
                fields[k][2 * PACK - 8 : 2 * PACK] + jnp.where(upper, 0.0, corner[k]),
            ],
            axis=0,
        )
        for k in range(2)
    ]
    lane = lax.broadcasted_iota(jnp.int32, (2 * PACK, 128), 1)
    mask = jnp.where(wet_depth > 0.0, 1.0, 0.0)

    def other_half(field):
        parts = [field[k * PACK : (k + 1) * PACK] for k in range(field.shape[0] // PACK)]
        swapped = []
        for k in range(0, len(parts), 2):
            swapped += [parts[k + 1], parts[k]]
        return jnp.concatenate(swapped, axis=0)

    def beside(field):
        count = field.shape[0]
        lanes = lane if count == 2 * PACK else jnp.concatenate([lane, lane], axis=0)
        up = pltpu.roll(field, 1, 0)
        down = pltpu.roll(field, count - 1, 0)
        from_left = pltpu.roll(field, 1, 1)
        from_left = jnp.where(lanes == 0, other_half(from_left), from_left)
        from_right = pltpu.roll(field, 127, 1)
        from_right = jnp.where(lanes == 127, other_half(from_right), from_right)
        return up, down, from_left, from_right

    weights = [
        0.5 * (near_mask * wet_depth + mask * near_depth)
        for near_mask, near_depth in zip(beside(mask), beside(wet_depth))
    ]
    diagonal = helm_coef * mask + weights[0] + weights[1] + weights[2] + weights[3]
    weights = [jnp.concatenate([w, w], axis=0) for w in weights]
    diagonal = jnp.concatenate([diagonal, diagonal], axis=0)
    residual = jnp.concatenate([start, mask], axis=0)
    direction = residual
    result = jnp.zeros_like(residual)
    for k in range(ITERS):
        result = result + params[2 + k : 3 + k] * direction
        if k + 1 < ITERS:
            applied = diagonal * direction
            for w, near in zip(weights, beside(direction)):
                applied = applied - w * near
            residual = residual - params[2 + k : 3 + k] * applied
            direction = residual + params[8 + k : 9 + k] * direction
    result = result * jnp.concatenate([mask, mask], axis=0)
    sums = jnp.sum(got_ref[...].astype(jnp.float32)[:, 0:8], axis=0)
    sums = sums[4:5] + sums[5:6] + sums[6:7]
    mean = jnp.broadcast_to(sums[:, 0:1], (1, 128)) / jnp.broadcast_to(sums[:, 127:128], (1, 128))
    force = result.T
    force = force - mean * pltpu.roll(force, 64, 1)
    proj = 0.5 * params[1:2]
    shift = jnp.where(upper, 2, 0)
    sum_bias = jnp.zeros((8, 128), jnp.float32)
    sum_proj = jnp.zeros((8, 128), jnp.float32)
    for g in range(rows + 2):
        at = g + 7
        edge = jnp.concatenate(
            [force[0:8, PACK + at : PACK + at + 1], force[120:128, PACK + at : PACK + at + 1]],
            axis=0,
        )
        for q in range(0, WIDE, CHUNK):
            parts = []
            if q < 128:
                parts.append(force[q : min(q + CHUNK, 128), at : at + 1])
            if q + CHUNK > 128:
                parts.append(edge)
            column = parts[0] if len(parts) == 1 else jnp.concatenate(parts, axis=0)
            column = jnp.broadcast_to(column, (CHUNK, 128))
            if g < 2:
                preact = jnp.where(upper, fixed_ref[g, q : q + CHUNK], preact_ref[g, q : q + CHUNK])
            elif g >= rows:
                preact = jnp.where(
                    upper, preact_ref[g - 2, q : q + CHUNK], fixed_ref[g - rows, q : q + CHUNK]
                )
            else:
                preact = preact_ref[g - shift, q : q + CHUNK]
            turn = jnp.tanh(preact)
            bent = preact * turn
            active = preact + bent
            slope_act = (1.0 + turn) * ((1.0 + preact) - bent)
            grad = (column * proj * slope_act).astype(jnp.bfloat16)
            grad_ref[g, q : q + CHUNK] = grad
            if 1 <= g <= rows:
                own = grad.astype(jnp.float32)
                drawn = active * column
                for k in range(min(CHUNK, 128 - q) // 8):
                    sum_bias = sum_bias + own[k * 8 : k * 8 + 8]
                    sum_proj = sum_proj + drawn[k * 8 : k * 8 + 8]
    for g in range(1, rows + 1):
        own = grad_ref[g, 0:128].astype(jnp.float32)
        own = jnp.concatenate([own, jnp.zeros((WIDE - 128, 128), jnp.float32)], axis=0)
        moved_ref[g - 1, :, 0:128] = pltpu.roll(own, WIDE - 1, 0).astype(jnp.bfloat16)
        moved_ref[g - 1, :, 128:256] = own.astype(jnp.bfloat16)
        moved_ref[g - 1, :, 256:384] = pltpu.roll(own, 1, 0).astype(jnp.bfloat16)
    copy = pltpu.make_async_copy(grad_ref, grad_hbm, sem)
    copy.start()
    to = lax.broadcasted_iota(jnp.int32, (128, 128), 0)
    of = lax.broadcasted_iota(jnp.int32, (128, 128), 1)
    source = (
        to // 32 * 32 + to // 2 % 2 * 16 + to // 16 % 2 * 8 + to // 4 % 4 * 2 + to % 2
    )
    order = jnp.where(of == source, 1.0, 0.0).astype(jnp.bfloat16)
    moved = moved_ref[...].reshape(rows * WIDE, 384)
    cells = jnp.concatenate(
        [ext_ref[a + 1 : a + 1 + rows].reshape(rows * WIDE, 128) for a in range(3)], axis=1
    )
    whole = lax.dot_general(
        cells, moved, (((0,), (0,)), ((), ())), preferred_element_type=jnp.float32
    )
    for a in range(3):
        out = whole[a * 128 : a * 128 + 128]
        out = jnp.dot(
            order, out.astype(jnp.bfloat16), preferred_element_type=jnp.float32
        )
        for c in range(3):
            weight_ref[a * 3 + c] = out[:, c * 128 : c * 128 + 128]
    vectors = jnp.concatenate(
        [jnp.sum(sum_bias, axis=0, keepdims=True), jnp.sum(sum_proj, axis=0, keepdims=True)], axis=0
    )
    vectors = jnp.concatenate(pieces_of(vectors, 2) + [jnp.zeros((4, 128), jnp.float32)], axis=0)
    vectors = pltpu.roll(vectors, 4, 0)
    low = lax.broadcasted_iota(jnp.int32, (8, 128), 0) < 4

    def one_pair(t, carry):
        start = pl.multiple_of(t * 8, 8)
        blocks = ([], [])
        for k in range(0, 9, 2):
            one = weight_ref[k, pl.ds(start, 8)]
            two = weight_ref[k + 1, pl.ds(start, 8)] if k < 8 else vectors
            two_low = pltpu.roll(two, 4, 0) if k < 8 else vectors
            blocks[0].append(jnp.where(low, one, two_low))
            blocks[1].append(jnp.where(low, pltpu.roll(one, 4, 0), two))
        for x in range(2):
            sent_ref[t * 2 + x] = jnp.concatenate(blocks[x], axis=0).astype(jnp.bfloat16)
        return carry

    lax.fori_loop(0, 16, one_pair, 0)
    copy.wait()


def middle_kernel(got_ref, sent_ref):
    total = jnp.sum(got_ref[...].astype(jnp.float32), axis=0)
    vectors = total[36:38] + total[38:40]
    vectors = jnp.concatenate(pieces_of(vectors, 2) + [jnp.zeros((2, 128), jnp.float32)], axis=0)
    peers = sent_ref.shape[0] // 2
    for z in range(2):
        block = [total[4 * k + 2 * z : 4 * k + 2 * z + 2] for k in range(9)]
        block = jnp.concatenate(block + [vectors], axis=0)
        block = block.astype(jnp.bfloat16)
        for d in range(peers):
            sent_ref[z * peers + d] = block


def last_kernel(scale, got_ref, weight_ref, bias_ref, proj_ref):
    total = jnp.sum(got_ref[...].astype(jnp.float32), axis=0) * scale
    for k in range(9):
        weight_ref[k // 3, k % 3] = total[k * 2 : k * 2 + 2]
    bias_ref[...] = total[18:19] + total[20:21]
    proj_ref[...] = total[19:20] + total[21:22]


def input_kernel(grad_ref, weight_ref, out_ref, rhs_ref):
    rows = out_ref.shape[0]
    for a in range(3):
        for c in range(3):
            rhs_ref[c * 128 : c * 128 + 128, a * 128 : a * 128 + 128] = weight_ref[a, c]
    group = 4
    for y in range(0, rows, group):
        lhs = jnp.concatenate(
            [
                grad_ref[y - a + 2 : y - a + 2 + group].reshape(group * WIDE, 128)
                for a in range(3)
            ],
            axis=1,
        )
        out = lax.dot_general(
            lhs, rhs_ref[...], (((1,), (1,)), ((), ())), preferred_element_type=jnp.float32
        )
        for j in range(group):
            part = out[j * WIDE : (j + 1) * WIDE]
            total = (
                pltpu.roll(part[:, 0:128], WIDE - 1, 0)
                + part[:, 128:256]
                + pltpu.roll(part[:, 256:384], 1, 0)
            )
            out_ref[y + j] = total[0:128].astype(jnp.bfloat16)


def call(kernel, shapes, scratch, in_specs, args, out_specs=None, aliases={}):
    return pl.pallas_call(
        kernel,
        out_shape=shapes,
        in_specs=in_specs,
        out_specs=jax.tree.map(lambda _: VMEM, shapes) if out_specs is None else out_specs,
        scratch_shapes=scratch,
        input_output_aliases=aliases,
        compiler_params=pltpu.CompilerParams(vmem_limit_bytes=40 * 1024 * 1024),
    )(*args)


def shape(dims, dtype):
    return jax.ShapeDtypeStruct(dims, dtype)


def shards(
    hidden_in, conv_weight, conv_bias, proj_weight, ocean_depth, sea_mask,
    step_alpha, step_beta, surface_cotangent,
):
    wide, narrow = jnp.float32, jnp.bfloat16
    rows = hidden_in.shape[1]
    hidden = hidden_in[0]
    n_x = lax.axis_size("lon")
    n_lat = lax.axis_size(LAT)
    n_all = lax.axis_size(("lat_0", "lat_2", "lon"))
    n_z = lax.axis_size(("lat_1", "dp"))
    lat, me = lax.axis_index(LAT), lax.axis_index("lon")
    row_group = lax.axis_index(("lat_0", "lat_2"))
    at = jnp.stack(
        [lat % 2, lat, n_lat - 1 - lat, (me + n_x - 1) % n_x, (me + 1) % n_x, row_group]
    ).astype(jnp.int32)
    mask = sea_mask.astype(wide)
    fields = jnp.stack([mask * surface_cotangent[0], mask * ocean_depth])
    cross, pair, near, planes, sums = call(
        first_kernel,
        (
            shape((304, 128), narrow),
            shape((304, 128), narrow),
            shape((2 * n_x, NEAR, 128), narrow),
            shape((PLANES, rows, 128), wide),
            shape((2, 128), wide),
        ),
        [],
        [SMEM] + [VMEM] * 2,
        (at, hidden, fields),
    )
    odd = [(i, (i + 1) % n_lat) for i in range(1, n_lat, 2)]
    odd = odd + [(j, i) for i, j in odd]
    cross = lax.ppermute(cross, LAT, odd)
    pair = lax.ppermute(pair, "lat_2", [(0, 1), (1, 0)])
    near = lax.all_to_all(near, ("lat_2", "lon"), 0, 0, tiled=True)
    sent = call(
        second_kernel, shape((n_all, 16, 128), narrow), [], [SMEM] + [VMEM] * 2, (at, sums, cross)
    )
    got = lax.all_to_all(sent, ("lat_0", "lat_2", "lon"), 0, 0, tiled=True)
    early, preact, side = call(
        forward_kernel,
        (
            shape((rows + 4, WIDE, 128), narrow),
            shape((rows, WIDE, 128), wide),
            shape((4 * PACK + 16, 128), wide),
        ),
        [pltpu.VMEM((384, 384), narrow)],
        [SMEM] + [VMEM] * 8 + [SMEM] * 2,
        (
            at, hidden, planes, cross, pair, near, conv_weight, conv_bias[None],
            proj_weight[None], step_alpha, step_beta,
        ),
    )
    grad, sent, _ = call(
        backward_kernel,
        (
            shape((rows + 2, WIDE, 128), narrow),
            shape((n_all, 40, 128), narrow),
            shape((rows + 4, WIDE, 128), narrow),
        ),
        [
            pltpu.VMEM((rows + 2, WIDE, 128), narrow),
            pltpu.VMEM((rows, WIDE, 384), narrow),
            pltpu.VMEM((9, 128, 128), wide),
            pltpu.VMEM((384, 384), narrow),
            pltpu.VMEM((2, WIDE, 128), wide),
            pltpu.SemaphoreType.DMA,
        ],
        [SMEM] + [VMEM] * 5,
        (at, got, conv_weight, side, preact, early),
        (HBM, VMEM, VMEM),
        {5: 2},
    )
    got = lax.all_to_all(sent, ("lat_0", "lat_2", "lon"), 0, 0, tiled=True)
    sent = call(middle_kernel, shape((n_z, 24, 128), narrow), [], [VMEM], (got,))
    got = lax.all_to_all(sent, ("lat_1", "dp"), 0, 0, tiled=True)
    grad_hidden = call(
        input_kernel,
        shape((rows, 128, 128), narrow),
        [pltpu.VMEM((384, 384), narrow)],
        [VMEM] * 2,
        (grad, conv_weight),
    )
    cells = rows * 128 * lax.axis_size("dp") * n_lat * n_x
    own_weight, total_bias, total_proj = call(
        functools.partial(last_kernel, 1.0 / math.sqrt(cells)),
        (shape((3, 3, 2, 128), wide), shape((1, 128), wide), shape((1, 128), wide)),
        [],
        [VMEM],
        (got,),
    )
    return grad_hidden[None], own_weight.transpose(2, 0, 1, 3), total_bias[0], total_proj[0]


def solution(mesh):
    split = Mesh(
        mesh.devices.reshape(mesh.shape["dp"], 4, 2, 2, mesh.shape["lon"]),
        ("dp", "lat_0", "lat_1", "lat_2", "lon"),
    )
    placed = (
        P("dp", LAT, "lon", None),
        P(),
        P(),
        P(),
        P(LAT, "lon"),
        P(LAT, "lon"),
        P(),
        P(),
        P("dp", LAT, "lon"),
    )
    return jax.shard_map(
        shards,
        mesh=split,
        in_specs=placed,
        out_specs=(P("dp", LAT, "lon", None), P(LAT_LON, None, None, None), P(), P()),
        check_vma=False,
    )
```

```python
import functools
import math

import jax
import jax.numpy as jnp
from jax import lax
from jax.experimental import pallas as pl
from jax.experimental.pallas import tpu as pltpu
from jax.sharding import Mesh
from jax.sharding import PartitionSpec as P

ITERS = 6
LAT_LON = ("lat_0", "lat_1", "lat_2", "lon")
LAT = ("lat_0", "lat_1", "lat_2")
WIDE = 144
SLIM = 136
PACK = 32
PLANES = 5
NEAR = 48

helm_coef = 0.5
VMEM = pl.BlockSpec(memory_space=pltpu.VMEM)
SMEM = pl.BlockSpec(memory_space=pltpu.SMEM)
HBM = pl.BlockSpec(memory_space=pltpu.HBM)


def rounded(values):
    return values.astype(jnp.bfloat16).astype(jnp.float32)


def pieces_of(values, count):
    out = []
    for _ in range(count):
        piece = rounded(values)
        out.append(piece)
        values = values - piece
    return out


def full(value):
    return jnp.full((1, 128), value, jnp.float32)


def packed(planes, shift):
    rows = planes[0].shape[0]
    lane = lax.broadcasted_iota(jnp.int32, (rows, 128), 1) // 8
    out = jnp.zeros((rows, 128), jnp.float32)
    for k, plane in enumerate(planes):
        by = (8 * k + shift) % 128
        out = jnp.where(lane == k, pltpu.roll(plane, by, 1) if by else plane, out)
    return out


def edge_columns(load, rows):
    place = lax.broadcasted_iota(jnp.int32, (8, 128), 0)
    columns = [[jnp.zeros((8, 128), jnp.float32) for _ in range(rows // 8)] for _ in range(4)]
    for r in range(rows):
        head = load(r, 0).astype(jnp.float32)
        tail = load(r, 112).astype(jnp.float32)
        for k, row in enumerate((head[0:1], head[1:2], tail[14:15], tail[15:16])):
            columns[k][r // 8] = jnp.where(place == r % 8, row, columns[k][r // 8])
    return columns


def unpacked(beyond, before, k):
    near = lax.broadcasted_iota(jnp.int32, beyond.shape, 1)
    if k:
        beyond = pltpu.roll(beyond, 128 - 8 * k, 1)
    before = pltpu.roll(before, 120 - 8 * k, 1)
    return jnp.where(near < 8, beyond, jnp.where(near >= 120, before, 0.0))


def first_kernel(
    at_ref, hidden_ref, fields_ref, cross_ref, pair_ref, near_ref, planes_ref, sums_ref
):
    rows = hidden_ref.shape[0]
    upper = at_ref[0] == 0
    wet, wet_depth = fields_ref[0], fields_ref[1]
    planes = pieces_of(wet, 3) + pieces_of(wet_depth, 2)
    summed = full(jnp.sum(wet))
    counted = full(jnp.sum(jnp.where(wet_depth > 0.0, 1.0, 0.0)))
    sums_ref[0:1] = summed
    sums_ref[1:2] = counted
    sums = pieces_of(summed, 3) + pieces_of(counted, 3)
    sums = jnp.concatenate(sums + [jnp.zeros((2, 128), jnp.float32)], axis=0)
    for k in range(PLANES):
        planes_ref[k] = planes[k]
    for ref, top in ((cross_ref, upper), (pair_ref, jnp.logical_not(upper))):
        start = jnp.where(top, 0, rows - 2)
        ref[0:256] = hidden_ref[pl.ds(start, 2)].reshape(256, 128)
        near = [jnp.where(top, p[0:8], p[rows - 8 : rows]) for p in planes] + [sums]
        for k in range(0, 6, 2):
            tile = jnp.concatenate(near[k : k + 2], axis=0)
            ref[256 + k * 8 : 272 + k * 8] = tile.astype(jnp.bfloat16)
    columns = edge_columns(lambda r, at: hidden_ref[r, at : at + 16], rows)
    head = jnp.concatenate(columns[0] + columns[1] + [packed(planes, 0)], axis=0)
    tail = jnp.concatenate(columns[2] + columns[3] + [packed(planes, 8)], axis=0)
    n_x = near_ref.shape[0] // 2
    for peer in range(n_x):
        chosen = jnp.where(at_ref[4] == peer, tail, head).astype(jnp.bfloat16)
        near_ref[peer] = chosen
        near_ref[n_x + peer] = chosen


def second_kernel(at_ref, sums_ref, cross_ref, sent_ref):
    tiles = [cross_ref[256 + k * 16 : 272 + k * 16].astype(jnp.float32) for k in range(3)]
    planes = [tiles[k // 2][k % 2 * 8 : k % 2 * 8 + 8] for k in range(PLANES)]
    got = tiles[2][8:16]
    summed = sums_ref[0:1] + got[0:1] + got[1:2] + got[2:3]
    counted = sums_ref[1:2] + got[3:4] + got[4:5] + got[5:6]
    lane = lax.broadcasted_iota(jnp.int32, (1, 128), 1)
    sums = pieces_of(jnp.where(lane < 64, summed, counted), 3)
    place = lax.broadcasted_iota(jnp.int32, (8, 128), 0)
    blocks = []
    for side in range(2):
        corner = jnp.zeros((8, 128), jnp.float32)
        for r in range(2):
            start = r * 128 + 112 * side
            tile = cross_ref[start : start + 16].astype(jnp.float32)
            for k in range(2):
                at = 14 * side + k
                corner = jnp.where(place == 2 * r + k, tile[at : at + 1], corner)
        for k in range(3):
            corner = jnp.where(place == 4 + k, sums[k], corner)
        blocks.append(jnp.concatenate([corner, packed(planes, 8 * side)], axis=0))
    n_x = 4
    for peer in range(n_x):
        chosen = jnp.where(at_ref[4] == peer, blocks[1], blocks[0]).astype(jnp.bfloat16)
        for group in range(sent_ref.shape[0] // n_x):
            sent_ref[group * n_x + peer] = chosen


def sides_of(at_ref):
    return (
        at_ref[0] == 0,
        jnp.where(at_ref[1] == 0, 0.0, 1.0),
        jnp.where(at_ref[2] == 0, 0.0, 1.0),
    )


def fill(rhs_ref, weight_ref):
    for a in range(3):
        for c in range(3):
            rhs_ref[a * 128 : a * 128 + 128, c * 128 : c * 128 + 128] = weight_ref[a, c]


def convolved(ext_ref, rhs_ref, bias, start, group):
    lhs = jnp.concatenate(
        [ext_ref[pl.ds(start + a, group)].reshape(group * WIDE, 128) for a in range(3)], axis=1
    )
    out = jnp.dot(lhs, rhs_ref[...], preferred_element_type=jnp.float32)
    rows = []
    for j in range(group):
        part = out[j * WIDE : (j + 1) * WIDE]
        rows.append(
            pltpu.roll(part[:, 0:128], 1, 0)
            + part[:, 128:256]
            + pltpu.roll(part[:, 256:384], WIDE - 1, 0)
            + bias
        )
    return rows


def slimmed(row):
    place = lax.broadcasted_iota(jnp.int32, (8, 128), 0)
    edge = jnp.where(place < 4, row[128:136], row[136:144])
    return jnp.concatenate([0.5 * row[0:128], 0.5 * edge], axis=0)


def forward_kernel(
    at_ref, hidden_ref, planes_ref, cross_ref, pair_ref, near_ref, weight_ref, bias_ref, proj_ref,
    alpha_ref, beta_ref,
    ext_ref, preact_ref, side_ref, rhs_ref,
):
    rows = hidden_ref.shape[0]
    n_x = near_ref.shape[0] // 2
    core, left, right = at_ref[0], at_ref[3], at_ref[4]
    upper, keep_above, keep_below = sides_of(at_ref)
    zero = jnp.zeros((), jnp.bfloat16)
    for k in range(2):
        cross = cross_ref[k * 128 : k * 128 + 128]
        pair = pair_ref[k * 128 : k * 128 + 128]
        ext_ref[k, 0:128] = jnp.where(keep_above > 0.0, jnp.where(upper, cross, pair), zero)
        ext_ref[k + rows + 2, 0:128] = jnp.where(
            keep_below > 0.0, jnp.where(upper, pair, cross), zero
        )
    ext_ref[2 : rows + 2, 0:128] = hidden_ref[...]
    place = lax.broadcasted_iota(jnp.int32, (WIDE - 128, 128), 0)
    tiles = [jnp.zeros((WIDE - 128, 128), jnp.float32) for _ in range(rows + 4)]
    second = []
    for side, base in ((right, 0), (left, WIDE - 130)):
        own = near_ref[core * n_x + side].astype(jnp.float32)
        other = near_ref[(1 - core) * n_x + side].astype(jnp.float32)
        for k in range(2):
            for r in range(rows + 4):
                at = r - 2
                if r < 2:
                    at = k * 16 + rows - 2 + r
                    row = other[at : at + 1] * keep_above
                elif r >= rows + 2:
                    at = k * 16 + r - rows - 2
                    row = other[at : at + 1] * keep_below
                else:
                    row = own[k * 16 + at : k * 16 + at + 1]
                tiles[r] = jnp.where(place == base + k, row, tiles[r])
        above = jnp.where(upper, 0.0, other[40:48] * keep_above)
        below = jnp.where(upper, other[32:40] * keep_below, 0.0)
        second.append(jnp.concatenate([above, own[32:48], below], axis=0))
    for r in range(rows + 4):
        ext_ref[r, 128:WIDE] = tiles[r].astype(jnp.bfloat16)
    cross = cross_ref[256:304].astype(jnp.float32)
    pair = pair_ref[256:304].astype(jnp.float32)
    above = jnp.where(upper, cross, pair) * keep_above
    below = jnp.where(upper, pair, cross) * keep_below
    planes = []
    for k in range(PLANES):
        at = k * 8
        tile = unpacked(second[0], second[1], k)
        planes.append(
            jnp.concatenate(
                [above[at : at + 8], planes_ref[k], below[at : at + 8], tile], axis=0
            )
        )
    side_ref[0 : 2 * PACK] = planes[0] + planes[1] + planes[2]
    side_ref[2 * PACK : 4 * PACK] = planes[3] + planes[4]
    fill(rhs_ref, weight_ref)
    bias = bias_ref[...]
    steps = [full(ref[k]) for ref in (alpha_ref, beta_ref) for k in range(ITERS)]
    params = [bias, proj_ref[...], *steps, full(0.0), full(0.0)]
    side_ref[4 * PACK : 4 * PACK + 16] = jnp.concatenate(params, axis=0)
    group = 4
    shift = jnp.where(upper, 2, 0)
    for g in range(0, rows, group):
        for j, row in enumerate(convolved(ext_ref, rhs_ref, bias, g + shift, group)):
            preact_ref[g + j] = slimmed(row)


def backward_kernel(
    at_ref, got_ref, kernel_ref, side_ref, preact_ref, early_ref,
    grad_ref, sent_ref, ext_ref,
    moved_ref, weight_ref, rhs_ref, fixed_ref,
):
    rows = grad_ref.shape[0] - 2
    n_x = 4
    fields = side_ref[0 : 4 * PACK]
    fields = (fields[0 : 2 * PACK], fields[2 * PACK : 4 * PACK])
    params = side_ref[4 * PACK : 4 * PACK + 16]
    left, right = at_ref[3], at_ref[4]
    upper, keep_above, keep_below = sides_of(at_ref)
    keep_cross = jnp.where(upper, keep_above, keep_below)
    place = lax.broadcasted_iota(jnp.int32, (WIDE - 128, 128), 0)
    tiles = [jnp.zeros((WIDE - 128, 128), jnp.float32) for _ in range(2)]
    second = []
    for side, base in ((right, 0), (left, WIDE - 130)):
        corner = got_ref[at_ref[5] * n_x + side].astype(jnp.float32) * keep_cross
        for r in range(2):
            for k in range(2):
                row = corner[2 * r + k : 2 * r + k + 1]
                tiles[r] = jnp.where(place == base + k, row, tiles[r])
        second.append(corner[8:16])
    crossed = jnp.where(upper, 0, rows + 2)
    for r in range(2):
        ext_ref[crossed + r, 128:WIDE] = tiles[r].astype(jnp.bfloat16)
    fill(rhs_ref, kernel_ref)
    again = jnp.where(upper, 0, rows)
    for g, row in enumerate(convolved(ext_ref, rhs_ref, params[0:1], again, 2)):
        fixed_ref[g] = slimmed(row)
    corner = [unpacked(second[0], second[1], k) for k in range(PLANES)]
    corner = (corner[0] + corner[1] + corner[2], corner[3] + corner[4])
    start, wet_depth = [
        jnp.concatenate(
            [
                fields[k][0:PACK],
                fields[k][PACK : PACK + 8] + jnp.where(upper, corner[k], 0.0),
                fields[k][PACK + 8 : 2 * PACK - 8],
                fields[k][2 * PACK - 8 : 2 * PACK] + jnp.where(upper, 0.0, corner[k]),
            ],
            axis=0,
        )
        for k in range(2)
    ]
    lane = lax.broadcasted_iota(jnp.int32, (2 * PACK, 128), 1)
    mask = jnp.where(wet_depth > 0.0, 1.0, 0.0)

    def other_half(field):
        parts = [field[k * PACK : (k + 1) * PACK] for k in range(field.shape[0] // PACK)]
        swapped = []
        for k in range(0, len(parts), 2):
            swapped += [parts[k + 1], parts[k]]
        return jnp.concatenate(swapped, axis=0)

    def beside(field):
        count = field.shape[0]
        lanes = lane if count == 2 * PACK else jnp.concatenate([lane, lane], axis=0)
        up = pltpu.roll(field, 1, 0)
        down = pltpu.roll(field, count - 1, 0)
        from_left = pltpu.roll(field, 1, 1)
        from_left = jnp.where(lanes == 0, other_half(from_left), from_left)
        from_right = pltpu.roll(field, 127, 1)
        from_right = jnp.where(lanes == 127, other_half(from_right), from_right)
        return up, down, from_left, from_right

    weights = [
        0.5 * (near_mask * wet_depth + mask * near_depth)
        for near_mask, near_depth in zip(beside(mask), beside(wet_depth))
    ]
    diagonal = helm_coef * mask + weights[0] + weights[1] + weights[2] + weights[3]
    weights = [jnp.concatenate([w, w], axis=0) for w in weights]
    diagonal = jnp.concatenate([diagonal, diagonal], axis=0)
    residual = jnp.concatenate([start, mask], axis=0)
    direction = residual
    result = jnp.zeros_like(residual)
    for k in range(ITERS):
        result = result + params[2 + k : 3 + k] * direction
        if k + 1 < ITERS:
            applied = diagonal * direction
            for w, near in zip(weights, beside(direction)):
                applied = applied - w * near
            residual = residual - params[2 + k : 3 + k] * applied
            direction = residual + params[8 + k : 9 + k] * direction
    result = result * jnp.concatenate([mask, mask], axis=0)
    sums = jnp.sum(got_ref[...].astype(jnp.float32)[:, 0:8], axis=0)
    sums = sums[4:5] + sums[5:6] + sums[6:7]
    mean = jnp.broadcast_to(sums[:, 0:1], (1, 128)) / jnp.broadcast_to(sums[:, 127:128], (1, 128))
    force = result.T
    force = force - mean * pltpu.roll(force, 64, 1)
    proj = 0.5 * params[1:2]
    shift = jnp.where(upper, 2, 0)
    sublane = lax.broadcasted_iota(jnp.int32, (8, 1), 0)
    sum_bias = jnp.zeros((8, 128), jnp.float32)
    sum_proj = jnp.zeros((8, 128), jnp.float32)
    for g in range(rows + 2):
        at = g + 7
        edge = jnp.where(
            sublane < 4,
            force[0:8, PACK + at : PACK + at + 1],
            force[120:128, PACK + at : PACK + at + 1],
        )
        for q, size in ((0, 48), (48, 48), (96, 32), (128, 8)):
            column = edge if q == 128 else force[q : q + size, at : at + 1]
            column = jnp.broadcast_to(column, (size, 128))
            if g < 2:
                preact = jnp.where(upper, fixed_ref[g, q : q + size], preact_ref[g, q : q + size])
            elif g >= rows:
                preact = jnp.where(
                    upper, preact_ref[g - 2, q : q + size], fixed_ref[g - rows, q : q + size]
                )
            else:
                preact = preact_ref[g - shift, q : q + size]
            turn = jnp.tanh(preact)
            bent = preact * turn
            active = preact + bent
            slope_act = (1.0 + turn) * ((1.0 + preact) - bent)
            grad = column * proj * slope_act
            if q == 128:
                grad_ref[g, 128:WIDE] = jnp.concatenate([grad, grad], axis=0).astype(jnp.bfloat16)
                continue
            grad = grad.astype(jnp.bfloat16)
            grad_ref[g, q : q + size] = grad
            if 1 <= g <= rows:
                own = grad.astype(jnp.float32)
                drawn = active * column
                for k in range(size // 8):
                    sum_bias = sum_bias + own[k * 8 : k * 8 + 8]
                    sum_proj = sum_proj + drawn[k * 8 : k * 8 + 8]
    for g in range(1, rows + 1):
        own = grad_ref[g, 0:128].astype(jnp.float32)
        own = jnp.concatenate([own, jnp.zeros((WIDE - 128, 128), jnp.float32)], axis=0)
        moved_ref[g - 1, :, 0:128] = pltpu.roll(own, WIDE - 1, 0).astype(jnp.bfloat16)
        moved_ref[g - 1, :, 128:256] = own.astype(jnp.bfloat16)
        moved_ref[g - 1, :, 256:384] = pltpu.roll(own, 1, 0).astype(jnp.bfloat16)
    to = lax.broadcasted_iota(jnp.int32, (128, 128), 0)
    of = lax.broadcasted_iota(jnp.int32, (128, 128), 1)
    source = (
        to // 32 * 32 + to // 2 % 2 * 16 + to // 16 % 2 * 8 + to // 4 % 4 * 2 + to % 2
    )
    order = jnp.where(of == source, 1.0, 0.0).astype(jnp.bfloat16)
    moved = moved_ref[...].reshape(rows * WIDE, 384)
    cells = jnp.concatenate(
        [ext_ref[a + 1 : a + 1 + rows].reshape(rows * WIDE, 128) for a in range(3)], axis=1
    )
    whole = lax.dot_general(
        cells, moved, (((0,), (0,)), ((), ())), preferred_element_type=jnp.float32
    )
    for a in range(3):
        out = whole[a * 128 : a * 128 + 128]
        out = jnp.dot(
            order, out.astype(jnp.bfloat16), preferred_element_type=jnp.float32
        )
        for c in range(3):
            weight_ref[a * 3 + c] = out[:, c * 128 : c * 128 + 128]
    vectors = jnp.concatenate(
        [jnp.sum(sum_bias, axis=0, keepdims=True), jnp.sum(sum_proj, axis=0, keepdims=True)], axis=0
    )
    vectors = jnp.concatenate(pieces_of(vectors, 2) + [jnp.zeros((4, 128), jnp.float32)], axis=0)
    vectors = pltpu.roll(vectors, 4, 0)
    low = lax.broadcasted_iota(jnp.int32, (8, 128), 0) < 4

    for t in range(16):
        start = t * 8
        blocks = ([], [])
        for k in range(0, 9, 2):
            one = weight_ref[k, start : start + 8]
            two = weight_ref[k + 1, start : start + 8] if k < 8 else vectors
            two_low = pltpu.roll(two, 4, 0) if k < 8 else vectors
            blocks[0].append(jnp.where(low, one, two_low))
            blocks[1].append(jnp.where(low, pltpu.roll(one, 4, 0), two))
        for x in range(2):
            sent_ref[t * 2 + x] = jnp.concatenate(blocks[x], axis=0).astype(jnp.bfloat16)


def middle_kernel(got_ref, sent_ref):
    total = jnp.sum(got_ref[...].astype(jnp.float32), axis=0)
    vectors = total[36:38] + total[38:40]
    vectors = jnp.concatenate(pieces_of(vectors, 2) + [jnp.zeros((2, 128), jnp.float32)], axis=0)
    peers = sent_ref.shape[0] // 2
    for z in range(2):
        block = [total[4 * k + 2 * z : 4 * k + 2 * z + 2] for k in range(9)]
        block = jnp.concatenate(block + [vectors], axis=0)
        block = block.astype(jnp.bfloat16)
        for d in range(peers):
            sent_ref[z * peers + d] = block


def last_kernel(scale, got_ref, weight_ref, bias_ref, proj_ref):
    total = jnp.sum(got_ref[...].astype(jnp.float32), axis=0) * scale
    for k in range(9):
        weight_ref[k // 3, k % 3] = total[k * 2 : k * 2 + 2]
    bias_ref[...] = total[18:19] + total[20:21]
    proj_ref[...] = total[19:20] + total[21:22]


def input_kernel(grad_ref, weight_ref, out_ref, rhs_ref):
    rows = out_ref.shape[0]
    for a in range(3):
        for c in range(3):
            rhs_ref[c * 128 : c * 128 + 128, a * 128 : a * 128 + 128] = weight_ref[a, c]
    group = 4
    for y in range(0, rows, group):
        lhs = jnp.concatenate(
            [
                grad_ref[y - a + 2 : y - a + 2 + group].reshape(group * WIDE, 128)
                for a in range(3)
            ],
            axis=1,
        )
        out = lax.dot_general(
            lhs, rhs_ref[...], (((1,), (1,)), ((), ())), preferred_element_type=jnp.float32
        )
        for j in range(group):
            part = out[j * WIDE : (j + 1) * WIDE]
            total = (
                pltpu.roll(part[:, 0:128], WIDE - 1, 0)
                + part[:, 128:256]
                + pltpu.roll(part[:, 256:384], 1, 0)
            )
            out_ref[y + j] = total[0:128].astype(jnp.bfloat16)


def call(kernel, shapes, scratch, in_specs, args, out_specs=None, aliases={}):
    return pl.pallas_call(
        kernel,
        out_shape=shapes,
        in_specs=in_specs,
        out_specs=jax.tree.map(lambda _: VMEM, shapes) if out_specs is None else out_specs,
        scratch_shapes=scratch,
        input_output_aliases=aliases,
        compiler_params=pltpu.CompilerParams(vmem_limit_bytes=40 * 1024 * 1024),
    )(*args)


def shape(dims, dtype):
    return jax.ShapeDtypeStruct(dims, dtype)


def shards(
    hidden_in, conv_weight, conv_bias, proj_weight, ocean_depth, sea_mask,
    step_alpha, step_beta, surface_cotangent,
):
    wide, narrow = jnp.float32, jnp.bfloat16
    rows = hidden_in.shape[1]
    hidden = hidden_in[0]
    n_x = lax.axis_size("lon")
    n_lat = lax.axis_size(LAT)
    n_all = lax.axis_size(("lat_0", "lat_2", "lon"))
    n_z = lax.axis_size(("lat_1", "dp"))
    lat, me = lax.axis_index(LAT), lax.axis_index("lon")
    row_group = lax.axis_index(("lat_0", "lat_2"))
    at = jnp.stack(
        [lat % 2, lat, n_lat - 1 - lat, (me + n_x - 1) % n_x, (me + 1) % n_x, row_group]
    ).astype(jnp.int32)
    mask = sea_mask.astype(wide)
    fields = jnp.stack([mask * surface_cotangent[0], mask * ocean_depth])
    cross, pair, near, planes, sums = call(
        first_kernel,
        (
            shape((304, 128), narrow),
            shape((304, 128), narrow),
            shape((2 * n_x, NEAR, 128), narrow),
            shape((PLANES, rows, 128), wide),
            shape((2, 128), wide),
        ),
        [],
        [SMEM] + [VMEM] * 2,
        (at, hidden, fields),
    )
    odd = [(i, (i + 1) % n_lat) for i in range(1, n_lat, 2)]
    odd = odd + [(j, i) for i, j in odd]
    cross = lax.ppermute(cross, LAT, odd)
    pair = lax.ppermute(pair, "lat_2", [(0, 1), (1, 0)])
    near = lax.all_to_all(near, ("lat_2", "lon"), 0, 0, tiled=True)
    sent = call(
        second_kernel, shape((n_all, 16, 128), narrow), [], [SMEM] + [VMEM] * 2, (at, sums, cross)
    )
    got = lax.all_to_all(sent, ("lat_0", "lat_2", "lon"), 0, 0, tiled=True)
    early, preact, side = call(
        forward_kernel,
        (
            shape((rows + 4, WIDE, 128), narrow),
            shape((rows, SLIM, 128), wide),
            shape((4 * PACK + 16, 128), wide),
        ),
        [pltpu.VMEM((384, 384), narrow)],
        [SMEM] + [VMEM] * 8 + [SMEM] * 2,
        (
            at, hidden, planes, cross, pair, near, conv_weight, conv_bias[None],
            proj_weight[None], step_alpha, step_beta,
        ),
    )
    grad, sent, _ = call(
        backward_kernel,
        (
            shape((rows + 2, WIDE, 128), narrow),
            shape((n_all, 40, 128), narrow),
            shape((rows + 4, WIDE, 128), narrow),
        ),
        [
            pltpu.VMEM((rows, WIDE, 384), narrow),
            pltpu.VMEM((9, 128, 128), wide),
            pltpu.VMEM((384, 384), narrow),
            pltpu.VMEM((2, SLIM, 128), wide),
        ],
        [SMEM] + [VMEM] * 5,
        (at, got, conv_weight, side, preact, early),
        None,
        {5: 2},
    )
    got = lax.all_to_all(sent, ("lat_0", "lat_2", "lon"), 0, 0, tiled=True)
    sent = call(middle_kernel, shape((n_z, 24, 128), narrow), [], [VMEM], (got,))
    got = lax.all_to_all(sent, ("lat_1", "dp"), 0, 0, tiled=True)
    grad_hidden = call(
        input_kernel,
        shape((rows, 128, 128), narrow),
        [pltpu.VMEM((384, 384), narrow)],
        [VMEM] * 2,
        (grad, conv_weight),
    )
    cells = rows * 128 * lax.axis_size("dp") * n_lat * n_x
    own_weight, total_bias, total_proj = call(
        functools.partial(last_kernel, 1.0 / math.sqrt(cells)),
        (shape((3, 3, 2, 128), wide), shape((1, 128), wide), shape((1, 128), wide)),
        [],
        [VMEM],
        (got,),
    )
    return grad_hidden[None], own_weight.transpose(2, 0, 1, 3), total_bias[0], total_proj[0]


def solution(mesh):
    split = Mesh(
        mesh.devices.reshape(mesh.shape["dp"], 4, 2, 2, mesh.shape["lon"]),
        ("dp", "lat_0", "lat_1", "lat_2", "lon"),
    )
    placed = (
        P("dp", LAT, "lon", None),
        P(),
        P(),
        P(),
        P(LAT, "lon"),
        P(LAT, "lon"),
        P(),
        P(),
        P("dp", LAT, "lon"),
    )
    return jax.shard_map(
        shards,
        mesh=split,
        in_specs=placed,
        out_specs=(P("dp", LAT, "lon", None), P(LAT_LON, None, None, None), P(), P()),
        check_vma=False,
    )
```

```python
import functools
import math

import jax
import jax.numpy as jnp
from jax import lax
from jax.experimental import pallas as pl
from jax.experimental.pallas import tpu as pltpu
from jax.sharding import Mesh
from jax.sharding import PartitionSpec as P

ITERS = 6
LAT_LON = ("lat_0", "lat_1", "lat_2", "lon")
LAT = ("lat_0", "lat_1", "lat_2")
WIDE = 144
SLIM = 136
PACK = 32
PLANES = 5
NEAR = 48

helm_coef = 0.5
VMEM = pl.BlockSpec(memory_space=pltpu.VMEM)
SMEM = pl.BlockSpec(memory_space=pltpu.SMEM)
HBM = pl.BlockSpec(memory_space=pltpu.HBM)


def rounded(values):
    return values.astype(jnp.bfloat16).astype(jnp.float32)


def pieces_of(values, count):
    out = []
    for _ in range(count):
        piece = rounded(values)
        out.append(piece)
        values = values - piece
    return out


def full(value):
    return jnp.full((1, 128), value, jnp.float32)


def packed(planes, shift):
    rows = planes[0].shape[0]
    lane = lax.broadcasted_iota(jnp.int32, (rows, 128), 1) // 8
    out = jnp.zeros((rows, 128), jnp.float32)
    for k, plane in enumerate(planes):
        by = (8 * k + shift) % 128
        out = jnp.where(lane == k, pltpu.roll(plane, by, 1) if by else plane, out)
    return out


def edge_columns(load, rows):
    place = lax.broadcasted_iota(jnp.int32, (8, 128), 0)
    columns = [[jnp.zeros((8, 128), jnp.float32) for _ in range(rows // 8)] for _ in range(4)]
    for r in range(rows):
        head = load(r, 0).astype(jnp.float32)
        tail = load(r, 112).astype(jnp.float32)
        for k, row in enumerate((head[0:1], head[1:2], tail[14:15], tail[15:16])):
            columns[k][r // 8] = jnp.where(place == r % 8, row, columns[k][r // 8])
    return columns


def unpacked(beyond, before, k):
    near = lax.broadcasted_iota(jnp.int32, beyond.shape, 1)
    if k:
        beyond = pltpu.roll(beyond, 128 - 8 * k, 1)
    before = pltpu.roll(before, 120 - 8 * k, 1)
    return jnp.where(near < 8, beyond, jnp.where(near >= 120, before, 0.0))


def near_rows(planes, top):
    rows = planes[0].shape[0]
    return [jnp.where(top, p[0:8], p[rows - 8 : rows]) for p in planes]


def first_kernel(at_ref, hidden_ref, fields_ref, cross_ref, planes_ref, sums_ref):
    upper = at_ref[0] == 0
    wet, wet_depth = fields_ref[0], fields_ref[1]
    planes = pieces_of(wet, 3) + pieces_of(wet_depth, 2)
    summed = full(jnp.sum(wet))
    counted = full(jnp.sum(jnp.where(wet_depth > 0.0, 1.0, 0.0)))
    sums_ref[0:1] = summed
    sums_ref[1:2] = counted
    sums = pieces_of(summed, 3) + pieces_of(counted, 3)
    sums = jnp.concatenate(sums + [jnp.zeros((2, 128), jnp.float32)], axis=0)
    for k in range(PLANES):
        planes_ref[k] = planes[k]
    cross_ref[0:256] = hidden_ref[...].reshape(256, 128)
    near = near_rows(planes, upper) + [sums]
    for k in range(0, 6, 2):
        tile = jnp.concatenate(near[k : k + 2], axis=0)
        cross_ref[256 + k * 8 : 272 + k * 8] = tile.astype(jnp.bfloat16)


def edges_kernel(at_ref, hidden_ref, planes_ref, pair_ref, near_ref):
    rows = hidden_ref.shape[0]
    upper = at_ref[0] == 0
    planes = [planes_ref[k] for k in range(PLANES)]
    start = jnp.where(upper, rows - 2, 0)
    pair_ref[0:256] = hidden_ref[pl.ds(start, 2)].reshape(256, 128)
    near = near_rows(planes + planes[:1], jnp.logical_not(upper))
    for k in range(0, 6, 2):
        tile = jnp.concatenate(near[k : k + 2], axis=0)
        pair_ref[256 + k * 8 : 272 + k * 8] = tile.astype(jnp.bfloat16)
    columns = edge_columns(lambda r, at: hidden_ref[r, at : at + 16], rows)
    head = jnp.concatenate(columns[0] + columns[1] + [packed(planes, 0)], axis=0)
    tail = jnp.concatenate(columns[2] + columns[3] + [packed(planes, 8)], axis=0)
    n_x = near_ref.shape[0] // 2
    for peer in range(n_x):
        chosen = jnp.where(at_ref[4] == peer, tail, head).astype(jnp.bfloat16)
        near_ref[peer] = chosen
        near_ref[n_x + peer] = chosen


def second_kernel(at_ref, sums_ref, cross_ref, sent_ref):
    tiles = [cross_ref[256 + k * 16 : 272 + k * 16].astype(jnp.float32) for k in range(3)]
    planes = [tiles[k // 2][k % 2 * 8 : k % 2 * 8 + 8] for k in range(PLANES)]
    got = tiles[2][8:16]
    summed = sums_ref[0:1] + got[0:1] + got[1:2] + got[2:3]
    counted = sums_ref[1:2] + got[3:4] + got[4:5] + got[5:6]
    lane = lax.broadcasted_iota(jnp.int32, (1, 128), 1)
    sums = pieces_of(jnp.where(lane < 64, summed, counted), 3)
    place = lax.broadcasted_iota(jnp.int32, (8, 128), 0)
    blocks = []
    for side in range(2):
        corner = jnp.zeros((8, 128), jnp.float32)
        for r in range(2):
            start = r * 128 + 112 * side
            tile = cross_ref[start : start + 16].astype(jnp.float32)
            for k in range(2):
                at = 14 * side + k
                corner = jnp.where(place == 2 * r + k, tile[at : at + 1], corner)
        for k in range(3):
            corner = jnp.where(place == 4 + k, sums[k], corner)
        blocks.append(jnp.concatenate([corner, packed(planes, 8 * side)], axis=0))
    n_x = 4
    for peer in range(n_x):
        chosen = jnp.where(at_ref[4] == peer, blocks[1], blocks[0]).astype(jnp.bfloat16)
        for group in range(sent_ref.shape[0] // n_x):
            sent_ref[group * n_x + peer] = chosen


def sides_of(at_ref):
    return (
        at_ref[0] == 0,
        jnp.where(at_ref[1] == 0, 0.0, 1.0),
        jnp.where(at_ref[2] == 0, 0.0, 1.0),
    )


def fill(rhs_ref, weight_ref):
    for a in range(3):
        for c in range(3):
            rhs_ref[a * 128 : a * 128 + 128, c * 128 : c * 128 + 128] = weight_ref[a, c]


def convolved(ext_ref, rhs_ref, bias, start, group):
    lhs = jnp.concatenate(
        [ext_ref[pl.ds(start + a, group)].reshape(group * WIDE, 128) for a in range(3)], axis=1
    )
    out = jnp.dot(lhs, rhs_ref[...], preferred_element_type=jnp.float32)
    rows = []
    for j in range(group):
        part = out[j * WIDE : (j + 1) * WIDE]
        rows.append(
            pltpu.roll(part[:, 0:128], 1, 0)
            + part[:, 128:256]
            + pltpu.roll(part[:, 256:384], WIDE - 1, 0)
            + bias
        )
    return rows


def slimmed(row):
    place = lax.broadcasted_iota(jnp.int32, (8, 128), 0)
    edge = jnp.where(place < 4, row[128:136], row[136:144])
    return jnp.concatenate([0.5 * row[0:128], 0.5 * edge], axis=0)


def forward_kernel(
    at_ref, hidden_ref, planes_ref, cross_ref, pair_ref, near_ref, weight_ref, bias_ref, proj_ref,
    alpha_ref, beta_ref,
    ext_ref, preact_ref, side_ref, rhs_ref,
):
    rows = hidden_ref.shape[0]
    n_x = near_ref.shape[0] // 2
    core, left, right = at_ref[0], at_ref[3], at_ref[4]
    upper, keep_above, keep_below = sides_of(at_ref)
    zero = jnp.zeros((), jnp.bfloat16)
    for k in range(2):
        cross = cross_ref[k * 128 : k * 128 + 128]
        pair = pair_ref[k * 128 : k * 128 + 128]
        ext_ref[k, 0:128] = jnp.where(keep_above > 0.0, jnp.where(upper, cross, pair), zero)
        ext_ref[k + rows + 2, 0:128] = jnp.where(
            keep_below > 0.0, jnp.where(upper, pair, cross), zero
        )
    ext_ref[2 : rows + 2, 0:128] = hidden_ref[...]
    place = lax.broadcasted_iota(jnp.int32, (WIDE - 128, 128), 0)
    tiles = [jnp.zeros((WIDE - 128, 128), jnp.float32) for _ in range(rows + 4)]
    second = []
    for side, base in ((right, 0), (left, WIDE - 130)):
        own = near_ref[core * n_x + side].astype(jnp.float32)
        other = near_ref[(1 - core) * n_x + side].astype(jnp.float32)
        for k in range(2):
            for r in range(rows + 4):
                at = r - 2
                if r < 2:
                    at = k * 16 + rows - 2 + r
                    row = other[at : at + 1] * keep_above
                elif r >= rows + 2:
                    at = k * 16 + r - rows - 2
                    row = other[at : at + 1] * keep_below
                else:
                    row = own[k * 16 + at : k * 16 + at + 1]
                tiles[r] = jnp.where(place == base + k, row, tiles[r])
        above = jnp.where(upper, 0.0, other[40:48] * keep_above)
        below = jnp.where(upper, other[32:40] * keep_below, 0.0)
        second.append(jnp.concatenate([above, own[32:48], below], axis=0))
    for r in range(rows + 4):
        ext_ref[r, 128:WIDE] = tiles[r].astype(jnp.bfloat16)
    cross = cross_ref[256:304].astype(jnp.float32)
    pair = pair_ref[256:304].astype(jnp.float32)
    above = jnp.where(upper, cross, pair) * keep_above
    below = jnp.where(upper, pair, cross) * keep_below
    planes = []
    for k in range(PLANES):
        at = k * 8
        tile = unpacked(second[0], second[1], k)
        planes.append(
            jnp.concatenate(
                [above[at : at + 8], planes_ref[k], below[at : at + 8], tile], axis=0
            )
        )
    side_ref[0 : 2 * PACK] = planes[0] + planes[1] + planes[2]
    side_ref[2 * PACK : 4 * PACK] = planes[3] + planes[4]
    fill(rhs_ref, weight_ref)
    bias = bias_ref[...]
    steps = [full(ref[k]) for ref in (alpha_ref, beta_ref) for k in range(ITERS)]
    params = [bias, proj_ref[...], *steps, full(0.0), full(0.0)]
    side_ref[4 * PACK : 4 * PACK + 16] = jnp.concatenate(params, axis=0)
    group = 4
    shift = jnp.where(upper, 2, 0)
    for g in range(0, rows, group):
        for j, row in enumerate(convolved(ext_ref, rhs_ref, bias, g + shift, group)):
            preact_ref[g + j] = slimmed(row)


def backward_kernel(
    at_ref, got_ref, kernel_ref, side_ref, preact_ref, early_ref,
    grad_ref, sent_ref, ext_ref,
    moved_ref, weight_ref, rhs_ref, fixed_ref,
):
    rows = grad_ref.shape[0] - 2
    n_x = 4
    fields = side_ref[0 : 4 * PACK]
    fields = (fields[0 : 2 * PACK], fields[2 * PACK : 4 * PACK])
    params = side_ref[4 * PACK : 4 * PACK + 16]
    left, right = at_ref[3], at_ref[4]
    upper, keep_above, keep_below = sides_of(at_ref)
    keep_cross = jnp.where(upper, keep_above, keep_below)
    place = lax.broadcasted_iota(jnp.int32, (WIDE - 128, 128), 0)
    tiles = [jnp.zeros((WIDE - 128, 128), jnp.float32) for _ in range(2)]
    second = []
    for side, base in ((right, 0), (left, WIDE - 130)):
        corner = got_ref[at_ref[5] * n_x + side].astype(jnp.float32) * keep_cross
        for r in range(2):
            for k in range(2):
                row = corner[2 * r + k : 2 * r + k + 1]
                tiles[r] = jnp.where(place == base + k, row, tiles[r])
        second.append(corner[8:16])
    crossed = jnp.where(upper, 0, rows + 2)
    for r in range(2):
        ext_ref[crossed + r, 128:WIDE] = tiles[r].astype(jnp.bfloat16)
    fill(rhs_ref, kernel_ref)
    again = jnp.where(upper, 0, rows)
    for g, row in enumerate(convolved(ext_ref, rhs_ref, params[0:1], again, 2)):
        fixed_ref[g] = slimmed(row)
    corner = [unpacked(second[0], second[1], k) for k in range(PLANES)]
    corner = (corner[0] + corner[1] + corner[2], corner[3] + corner[4])
    start, wet_depth = [
        jnp.concatenate(
            [
                fields[k][0:PACK],
                fields[k][PACK : PACK + 8] + jnp.where(upper, corner[k], 0.0),
                fields[k][PACK + 8 : 2 * PACK - 8],
                fields[k][2 * PACK - 8 : 2 * PACK] + jnp.where(upper, 0.0, corner[k]),
            ],
            axis=0,
        )
        for k in range(2)
    ]
    lane = lax.broadcasted_iota(jnp.int32, (2 * PACK, 128), 1)
    mask = jnp.where(wet_depth > 0.0, 1.0, 0.0)

    def other_half(field):
        parts = [field[k * PACK : (k + 1) * PACK] for k in range(field.shape[0] // PACK)]
        swapped = []
        for k in range(0, len(parts), 2):
            swapped += [parts[k + 1], parts[k]]
        return jnp.concatenate(swapped, axis=0)

    def beside(field):
        count = field.shape[0]
        lanes = lane if count == 2 * PACK else jnp.concatenate([lane, lane], axis=0)
        up = pltpu.roll(field, 1, 0)
        down = pltpu.roll(field, count - 1, 0)
        from_left = pltpu.roll(field, 1, 1)
        from_left = jnp.where(lanes == 0, other_half(from_left), from_left)
        from_right = pltpu.roll(field, 127, 1)
        from_right = jnp.where(lanes == 127, other_half(from_right), from_right)
        return up, down, from_left, from_right

    weights = [
        0.5 * (near_mask * wet_depth + mask * near_depth)
        for near_mask, near_depth in zip(beside(mask), beside(wet_depth))
    ]
    diagonal = helm_coef * mask + weights[0] + weights[1] + weights[2] + weights[3]
    weights = [jnp.concatenate([w, w], axis=0) for w in weights]
    diagonal = jnp.concatenate([diagonal, diagonal], axis=0)
    residual = jnp.concatenate([start, mask], axis=0)
    direction = residual
    result = jnp.zeros_like(residual)
    for k in range(ITERS):
        result = result + params[2 + k : 3 + k] * direction
        if k + 1 < ITERS:
            applied = diagonal * direction
            for w, near in zip(weights, beside(direction)):
                applied = applied - w * near
            residual = residual - params[2 + k : 3 + k] * applied
            direction = residual + params[8 + k : 9 + k] * direction
    result = result * jnp.concatenate([mask, mask], axis=0)
    sums = jnp.sum(got_ref[...].astype(jnp.float32)[:, 0:8], axis=0)
    sums = sums[4:5] + sums[5:6] + sums[6:7]
    mean = jnp.broadcast_to(sums[:, 0:1], (1, 128)) / jnp.broadcast_to(sums[:, 127:128], (1, 128))
    force = result.T
    force = force - mean * pltpu.roll(force, 64, 1)
    proj = 0.5 * params[1:2]
    shift = jnp.where(upper, 2, 0)
    sublane = lax.broadcasted_iota(jnp.int32, (8, 1), 0)
    sum_bias = jnp.zeros((8, 128), jnp.float32)
    sum_proj = jnp.zeros((8, 128), jnp.float32)
    for g in range(rows + 2):
        at = g + 7
        edge = jnp.where(
            sublane < 4,
            force[0:8, PACK + at : PACK + at + 1],
            force[120:128, PACK + at : PACK + at + 1],
        )
        for q, size in ((0, 48), (48, 48), (96, 32), (128, 8)):
            column = edge if q == 128 else force[q : q + size, at : at + 1]
            column = jnp.broadcast_to(column, (size, 128))
            if g < 2:
                preact = jnp.where(upper, fixed_ref[g, q : q + size], preact_ref[g, q : q + size])
            elif g >= rows:
                preact = jnp.where(
                    upper, preact_ref[g - 2, q : q + size], fixed_ref[g - rows, q : q + size]
                )
            else:
                preact = preact_ref[g - shift, q : q + size]
            turn = jnp.tanh(preact)
            bent = preact * turn
            active = preact + bent
            slope_act = (1.0 + turn) * ((1.0 + preact) - bent)
            grad = column * proj * slope_act
            if q == 128:
                grad_ref[g, 128:WIDE] = jnp.concatenate([grad, grad], axis=0).astype(jnp.bfloat16)
                continue
            grad = grad.astype(jnp.bfloat16)
            grad_ref[g, q : q + size] = grad
            if 1 <= g <= rows:
                own = grad.astype(jnp.float32)
                drawn = active * column
                for k in range(size // 8):
                    sum_bias = sum_bias + own[k * 8 : k * 8 + 8]
                    sum_proj = sum_proj + drawn[k * 8 : k * 8 + 8]
    for g in range(1, rows + 1):
        own = grad_ref[g, 0:128].astype(jnp.float32)
        own = jnp.concatenate([own, jnp.zeros((WIDE - 128, 128), jnp.float32)], axis=0)
        moved_ref[g - 1, :, 0:128] = pltpu.roll(own, WIDE - 1, 0).astype(jnp.bfloat16)
        moved_ref[g - 1, :, 128:256] = own.astype(jnp.bfloat16)
        moved_ref[g - 1, :, 256:384] = pltpu.roll(own, 1, 0).astype(jnp.bfloat16)
    to = lax.broadcasted_iota(jnp.int32, (128, 128), 0)
    of = lax.broadcasted_iota(jnp.int32, (128, 128), 1)
    source = (
        to // 32 * 32 + to // 2 % 2 * 16 + to // 16 % 2 * 8 + to // 4 % 4 * 2 + to % 2
    )
    order = jnp.where(of == source, 1.0, 0.0).astype(jnp.bfloat16)
    moved = moved_ref[...].reshape(rows * WIDE, 384)
    cells = jnp.concatenate(
        [ext_ref[a + 1 : a + 1 + rows].reshape(rows * WIDE, 128) for a in range(3)], axis=1
    )
    whole = lax.dot_general(
        cells, moved, (((0,), (0,)), ((), ())), preferred_element_type=jnp.float32
    )
    for a in range(3):
        out = whole[a * 128 : a * 128 + 128]
        out = jnp.dot(
            order, out.astype(jnp.bfloat16), preferred_element_type=jnp.float32
        )
        for c in range(3):
            weight_ref[a * 3 + c] = out[:, c * 128 : c * 128 + 128]
    vectors = jnp.concatenate(
        [jnp.sum(sum_bias, axis=0, keepdims=True), jnp.sum(sum_proj, axis=0, keepdims=True)], axis=0
    )
    vectors = jnp.concatenate(pieces_of(vectors, 2) + [jnp.zeros((4, 128), jnp.float32)], axis=0)
    vectors = pltpu.roll(vectors, 4, 0)
    low = lax.broadcasted_iota(jnp.int32, (8, 128), 0) < 4

    for t in range(16):
        start = t * 8
        blocks = ([], [])
        for k in range(0, 9, 2):
            one = weight_ref[k, start : start + 8]
            two = weight_ref[k + 1, start : start + 8] if k < 8 else vectors
            two_low = pltpu.roll(two, 4, 0) if k < 8 else vectors
            blocks[0].append(jnp.where(low, one, two_low))
            blocks[1].append(jnp.where(low, pltpu.roll(one, 4, 0), two))
        for x in range(2):
            sent_ref[t * 2 + x] = jnp.concatenate(blocks[x], axis=0).astype(jnp.bfloat16)


def middle_kernel(got_ref, sent_ref):
    total = jnp.sum(got_ref[...].astype(jnp.float32), axis=0)
    vectors = total[36:38] + total[38:40]
    vectors = jnp.concatenate(pieces_of(vectors, 2) + [jnp.zeros((2, 128), jnp.float32)], axis=0)
    peers = sent_ref.shape[0] // 2
    for z in range(2):
        block = [total[4 * k + 2 * z : 4 * k + 2 * z + 2] for k in range(9)]
        block = jnp.concatenate(block + [vectors], axis=0)
        block = block.astype(jnp.bfloat16)
        for d in range(peers):
            sent_ref[z * peers + d] = block


def last_kernel(scale, got_ref, weight_ref, bias_ref, proj_ref):
    total = jnp.sum(got_ref[...].astype(jnp.float32), axis=0) * scale
    for k in range(9):
        weight_ref[k // 3, k % 3] = total[k * 2 : k * 2 + 2]
    bias_ref[...] = total[18:19] + total[20:21]
    proj_ref[...] = total[19:20] + total[21:22]


def input_kernel(grad_ref, weight_ref, out_ref, rhs_ref):
    rows = out_ref.shape[0]
    for a in range(3):
        for c in range(3):
            rhs_ref[c * 128 : c * 128 + 128, a * 128 : a * 128 + 128] = weight_ref[a, c]
    group = 4
    for y in range(0, rows, group):
        lhs = jnp.concatenate(
            [
                grad_ref[y - a + 2 : y - a + 2 + group].reshape(group * WIDE, 128)
                for a in range(3)
            ],
            axis=1,
        )
        out = lax.dot_general(
            lhs, rhs_ref[...], (((1,), (1,)), ((), ())), preferred_element_type=jnp.float32
        )
        for j in range(group):
            part = out[j * WIDE : (j + 1) * WIDE]
            total = (
                pltpu.roll(part[:, 0:128], WIDE - 1, 0)
                + part[:, 128:256]
                + pltpu.roll(part[:, 256:384], 1, 0)
            )
            out_ref[y + j] = total[0:128].astype(jnp.bfloat16)


def call(kernel, shapes, scratch, in_specs, args, out_specs=None, aliases={}):
    return pl.pallas_call(
        kernel,
        out_shape=shapes,
        in_specs=in_specs,
        out_specs=jax.tree.map(lambda _: VMEM, shapes) if out_specs is None else out_specs,
        scratch_shapes=scratch,
        input_output_aliases=aliases,
        compiler_params=pltpu.CompilerParams(vmem_limit_bytes=40 * 1024 * 1024),
    )(*args)


def shape(dims, dtype):
    return jax.ShapeDtypeStruct(dims, dtype)


def shards(
    hidden_in, conv_weight, conv_bias, proj_weight, ocean_depth, sea_mask,
    step_alpha, step_beta, surface_cotangent,
):
    wide, narrow = jnp.float32, jnp.bfloat16
    rows = hidden_in.shape[1]
    hidden = hidden_in[0]
    n_x = lax.axis_size("lon")
    n_lat = lax.axis_size(LAT)
    n_all = lax.axis_size(("lat_0", "lat_2", "lon"))
    n_z = lax.axis_size(("lat_1", "dp"))
    lat, me = lax.axis_index(LAT), lax.axis_index("lon")
    row_group = lax.axis_index(("lat_0", "lat_2"))
    at = jnp.stack(
        [lat % 2, lat, n_lat - 1 - lat, (me + n_x - 1) % n_x, (me + 1) % n_x, row_group]
    ).astype(jnp.int32)
    mask = sea_mask.astype(wide)
    fields = jnp.stack([mask * surface_cotangent[0], mask * ocean_depth])
    facing = lax.dynamic_slice_in_dim(
        hidden, jnp.where(lax.axis_index("lat_2") == 0, 0, rows - 2), 2, axis=0
    )
    cross, planes, sums = call(
        first_kernel,
        (
            shape((304, 128), narrow),
            shape((PLANES, rows, 128), wide),
            shape((2, 128), wide),
        ),
        [],
        [SMEM] + [VMEM] * 2,
        (at, facing, fields),
    )
    odd = [(i, (i + 1) % n_lat) for i in range(1, n_lat, 2)]
    odd = odd + [(j, i) for i, j in odd]
    cross = lax.ppermute(cross, LAT, odd)
    pair, near = call(
        edges_kernel,
        (shape((304, 128), narrow), shape((2 * n_x, NEAR, 128), narrow)),
        [],
        [SMEM] + [VMEM] * 2,
        (at, hidden, planes),
    )
    pair = lax.ppermute(pair, "lat_2", [(0, 1), (1, 0)])
    near = lax.all_to_all(near, ("lat_2", "lon"), 0, 0, tiled=True)
    sent = call(
        second_kernel, shape((n_all, 16, 128), narrow), [], [SMEM] + [VMEM] * 2, (at, sums, cross)
    )
    got = lax.all_to_all(sent, ("lat_0", "lat_2", "lon"), 0, 0, tiled=True)
    early, preact, side = call(
        forward_kernel,
        (
            shape((rows + 4, WIDE, 128), narrow),
            shape((rows, SLIM, 128), wide),
            shape((4 * PACK + 16, 128), wide),
        ),
        [pltpu.VMEM((384, 384), narrow)],
        [SMEM] + [VMEM] * 8 + [SMEM] * 2,
        (
            at, hidden, planes, cross, pair, near, conv_weight, conv_bias[None],
            proj_weight[None], step_alpha, step_beta,
        ),
    )
    grad, sent, _ = call(
        backward_kernel,
        (
            shape((rows + 2, WIDE, 128), narrow),
            shape((n_all, 40, 128), narrow),
            shape((rows + 4, WIDE, 128), narrow),
        ),
        [
            pltpu.VMEM((rows, WIDE, 384), narrow),
            pltpu.VMEM((9, 128, 128), wide),
            pltpu.VMEM((384, 384), narrow),
            pltpu.VMEM((2, SLIM, 128), wide),
        ],
        [SMEM] + [VMEM] * 5,
        (at, got, conv_weight, side, preact, early),
        None,
        {5: 2},
    )
    got = lax.all_to_all(sent, ("lat_0", "lat_2", "lon"), 0, 0, tiled=True)
    sent = call(middle_kernel, shape((n_z, 24, 128), narrow), [], [VMEM], (got,))
    got = lax.all_to_all(sent, ("lat_1", "dp"), 0, 0, tiled=True)
    grad_hidden = call(
        input_kernel,
        shape((rows, 128, 128), narrow),
        [pltpu.VMEM((384, 384), narrow)],
        [VMEM] * 2,
        (grad, conv_weight),
    )
    cells = rows * 128 * lax.axis_size("dp") * n_lat * n_x
    own_weight, total_bias, total_proj = call(
        functools.partial(last_kernel, 1.0 / math.sqrt(cells)),
        (shape((3, 3, 2, 128), wide), shape((1, 128), wide), shape((1, 128), wide)),
        [],
        [VMEM],
        (got,),
    )
    return grad_hidden[None], own_weight.transpose(2, 0, 1, 3), total_bias[0], total_proj[0]


def solution(mesh):
    split = Mesh(
        mesh.devices.reshape(mesh.shape["dp"], 4, 2, 2, mesh.shape["lon"]),
        ("dp", "lat_0", "lat_1", "lat_2", "lon"),
    )
    placed = (
        P("dp", LAT, "lon", None),
        P(),
        P(),
        P(),
        P(LAT, "lon"),
        P(LAT, "lon"),
        P(),
        P(),
        P("dp", LAT, "lon"),
    )
    return jax.shard_map(
        shards,
        mesh=split,
        in_specs=placed,
        out_specs=(P("dp", LAT, "lon", None), P(LAT_LON, None, None, None), P(), P()),
        check_vma=False,
    )
```

```python
import functools
import math

import jax
import jax.numpy as jnp
from jax import lax
from jax.experimental import pallas as pl
from jax.experimental.pallas import tpu as pltpu
from jax.sharding import Mesh
from jax.sharding import PartitionSpec as P

ITERS = 6
LAT_LON = ("lat_0", "lat_1", "lat_2", "lon")
LAT = ("lat_0", "lat_1", "lat_2")
WIDE = 144
SLIM = 136
PACK = 32
PLANES = 5
NEAR = 48

helm_coef = 0.5
VMEM = pl.BlockSpec(memory_space=pltpu.VMEM)
SMEM = pl.BlockSpec(memory_space=pltpu.SMEM)
HBM = pl.BlockSpec(memory_space=pltpu.HBM)


def rounded(values):
    return values.astype(jnp.bfloat16).astype(jnp.float32)


def pieces_of(values, count):
    out = []
    for _ in range(count):
        piece = rounded(values)
        out.append(piece)
        values = values - piece
    return out


def full(value):
    return jnp.full((1, 128), value, jnp.float32)


def packed(planes, shift):
    rows = planes[0].shape[0]
    lane = lax.broadcasted_iota(jnp.int32, (rows, 128), 1) // 8
    out = jnp.zeros((rows, 128), jnp.float32)
    for k, plane in enumerate(planes):
        by = (8 * k + shift) % 128
        out = jnp.where(lane == k, pltpu.roll(plane, by, 1) if by else plane, out)
    return out


def edge_columns(load, rows):
    place = lax.broadcasted_iota(jnp.int32, (8, 128), 0)
    columns = [[jnp.zeros((8, 128), jnp.float32) for _ in range(rows // 8)] for _ in range(4)]
    for r in range(rows):
        head = load(r, 0).astype(jnp.float32)
        tail = load(r, 112).astype(jnp.float32)
        for k, row in enumerate((head[0:1], head[1:2], tail[14:15], tail[15:16])):
            columns[k][r // 8] = jnp.where(place == r % 8, row, columns[k][r // 8])
    return columns


def unpacked(beyond, before, k):
    near = lax.broadcasted_iota(jnp.int32, beyond.shape, 1)
    if k:
        beyond = pltpu.roll(beyond, 128 - 8 * k, 1)
    before = pltpu.roll(before, 120 - 8 * k, 1)
    return jnp.where(near < 8, beyond, jnp.where(near >= 120, before, 0.0))


def near_rows(planes, top):
    rows = planes[0].shape[0]
    return [jnp.where(top, p[0:8], p[rows - 8 : rows]) for p in planes]


def first_kernel(at_ref, hidden_ref, fields_ref, cross_ref, planes_ref, sums_ref):
    upper = at_ref[0] == 0
    wet, wet_depth = fields_ref[0], fields_ref[1]
    planes = pieces_of(wet, 3) + pieces_of(wet_depth, 2)
    summed = full(jnp.sum(wet))
    counted = full(jnp.sum(jnp.where(wet_depth > 0.0, 1.0, 0.0)))
    sums_ref[0:1] = summed
    sums_ref[1:2] = counted
    sums = pieces_of(summed, 3) + pieces_of(counted, 3)
    sums = jnp.concatenate(sums + [jnp.zeros((2, 128), jnp.float32)], axis=0)
    for k in range(PLANES):
        planes_ref[k] = planes[k]
    cross_ref[0:256] = hidden_ref[...].reshape(256, 128)
    near = near_rows(planes, upper) + [sums]
    for k in range(0, 6, 2):
        tile = jnp.concatenate(near[k : k + 2], axis=0)
        cross_ref[256 + k * 8 : 272 + k * 8] = tile.astype(jnp.bfloat16)


def edges_kernel(at_ref, hidden_ref, planes_ref, pair_ref, near_ref):
    rows = hidden_ref.shape[0]
    upper = at_ref[0] == 0
    planes = [planes_ref[k] for k in range(PLANES)]
    start = jnp.where(upper, rows - 2, 0)
    pair_ref[0:256] = hidden_ref[pl.ds(start, 2)].reshape(256, 128)
    near = near_rows(planes + planes[:1], jnp.logical_not(upper))
    for k in range(0, 6, 2):
        tile = jnp.concatenate(near[k : k + 2], axis=0)
        pair_ref[256 + k * 8 : 272 + k * 8] = tile.astype(jnp.bfloat16)
    columns = edge_columns(lambda r, at: hidden_ref[r, at : at + 16], rows)
    head = jnp.concatenate(columns[0] + columns[1] + [packed(planes, 0)], axis=0)
    tail = jnp.concatenate(columns[2] + columns[3] + [packed(planes, 8)], axis=0)
    n_x = near_ref.shape[0] // 2
    for peer in range(n_x):
        chosen = jnp.where(at_ref[4] == peer, tail, head).astype(jnp.bfloat16)
        near_ref[peer] = chosen
        near_ref[n_x + peer] = chosen


def second_kernel(at_ref, sums_ref, cross_ref, sent_ref):
    tiles = [cross_ref[256 + k * 16 : 272 + k * 16].astype(jnp.float32) for k in range(3)]
    planes = [tiles[k // 2][k % 2 * 8 : k % 2 * 8 + 8] for k in range(PLANES)]
    got = tiles[2][8:16]
    summed = sums_ref[0:1] + got[0:1] + got[1:2] + got[2:3]
    counted = sums_ref[1:2] + got[3:4] + got[4:5] + got[5:6]
    lane = lax.broadcasted_iota(jnp.int32, (1, 128), 1)
    sums = pieces_of(jnp.where(lane < 64, summed, counted), 3)
    place = lax.broadcasted_iota(jnp.int32, (8, 128), 0)
    blocks = []
    for side in range(2):
        corner = jnp.zeros((8, 128), jnp.float32)
        for r in range(2):
            start = r * 128 + 112 * side
            tile = cross_ref[start : start + 16].astype(jnp.float32)
            for k in range(2):
                at = 14 * side + k
                corner = jnp.where(place == 2 * r + k, tile[at : at + 1], corner)
        for k in range(3):
            corner = jnp.where(place == 4 + k, sums[k], corner)
        blocks.append(jnp.concatenate([corner, packed(planes, 8 * side)], axis=0))
    n_x = 4
    for peer in range(n_x):
        chosen = jnp.where(at_ref[4] == peer, blocks[1], blocks[0]).astype(jnp.bfloat16)
        for group in range(sent_ref.shape[0] // n_x):
            sent_ref[group * n_x + peer] = chosen


def sides_of(at_ref):
    return (
        at_ref[0] == 0,
        jnp.where(at_ref[1] == 0, 0.0, 1.0),
        jnp.where(at_ref[2] == 0, 0.0, 1.0),
    )


def fill(rhs_ref, weight_ref):
    for a in range(3):
        for c in range(3):
            rhs_ref[a * 128 : a * 128 + 128, c * 128 : c * 128 + 128] = weight_ref[a, c]


def convolved(ext_ref, rhs_ref, bias, start, group):
    lhs = jnp.concatenate(
        [ext_ref[pl.ds(start + a, group)].reshape(group * WIDE, 128) for a in range(3)], axis=1
    )
    out = jnp.dot(lhs, rhs_ref[...], preferred_element_type=jnp.float32)
    rows = []
    for j in range(group):
        part = out[j * WIDE : (j + 1) * WIDE]
        rows.append(
            pltpu.roll(part[:, 0:128], 1, 0)
            + part[:, 128:256]
            + pltpu.roll(part[:, 256:384], WIDE - 1, 0)
            + bias
        )
    return rows


def slimmed(row):
    place = lax.broadcasted_iota(jnp.int32, (8, 128), 0)
    edge = jnp.where(place < 4, row[128:136], row[136:144])
    return jnp.concatenate([0.5 * row[0:128], 0.5 * edge], axis=0)


def forward_kernel(
    at_ref, hidden_ref, planes_ref, pair_ref, near_ref, weight_ref, bias_ref, proj_ref,
    alpha_ref, beta_ref,
    ext_ref, preact_ref, side_ref, rhs_ref,
):
    rows = hidden_ref.shape[0]
    n_x = near_ref.shape[0] // 2
    core, left, right = at_ref[0], at_ref[3], at_ref[4]
    upper, keep_above, keep_below = sides_of(at_ref)
    zero = jnp.zeros((), jnp.bfloat16)
    paired = jnp.where(upper, rows + 2, 0)
    keep = jnp.where(upper, keep_below, keep_above) > 0.0
    for k in range(2):
        pair = pair_ref[k * 128 : k * 128 + 128]
        ext_ref[paired + k, 0:128] = jnp.where(keep, pair, zero)
    ext_ref[2 : rows + 2, 0:128] = hidden_ref[...]
    place = lax.broadcasted_iota(jnp.int32, (WIDE - 128, 128), 0)
    tiles = [jnp.zeros((WIDE - 128, 128), jnp.float32) for _ in range(rows + 4)]
    second = []
    for side, base in ((right, 0), (left, WIDE - 130)):
        own = near_ref[core * n_x + side].astype(jnp.float32)
        other = near_ref[(1 - core) * n_x + side].astype(jnp.float32)
        for k in range(2):
            for r in range(rows + 4):
                at = r - 2
                if r < 2:
                    at = k * 16 + rows - 2 + r
                    row = other[at : at + 1] * keep_above
                elif r >= rows + 2:
                    at = k * 16 + r - rows - 2
                    row = other[at : at + 1] * keep_below
                else:
                    row = own[k * 16 + at : k * 16 + at + 1]
                tiles[r] = jnp.where(place == base + k, row, tiles[r])
        above = jnp.where(upper, 0.0, other[40:48] * keep_above)
        below = jnp.where(upper, other[32:40] * keep_below, 0.0)
        second.append(jnp.concatenate([above, own[32:48], below], axis=0))
    for r in range(rows + 4):
        ext_ref[r, 128:WIDE] = tiles[r].astype(jnp.bfloat16)
    pair = pair_ref[256:304].astype(jnp.float32)
    above = jnp.where(upper, 0.0, pair * keep_above)
    below = jnp.where(upper, pair * keep_below, 0.0)
    planes = []
    for k in range(PLANES):
        at = k * 8
        tile = unpacked(second[0], second[1], k)
        planes.append(
            jnp.concatenate(
                [above[at : at + 8], planes_ref[k], below[at : at + 8], tile], axis=0
            )
        )
    side_ref[0 : 2 * PACK] = planes[0] + planes[1] + planes[2]
    side_ref[2 * PACK : 4 * PACK] = planes[3] + planes[4]
    fill(rhs_ref, weight_ref)
    bias = bias_ref[...]
    steps = [full(ref[k]) for ref in (alpha_ref, beta_ref) for k in range(ITERS)]
    params = [bias, proj_ref[...], *steps, full(0.0), full(0.0)]
    side_ref[4 * PACK : 4 * PACK + 16] = jnp.concatenate(params, axis=0)
    group = 4
    shift = jnp.where(upper, 2, 0)
    for g in range(0, rows, group):
        for j, row in enumerate(convolved(ext_ref, rhs_ref, bias, g + shift, group)):
            preact_ref[g + j] = slimmed(row)


def backward_kernel(
    at_ref, cross_ref, got_ref, kernel_ref, side_ref, preact_ref, early_ref,
    grad_ref, sent_ref, ext_ref,
    moved_ref, weight_ref, rhs_ref, fixed_ref,
):
    rows = grad_ref.shape[0] - 2
    n_x = 4
    fields = side_ref[0 : 4 * PACK]
    fields = (fields[0 : 2 * PACK], fields[2 * PACK : 4 * PACK])
    params = side_ref[4 * PACK : 4 * PACK + 16]
    left, right = at_ref[3], at_ref[4]
    upper, keep_above, keep_below = sides_of(at_ref)
    keep_cross = jnp.where(upper, keep_above, keep_below)
    place = lax.broadcasted_iota(jnp.int32, (WIDE - 128, 128), 0)
    tiles = [jnp.zeros((WIDE - 128, 128), jnp.float32) for _ in range(2)]
    second = []
    for side, base in ((right, 0), (left, WIDE - 130)):
        corner = got_ref[at_ref[5] * n_x + side].astype(jnp.float32) * keep_cross
        for r in range(2):
            for k in range(2):
                row = corner[2 * r + k : 2 * r + k + 1]
                tiles[r] = jnp.where(place == base + k, row, tiles[r])
        second.append(corner[8:16])
    crossed = jnp.where(upper, 0, rows + 2)
    for r in range(2):
        facing = cross_ref[r * 128 : r * 128 + 128]
        facing = jnp.where(keep_cross > 0.0, facing, jnp.zeros((), jnp.bfloat16))
        ext_ref[crossed + r, 0:128] = facing
        ext_ref[crossed + r, 128:WIDE] = tiles[r].astype(jnp.bfloat16)
    fill(rhs_ref, kernel_ref)
    again = jnp.where(upper, 0, rows)
    for g, row in enumerate(convolved(ext_ref, rhs_ref, params[0:1], again, 2)):
        fixed_ref[g] = slimmed(row)
    corner = [unpacked(second[0], second[1], k) for k in range(PLANES)]
    corner = (corner[0] + corner[1] + corner[2], corner[3] + corner[4])
    facing = cross_ref[256:304].astype(jnp.float32) * keep_cross
    facing = (facing[0:8] + facing[8:16] + facing[16:24], facing[24:32] + facing[32:40])
    start, wet_depth = [
        jnp.concatenate(
            [
                fields[k][0:8] + jnp.where(upper, facing[k], 0.0),
                fields[k][8 : PACK - 8],
                fields[k][PACK - 8 : PACK] + jnp.where(upper, 0.0, facing[k]),
                fields[k][PACK : PACK + 8] + jnp.where(upper, corner[k], 0.0),
                fields[k][PACK + 8 : 2 * PACK - 8],
                fields[k][2 * PACK - 8 : 2 * PACK] + jnp.where(upper, 0.0, corner[k]),
            ],
            axis=0,
        )
        for k in range(2)
    ]
    lane = lax.broadcasted_iota(jnp.int32, (2 * PACK, 128), 1)
    mask = jnp.where(wet_depth > 0.0, 1.0, 0.0)

    def other_half(field):
        parts = [field[k * PACK : (k + 1) * PACK] for k in range(field.shape[0] // PACK)]
        swapped = []
        for k in range(0, len(parts), 2):
            swapped += [parts[k + 1], parts[k]]
        return jnp.concatenate(swapped, axis=0)

    def beside(field):
        count = field.shape[0]
        lanes = lane if count == 2 * PACK else jnp.concatenate([lane, lane], axis=0)
        up = pltpu.roll(field, 1, 0)
        down = pltpu.roll(field, count - 1, 0)
        from_left = pltpu.roll(field, 1, 1)
        from_left = jnp.where(lanes == 0, other_half(from_left), from_left)
        from_right = pltpu.roll(field, 127, 1)
        from_right = jnp.where(lanes == 127, other_half(from_right), from_right)
        return up, down, from_left, from_right

    weights = [
        0.5 * (near_mask * wet_depth + mask * near_depth)
        for near_mask, near_depth in zip(beside(mask), beside(wet_depth))
    ]
    diagonal = helm_coef * mask + weights[0] + weights[1] + weights[2] + weights[3]
    weights = [jnp.concatenate([w, w], axis=0) for w in weights]
    diagonal = jnp.concatenate([diagonal, diagonal], axis=0)
    residual = jnp.concatenate([start, mask], axis=0)
    direction = residual
    result = jnp.zeros_like(residual)
    for k in range(ITERS):
        result = result + params[2 + k : 3 + k] * direction
        if k + 1 < ITERS:
            applied = diagonal * direction
            for w, near in zip(weights, beside(direction)):
                applied = applied - w * near
            residual = residual - params[2 + k : 3 + k] * applied
            direction = residual + params[8 + k : 9 + k] * direction
    result = result * jnp.concatenate([mask, mask], axis=0)
    sums = jnp.sum(got_ref[...].astype(jnp.float32)[:, 0:8], axis=0)
    sums = sums[4:5] + sums[5:6] + sums[6:7]
    mean = jnp.broadcast_to(sums[:, 0:1], (1, 128)) / jnp.broadcast_to(sums[:, 127:128], (1, 128))
    force = result.T
    force = force - mean * pltpu.roll(force, 64, 1)
    proj = 0.5 * params[1:2]
    shift = jnp.where(upper, 2, 0)
    sublane = lax.broadcasted_iota(jnp.int32, (8, 1), 0)
    sum_bias = jnp.zeros((8, 128), jnp.float32)
    sum_proj = jnp.zeros((8, 128), jnp.float32)
    for g in range(rows + 2):
        at = g + 7
        edge = jnp.where(
            sublane < 4,
            force[0:8, PACK + at : PACK + at + 1],
            force[120:128, PACK + at : PACK + at + 1],
        )
        for q, size in ((0, 48), (48, 48), (96, 32), (128, 8)):
            column = edge if q == 128 else force[q : q + size, at : at + 1]
            column = jnp.broadcast_to(column, (size, 128))
            if g < 2:
                preact = jnp.where(upper, fixed_ref[g, q : q + size], preact_ref[g, q : q + size])
            elif g >= rows:
                preact = jnp.where(
                    upper, preact_ref[g - 2, q : q + size], fixed_ref[g - rows, q : q + size]
                )
            else:
                preact = preact_ref[g - shift, q : q + size]
            turn = jnp.tanh(preact)
            bent = preact * turn
            active = preact + bent
            slope_act = (1.0 + turn) * ((1.0 + preact) - bent)
            grad = column * proj * slope_act
            if q == 128:
                grad_ref[g, 128:WIDE] = jnp.concatenate([grad, grad], axis=0).astype(jnp.bfloat16)
                continue
            grad = grad.astype(jnp.bfloat16)
            grad_ref[g, q : q + size] = grad
            if 1 <= g <= rows:
                own = grad.astype(jnp.float32)
                drawn = active * column
                for k in range(size // 8):
                    sum_bias = sum_bias + own[k * 8 : k * 8 + 8]
                    sum_proj = sum_proj + drawn[k * 8 : k * 8 + 8]
    for g in range(1, rows + 1):
        own = grad_ref[g, 0:128].astype(jnp.float32)
        own = jnp.concatenate([own, jnp.zeros((WIDE - 128, 128), jnp.float32)], axis=0)
        moved_ref[g - 1, :, 0:128] = pltpu.roll(own, WIDE - 1, 0).astype(jnp.bfloat16)
        moved_ref[g - 1, :, 128:256] = own.astype(jnp.bfloat16)
        moved_ref[g - 1, :, 256:384] = pltpu.roll(own, 1, 0).astype(jnp.bfloat16)
    to = lax.broadcasted_iota(jnp.int32, (128, 128), 0)
    of = lax.broadcasted_iota(jnp.int32, (128, 128), 1)
    source = (
        to // 32 * 32 + to // 2 % 2 * 16 + to // 16 % 2 * 8 + to // 4 % 4 * 2 + to % 2
    )
    order = jnp.where(of == source, 1.0, 0.0).astype(jnp.bfloat16)
    moved = moved_ref[...].reshape(rows * WIDE, 384)
    cells = jnp.concatenate(
        [ext_ref[a + 1 : a + 1 + rows].reshape(rows * WIDE, 128) for a in range(3)], axis=1
    )
    whole = lax.dot_general(
        cells, moved, (((0,), (0,)), ((), ())), preferred_element_type=jnp.float32
    )
    for a in range(3):
        out = whole[a * 128 : a * 128 + 128]
        out = jnp.dot(
            order, out.astype(jnp.bfloat16), preferred_element_type=jnp.float32
        )
        for c in range(3):
            weight_ref[a * 3 + c] = out[:, c * 128 : c * 128 + 128]
    vectors = jnp.concatenate(
        [jnp.sum(sum_bias, axis=0, keepdims=True), jnp.sum(sum_proj, axis=0, keepdims=True)], axis=0
    )
    vectors = jnp.concatenate(pieces_of(vectors, 2) + [jnp.zeros((4, 128), jnp.float32)], axis=0)
    vectors = pltpu.roll(vectors, 4, 0)
    low = lax.broadcasted_iota(jnp.int32, (8, 128), 0) < 4

    for t in range(16):
        start = t * 8
        blocks = ([], [])
        for k in range(0, 9, 2):
            one = weight_ref[k, start : start + 8]
            two = weight_ref[k + 1, start : start + 8] if k < 8 else vectors
            two_low = pltpu.roll(two, 4, 0) if k < 8 else vectors
            blocks[0].append(jnp.where(low, one, two_low))
            blocks[1].append(jnp.where(low, pltpu.roll(one, 4, 0), two))
        for x in range(2):
            sent_ref[t * 2 + x] = jnp.concatenate(blocks[x], axis=0).astype(jnp.bfloat16)


def middle_kernel(got_ref, sent_ref):
    total = jnp.sum(got_ref[...].astype(jnp.float32), axis=0)
    vectors = total[36:38] + total[38:40]
    vectors = jnp.concatenate(pieces_of(vectors, 2) + [jnp.zeros((2, 128), jnp.float32)], axis=0)
    peers = sent_ref.shape[0] // 2
    for z in range(2):
        block = [total[4 * k + 2 * z : 4 * k + 2 * z + 2] for k in range(9)]
        block = jnp.concatenate(block + [vectors], axis=0)
        block = block.astype(jnp.bfloat16)
        for d in range(peers):
            sent_ref[z * peers + d] = block


def last_kernel(scale, got_ref, weight_ref, bias_ref, proj_ref):
    total = jnp.sum(got_ref[...].astype(jnp.float32), axis=0) * scale
    for k in range(9):
        weight_ref[k // 3, k % 3] = total[k * 2 : k * 2 + 2]
    bias_ref[...] = total[18:19] + total[20:21]
    proj_ref[...] = total[19:20] + total[21:22]


def input_kernel(grad_ref, weight_ref, out_ref, rhs_ref):
    rows = out_ref.shape[0]
    for a in range(3):
        for c in range(3):
            rhs_ref[c * 128 : c * 128 + 128, a * 128 : a * 128 + 128] = weight_ref[a, c]
    group = 4
    for y in range(0, rows, group):
        lhs = jnp.concatenate(
            [
                grad_ref[y - a + 2 : y - a + 2 + group].reshape(group * WIDE, 128)
                for a in range(3)
            ],
            axis=1,
        )
        out = lax.dot_general(
            lhs, rhs_ref[...], (((1,), (1,)), ((), ())), preferred_element_type=jnp.float32
        )
        for j in range(group):
            part = out[j * WIDE : (j + 1) * WIDE]
            total = (
                pltpu.roll(part[:, 0:128], WIDE - 1, 0)
                + part[:, 128:256]
                + pltpu.roll(part[:, 256:384], 1, 0)
            )
            out_ref[y + j] = total[0:128].astype(jnp.bfloat16)


def call(kernel, shapes, scratch, in_specs, args, out_specs=None, aliases={}):
    return pl.pallas_call(
        kernel,
        out_shape=shapes,
        in_specs=in_specs,
        out_specs=jax.tree.map(lambda _: VMEM, shapes) if out_specs is None else out_specs,
        scratch_shapes=scratch,
        input_output_aliases=aliases,
        compiler_params=pltpu.CompilerParams(vmem_limit_bytes=40 * 1024 * 1024),
    )(*args)


def shape(dims, dtype):
    return jax.ShapeDtypeStruct(dims, dtype)


def shards(
    hidden_in, conv_weight, conv_bias, proj_weight, ocean_depth, sea_mask,
    step_alpha, step_beta, surface_cotangent,
):
    wide, narrow = jnp.float32, jnp.bfloat16
    rows = hidden_in.shape[1]
    hidden = hidden_in[0]
    n_x = lax.axis_size("lon")
    n_lat = lax.axis_size(LAT)
    n_all = lax.axis_size(("lat_0", "lat_2", "lon"))
    n_z = lax.axis_size(("lat_1", "dp"))
    lat, me = lax.axis_index(LAT), lax.axis_index("lon")
    row_group = lax.axis_index(("lat_0", "lat_2"))
    at = jnp.stack(
        [lat % 2, lat, n_lat - 1 - lat, (me + n_x - 1) % n_x, (me + 1) % n_x, row_group]
    ).astype(jnp.int32)
    mask = sea_mask.astype(wide)
    fields = jnp.stack([mask * surface_cotangent[0], mask * ocean_depth])
    facing = lax.dynamic_slice_in_dim(
        hidden, jnp.where(lax.axis_index("lat_2") == 0, 0, rows - 2), 2, axis=0
    )
    cross, planes, sums = call(
        first_kernel,
        (
            shape((304, 128), narrow),
            shape((PLANES, rows, 128), wide),
            shape((2, 128), wide),
        ),
        [],
        [SMEM] + [VMEM] * 2,
        (at, facing, fields),
    )
    odd = [(i, (i + 1) % n_lat) for i in range(1, n_lat, 2)]
    odd = odd + [(j, i) for i, j in odd]
    cross = lax.ppermute(cross, LAT, odd)
    pair, near = call(
        edges_kernel,
        (shape((304, 128), narrow), shape((2 * n_x, NEAR, 128), narrow)),
        [],
        [SMEM] + [VMEM] * 2,
        (at, hidden, planes),
    )
    pair = lax.ppermute(pair, "lat_2", [(0, 1), (1, 0)])
    near = lax.all_to_all(near, ("lat_2", "lon"), 0, 0, tiled=True)
    sent = call(
        second_kernel, shape((n_all, 16, 128), narrow), [], [SMEM] + [VMEM] * 2, (at, sums, cross)
    )
    got = lax.all_to_all(sent, ("lat_0", "lat_2", "lon"), 0, 0, tiled=True)
    early, preact, side = call(
        forward_kernel,
        (
            shape((rows + 4, WIDE, 128), narrow),
            shape((rows, SLIM, 128), wide),
            shape((4 * PACK + 16, 128), wide),
        ),
        [pltpu.VMEM((384, 384), narrow)],
        [SMEM] + [VMEM] * 7 + [SMEM] * 2,
        (
            at, hidden, planes, pair, near, conv_weight, conv_bias[None],
            proj_weight[None], step_alpha, step_beta,
        ),
    )
    grad, sent, _ = call(
        backward_kernel,
        (
            shape((rows + 2, WIDE, 128), narrow),
            shape((n_all, 40, 128), narrow),
            shape((rows + 4, WIDE, 128), narrow),
        ),
        [
            pltpu.VMEM((rows, WIDE, 384), narrow),
            pltpu.VMEM((9, 128, 128), wide),
            pltpu.VMEM((384, 384), narrow),
            pltpu.VMEM((2, SLIM, 128), wide),
        ],
        [SMEM] + [VMEM] * 6,
        (at, cross, got, conv_weight, side, preact, early),
        None,
        {6: 2},
    )
    got = lax.all_to_all(sent, ("lat_0", "lat_2", "lon"), 0, 0, tiled=True)
    sent = call(middle_kernel, shape((n_z, 24, 128), narrow), [], [VMEM], (got,))
    got = lax.all_to_all(sent, ("lat_1", "dp"), 0, 0, tiled=True)
    grad_hidden = call(
        input_kernel,
        shape((rows, 128, 128), narrow),
        [pltpu.VMEM((384, 384), narrow)],
        [VMEM] * 2,
        (grad, conv_weight),
    )
    cells = rows * 128 * lax.axis_size("dp") * n_lat * n_x
    own_weight, total_bias, total_proj = call(
        functools.partial(last_kernel, 1.0 / math.sqrt(cells)),
        (shape((3, 3, 2, 128), wide), shape((1, 128), wide), shape((1, 128), wide)),
        [],
        [VMEM],
        (got,),
    )
    return grad_hidden[None], own_weight.transpose(2, 0, 1, 3), total_bias[0], total_proj[0]


def solution(mesh):
    split = Mesh(
        mesh.devices.reshape(mesh.shape["dp"], 4, 2, 2, mesh.shape["lon"]),
        ("dp", "lat_0", "lat_1", "lat_2", "lon"),
    )
    placed = (
        P("dp", LAT, "lon", None),
        P(),
        P(),
        P(),
        P(LAT, "lon"),
        P(LAT, "lon"),
        P(),
        P(),
        P("dp", LAT, "lon"),
    )
    return jax.shard_map(
        shards,
        mesh=split,
        in_specs=placed,
        out_specs=(P("dp", LAT, "lon", None), P(LAT_LON, None, None, None), P(), P()),
        check_vma=False,
    )
```

```python
import functools
import math

import jax
import jax.numpy as jnp
from jax import lax
from jax.experimental import pallas as pl
from jax.experimental.pallas import tpu as pltpu
from jax.sharding import Mesh
from jax.sharding import PartitionSpec as P

ITERS = 6
LAT_LON = ("lat_0", "lat_1", "lat_2", "lon")
LAT = ("lat_0", "lat_1", "lat_2")
WIDE = 144
SLIM = 136
PACK = 32
PLANES = 5
NEAR = 48

helm_coef = 0.5
VMEM = pl.BlockSpec(memory_space=pltpu.VMEM)
SMEM = pl.BlockSpec(memory_space=pltpu.SMEM)
HBM = pl.BlockSpec(memory_space=pltpu.HBM)


def rounded(values):
    return values.astype(jnp.bfloat16).astype(jnp.float32)


def pieces_of(values, count):
    out = []
    for _ in range(count):
        piece = rounded(values)
        out.append(piece)
        values = values - piece
    return out


def full(value):
    return jnp.full((1, 128), value, jnp.float32)


def packed(planes, shift):
    rows = planes[0].shape[0]
    lane = lax.broadcasted_iota(jnp.int32, (rows, 128), 1) // 8
    out = jnp.zeros((rows, 128), jnp.float32)
    for k, plane in enumerate(planes):
        by = (8 * k + shift) % 128
        out = jnp.where(lane == k, pltpu.roll(plane, by, 1) if by else plane, out)
    return out


def edge_columns(load, rows):
    place = lax.broadcasted_iota(jnp.int32, (8, 128), 0)
    columns = [[jnp.zeros((8, 128), jnp.float32) for _ in range(rows // 8)] for _ in range(4)]
    for r in range(rows):
        head = load(r, 0).astype(jnp.float32)
        tail = load(r, 112).astype(jnp.float32)
        for k, row in enumerate((head[0:1], head[1:2], tail[14:15], tail[15:16])):
            columns[k][r // 8] = jnp.where(place == r % 8, row, columns[k][r // 8])
    return columns


def unpacked(beyond, before, k):
    near = lax.broadcasted_iota(jnp.int32, beyond.shape, 1)
    if k:
        beyond = pltpu.roll(beyond, 128 - 8 * k, 1)
    before = pltpu.roll(before, 120 - 8 * k, 1)
    return jnp.where(near < 8, beyond, jnp.where(near >= 120, before, 0.0))


def near_rows(planes, top):
    rows = planes[0].shape[0]
    return [jnp.where(top, p[0:8], p[rows - 8 : rows]) for p in planes]


def first_kernel(
    at_ref, top_ref, bottom_ref, wet_ref, depth_ref, cross_ref, planes_ref, sums_ref
):
    upper = at_ref[0] == 0
    wet, wet_depth = wet_ref[...], depth_ref[...]
    planes = pieces_of(wet, 3) + pieces_of(wet_depth, 2)
    summed = full(jnp.sum(wet))
    counted = full(jnp.sum(jnp.where(wet_depth > 0.0, 1.0, 0.0)))
    sums_ref[0:1] = summed
    sums_ref[1:2] = counted
    sums = pieces_of(summed, 3) + pieces_of(counted, 3)
    sums = jnp.concatenate(sums + [jnp.zeros((2, 128), jnp.float32)], axis=0)
    for k in range(PLANES):
        planes_ref[k] = planes[k]
    facing = jnp.where(upper, top_ref[...], bottom_ref[...])
    cross_ref[0:256] = facing.reshape(256, 128)
    near = near_rows(planes, upper) + [sums]
    for k in range(0, 6, 2):
        tile = jnp.concatenate(near[k : k + 2], axis=0)
        cross_ref[256 + k * 8 : 272 + k * 8] = tile.astype(jnp.bfloat16)


def edges_kernel(at_ref, hidden_ref, planes_ref, pair_ref, near_ref):
    rows = hidden_ref.shape[0]
    upper = at_ref[0] == 0
    planes = [planes_ref[k] for k in range(PLANES)]
    start = jnp.where(upper, rows - 2, 0)
    pair_ref[0:256] = hidden_ref[pl.ds(start, 2)].reshape(256, 128)
    near = near_rows(planes + planes[:1], jnp.logical_not(upper))
    for k in range(0, 6, 2):
        tile = jnp.concatenate(near[k : k + 2], axis=0)
        pair_ref[256 + k * 8 : 272 + k * 8] = tile.astype(jnp.bfloat16)
    columns = edge_columns(lambda r, at: hidden_ref[r, at : at + 16], rows)
    head = jnp.concatenate(columns[0] + columns[1] + [packed(planes, 0)], axis=0)
    tail = jnp.concatenate(columns[2] + columns[3] + [packed(planes, 8)], axis=0)
    n_x = near_ref.shape[0] // 2
    for peer in range(n_x):
        chosen = jnp.where(at_ref[4] == peer, tail, head).astype(jnp.bfloat16)
        near_ref[peer] = chosen
        near_ref[n_x + peer] = chosen


def second_kernel(at_ref, sums_ref, cross_ref, sent_ref):
    tiles = [cross_ref[256 + k * 16 : 272 + k * 16].astype(jnp.float32) for k in range(3)]
    planes = [tiles[k // 2][k % 2 * 8 : k % 2 * 8 + 8] for k in range(PLANES)]
    got = tiles[2][8:16]
    summed = sums_ref[0:1] + got[0:1] + got[1:2] + got[2:3]
    counted = sums_ref[1:2] + got[3:4] + got[4:5] + got[5:6]
    lane = lax.broadcasted_iota(jnp.int32, (1, 128), 1)
    sums = pieces_of(jnp.where(lane < 64, summed, counted), 3)
    place = lax.broadcasted_iota(jnp.int32, (8, 128), 0)
    blocks = []
    for side in range(2):
        corner = jnp.zeros((8, 128), jnp.float32)
        for r in range(2):
            start = r * 128 + 112 * side
            tile = cross_ref[start : start + 16].astype(jnp.float32)
            for k in range(2):
                at = 14 * side + k
                corner = jnp.where(place == 2 * r + k, tile[at : at + 1], corner)
        for k in range(3):
            corner = jnp.where(place == 4 + k, sums[k], corner)
        blocks.append(jnp.concatenate([corner, packed(planes, 8 * side)], axis=0))
    n_x = 4
    for peer in range(n_x):
        chosen = jnp.where(at_ref[4] == peer, blocks[1], blocks[0]).astype(jnp.bfloat16)
        for group in range(sent_ref.shape[0] // n_x):
            sent_ref[group * n_x + peer] = chosen


def sides_of(at_ref):
    return (
        at_ref[0] == 0,
        jnp.where(at_ref[1] == 0, 0.0, 1.0),
        jnp.where(at_ref[2] == 0, 0.0, 1.0),
    )


def fill(rhs_ref, weight_ref):
    for a in range(3):
        for c in range(3):
            rhs_ref[a * 128 : a * 128 + 128, c * 128 : c * 128 + 128] = weight_ref[a, c]


def convolved(ext_ref, rhs_ref, bias, start, group):
    lhs = jnp.concatenate(
        [ext_ref[pl.ds(start + a, group)].reshape(group * WIDE, 128) for a in range(3)], axis=1
    )
    out = jnp.dot(lhs, rhs_ref[...], preferred_element_type=jnp.float32)
    rows = []
    for j in range(group):
        part = out[j * WIDE : (j + 1) * WIDE]
        rows.append(
            pltpu.roll(part[:, 0:128], 1, 0)
            + part[:, 128:256]
            + pltpu.roll(part[:, 256:384], WIDE - 1, 0)
            + bias
        )
    return rows


def slimmed(row):
    place = lax.broadcasted_iota(jnp.int32, (8, 128), 0)
    edge = jnp.where(place < 4, row[128:136], row[136:144])
    return jnp.concatenate([0.5 * row[0:128], 0.5 * edge], axis=0)


def forward_kernel(
    at_ref, hidden_ref, planes_ref, pair_ref, near_ref, weight_ref, bias_ref, proj_ref,
    alpha_ref, beta_ref,
    ext_ref, preact_ref, side_ref, rhs_ref,
):
    rows = hidden_ref.shape[0]
    n_x = near_ref.shape[0] // 2
    core, left, right = at_ref[0], at_ref[3], at_ref[4]
    upper, keep_above, keep_below = sides_of(at_ref)
    zero = jnp.zeros((), jnp.bfloat16)
    paired = jnp.where(upper, rows + 2, 0)
    keep = jnp.where(upper, keep_below, keep_above) > 0.0
    for k in range(2):
        pair = pair_ref[k * 128 : k * 128 + 128]
        ext_ref[paired + k, 0:128] = jnp.where(keep, pair, zero)
    ext_ref[2 : rows + 2, 0:128] = hidden_ref[...]
    place = lax.broadcasted_iota(jnp.int32, (WIDE - 128, 128), 0)
    tiles = [jnp.zeros((WIDE - 128, 128), jnp.float32) for _ in range(rows + 4)]
    second = []
    for side, base in ((right, 0), (left, WIDE - 130)):
        own = near_ref[core * n_x + side].astype(jnp.float32)
        other = near_ref[(1 - core) * n_x + side].astype(jnp.float32)
        for k in range(2):
            for r in range(rows + 4):
                at = r - 2
                if r < 2:
                    at = k * 16 + rows - 2 + r
                    row = other[at : at + 1] * keep_above
                elif r >= rows + 2:
                    at = k * 16 + r - rows - 2
                    row = other[at : at + 1] * keep_below
                else:
                    row = own[k * 16 + at : k * 16 + at + 1]
                tiles[r] = jnp.where(place == base + k, row, tiles[r])
        above = jnp.where(upper, 0.0, other[40:48] * keep_above)
        below = jnp.where(upper, other[32:40] * keep_below, 0.0)
        second.append(jnp.concatenate([above, own[32:48], below], axis=0))
    for r in range(rows + 4):
        ext_ref[r, 128:WIDE] = tiles[r].astype(jnp.bfloat16)
    pair = pair_ref[256:304].astype(jnp.float32)
    above = jnp.where(upper, 0.0, pair * keep_above)
    below = jnp.where(upper, pair * keep_below, 0.0)
    planes = []
    for k in range(PLANES):
        at = k * 8
        tile = unpacked(second[0], second[1], k)
        planes.append(
            jnp.concatenate(
                [above[at : at + 8], planes_ref[k], below[at : at + 8], tile], axis=0
            )
        )
    side_ref[0 : 2 * PACK] = planes[0] + planes[1] + planes[2]
    side_ref[2 * PACK : 4 * PACK] = planes[3] + planes[4]
    fill(rhs_ref, weight_ref)
    bias = bias_ref[...]
    steps = [full(ref[k]) for ref in (alpha_ref, beta_ref) for k in range(ITERS)]
    params = [bias, proj_ref[...], *steps, full(0.0), full(0.0)]
    side_ref[4 * PACK : 4 * PACK + 16] = jnp.concatenate(params, axis=0)
    group = 4
    shift = jnp.where(upper, 2, 0)
    for g in range(0, rows, group):
        for j, row in enumerate(convolved(ext_ref, rhs_ref, bias, g + shift, group)):
            preact_ref[g + j] = slimmed(row)


def backward_kernel(
    at_ref, cross_ref, got_ref, kernel_ref, side_ref, preact_ref, early_ref,
    grad_ref, sent_ref, ext_ref,
    moved_ref, weight_ref, rhs_ref, fixed_ref,
):
    rows = grad_ref.shape[0] - 2
    n_x = 4
    fields = side_ref[0 : 4 * PACK]
    fields = (fields[0 : 2 * PACK], fields[2 * PACK : 4 * PACK])
    params = side_ref[4 * PACK : 4 * PACK + 16]
    left, right = at_ref[3], at_ref[4]
    upper, keep_above, keep_below = sides_of(at_ref)
    keep_cross = jnp.where(upper, keep_above, keep_below)
    place = lax.broadcasted_iota(jnp.int32, (WIDE - 128, 128), 0)
    tiles = [jnp.zeros((WIDE - 128, 128), jnp.float32) for _ in range(2)]
    second = []
    for side, base in ((right, 0), (left, WIDE - 130)):
        corner = got_ref[at_ref[5] * n_x + side].astype(jnp.float32) * keep_cross
        for r in range(2):
            for k in range(2):
                row = corner[2 * r + k : 2 * r + k + 1]
                tiles[r] = jnp.where(place == base + k, row, tiles[r])
        second.append(corner[8:16])
    crossed = jnp.where(upper, 0, rows + 2)
    for r in range(2):
        facing = cross_ref[r * 128 : r * 128 + 128]
        facing = jnp.where(keep_cross > 0.0, facing, jnp.zeros((), jnp.bfloat16))
        ext_ref[crossed + r, 0:128] = facing
        ext_ref[crossed + r, 128:WIDE] = tiles[r].astype(jnp.bfloat16)
    fill(rhs_ref, kernel_ref)
    again = jnp.where(upper, 0, rows)
    for g, row in enumerate(convolved(ext_ref, rhs_ref, params[0:1], again, 2)):
        fixed_ref[g] = slimmed(row)
    corner = [unpacked(second[0], second[1], k) for k in range(PLANES)]
    corner = (corner[0] + corner[1] + corner[2], corner[3] + corner[4])
    facing = cross_ref[256:304].astype(jnp.float32) * keep_cross
    facing = (facing[0:8] + facing[8:16] + facing[16:24], facing[24:32] + facing[32:40])
    start, wet_depth = [
        jnp.concatenate(
            [
                fields[k][0:8] + jnp.where(upper, facing[k], 0.0),
                fields[k][8 : PACK - 8],
                fields[k][PACK - 8 : PACK] + jnp.where(upper, 0.0, facing[k]),
                fields[k][PACK : PACK + 8] + jnp.where(upper, corner[k], 0.0),
                fields[k][PACK + 8 : 2 * PACK - 8],
                fields[k][2 * PACK - 8 : 2 * PACK] + jnp.where(upper, 0.0, corner[k]),
            ],
            axis=0,
        )
        for k in range(2)
    ]
    lane = lax.broadcasted_iota(jnp.int32, (2 * PACK, 128), 1)
    mask = jnp.where(wet_depth > 0.0, 1.0, 0.0)

    def other_half(field):
        parts = [field[k * PACK : (k + 1) * PACK] for k in range(field.shape[0] // PACK)]
        swapped = []
        for k in range(0, len(parts), 2):
            swapped += [parts[k + 1], parts[k]]
        return jnp.concatenate(swapped, axis=0)

    def beside(field):
        count = field.shape[0]
        lanes = lane if count == 2 * PACK else jnp.concatenate([lane, lane], axis=0)
        up = pltpu.roll(field, 1, 0)
        down = pltpu.roll(field, count - 1, 0)
        from_left = pltpu.roll(field, 1, 1)
        from_left = jnp.where(lanes == 0, other_half(from_left), from_left)
        from_right = pltpu.roll(field, 127, 1)
        from_right = jnp.where(lanes == 127, other_half(from_right), from_right)
        return up, down, from_left, from_right

    weights = [
        0.5 * (near_mask * wet_depth + mask * near_depth)
        for near_mask, near_depth in zip(beside(mask), beside(wet_depth))
    ]
    diagonal = helm_coef * mask + weights[0] + weights[1] + weights[2] + weights[3]
    weights = [jnp.concatenate([w, w], axis=0) for w in weights]
    diagonal = jnp.concatenate([diagonal, diagonal], axis=0)
    residual = jnp.concatenate([start, mask], axis=0)
    direction = residual
    result = jnp.zeros_like(residual)
    for k in range(ITERS):
        result = result + params[2 + k : 3 + k] * direction
        if k + 1 < ITERS:
            applied = diagonal * direction
            for w, near in zip(weights, beside(direction)):
                applied = applied - w * near
            residual = residual - params[2 + k : 3 + k] * applied
            direction = residual + params[8 + k : 9 + k] * direction
    result = result * jnp.concatenate([mask, mask], axis=0)
    sums = jnp.sum(got_ref[...].astype(jnp.float32)[:, 0:8], axis=0)
    sums = sums[4:5] + sums[5:6] + sums[6:7]
    mean = jnp.broadcast_to(sums[:, 0:1], (1, 128)) / jnp.broadcast_to(sums[:, 127:128], (1, 128))
    force = result.T
    force = force - mean * pltpu.roll(force, 64, 1)
    proj = 0.5 * params[1:2]
    shift = jnp.where(upper, 2, 0)
    sublane = lax.broadcasted_iota(jnp.int32, (8, 1), 0)
    sum_bias = jnp.zeros((8, 128), jnp.float32)
    sum_proj = jnp.zeros((8, 128), jnp.float32)
    for g in range(rows + 2):
        at = g + 7
        edge = jnp.where(
            sublane < 4,
            force[0:8, PACK + at : PACK + at + 1],
            force[120:128, PACK + at : PACK + at + 1],
        )
        for q, size in ((0, 48), (48, 48), (96, 32), (128, 8)):
            column = edge if q == 128 else force[q : q + size, at : at + 1]
            column = jnp.broadcast_to(column, (size, 128))
            if g < 2:
                preact = jnp.where(upper, fixed_ref[g, q : q + size], preact_ref[g, q : q + size])
            elif g >= rows:
                preact = jnp.where(
                    upper, preact_ref[g - 2, q : q + size], fixed_ref[g - rows, q : q + size]
                )
            else:
                preact = preact_ref[g - shift, q : q + size]
            turn = jnp.tanh(preact)
            bent = preact * turn
            active = preact + bent
            slope_act = (1.0 + turn) * ((1.0 + preact) - bent)
            grad = column * proj * slope_act
            if q == 128:
                grad_ref[g, 128:WIDE] = jnp.concatenate([grad, grad], axis=0).astype(jnp.bfloat16)
                continue
            grad = grad.astype(jnp.bfloat16)
            grad_ref[g, q : q + size] = grad
            if 1 <= g <= rows:
                own = grad.astype(jnp.float32)
                drawn = active * column
                for k in range(size // 8):
                    sum_bias = sum_bias + own[k * 8 : k * 8 + 8]
                    sum_proj = sum_proj + drawn[k * 8 : k * 8 + 8]
    for g in range(1, rows + 1):
        own = grad_ref[g, 0:128].astype(jnp.float32)
        own = jnp.concatenate([own, jnp.zeros((WIDE - 128, 128), jnp.float32)], axis=0)
        moved_ref[g - 1, :, 0:128] = pltpu.roll(own, WIDE - 1, 0).astype(jnp.bfloat16)
        moved_ref[g - 1, :, 128:256] = own.astype(jnp.bfloat16)
        moved_ref[g - 1, :, 256:384] = pltpu.roll(own, 1, 0).astype(jnp.bfloat16)
    to = lax.broadcasted_iota(jnp.int32, (128, 128), 0)
    of = lax.broadcasted_iota(jnp.int32, (128, 128), 1)
    source = (
        to // 32 * 32 + to // 2 % 2 * 16 + to // 16 % 2 * 8 + to // 4 % 4 * 2 + to % 2
    )
    order = jnp.where(of == source, 1.0, 0.0).astype(jnp.bfloat16)
    moved = moved_ref[...].reshape(rows * WIDE, 384)
    cells = jnp.concatenate(
        [ext_ref[a + 1 : a + 1 + rows].reshape(rows * WIDE, 128) for a in range(3)], axis=1
    )
    whole = lax.dot_general(
        cells, moved, (((0,), (0,)), ((), ())), preferred_element_type=jnp.float32
    )
    for a in range(3):
        out = whole[a * 128 : a * 128 + 128]
        out = jnp.dot(
            order, out.astype(jnp.bfloat16), preferred_element_type=jnp.float32
        )
        for c in range(3):
            weight_ref[a * 3 + c] = out[:, c * 128 : c * 128 + 128]
    vectors = jnp.concatenate(
        [jnp.sum(sum_bias, axis=0, keepdims=True), jnp.sum(sum_proj, axis=0, keepdims=True)], axis=0
    )
    vectors = jnp.concatenate(pieces_of(vectors, 2) + [jnp.zeros((4, 128), jnp.float32)], axis=0)
    vectors = pltpu.roll(vectors, 4, 0)
    low = lax.broadcasted_iota(jnp.int32, (8, 128), 0) < 4

    for t in range(16):
        start = t * 8
        blocks = ([], [])
        for k in range(0, 9, 2):
            one = weight_ref[k, start : start + 8]
            two = weight_ref[k + 1, start : start + 8] if k < 8 else vectors
            two_low = pltpu.roll(two, 4, 0) if k < 8 else vectors
            blocks[0].append(jnp.where(low, one, two_low))
            blocks[1].append(jnp.where(low, pltpu.roll(one, 4, 0), two))
        for x in range(2):
            sent_ref[t * 2 + x] = jnp.concatenate(blocks[x], axis=0).astype(jnp.bfloat16)


def middle_kernel(got_ref, sent_ref):
    total = jnp.sum(got_ref[...].astype(jnp.float32), axis=0)
    vectors = total[36:38] + total[38:40]
    vectors = jnp.concatenate(pieces_of(vectors, 2) + [jnp.zeros((2, 128), jnp.float32)], axis=0)
    peers = sent_ref.shape[0] // 2
    for z in range(2):
        block = [total[4 * k + 2 * z : 4 * k + 2 * z + 2] for k in range(9)]
        block = jnp.concatenate(block + [vectors], axis=0)
        block = block.astype(jnp.bfloat16)
        for d in range(peers):
            sent_ref[z * peers + d] = block


def last_kernel(scale, got_ref, weight_ref, bias_ref, proj_ref):
    total = jnp.sum(got_ref[...].astype(jnp.float32), axis=0) * scale
    for k in range(9):
        weight_ref[k // 3, k % 3] = total[k * 2 : k * 2 + 2]
    bias_ref[...] = total[18:19] + total[20:21]
    proj_ref[...] = total[19:20] + total[21:22]


def input_kernel(grad_ref, weight_ref, out_ref, rhs_ref):
    rows = out_ref.shape[0]
    for a in range(3):
        for c in range(3):
            rhs_ref[c * 128 : c * 128 + 128, a * 128 : a * 128 + 128] = weight_ref[a, c]
    group = 4
    for y in range(0, rows, group):
        lhs = jnp.concatenate(
            [
                grad_ref[y - a + 2 : y - a + 2 + group].reshape(group * WIDE, 128)
                for a in range(3)
            ],
            axis=1,
        )
        out = lax.dot_general(
            lhs, rhs_ref[...], (((1,), (1,)), ((), ())), preferred_element_type=jnp.float32
        )
        for j in range(group):
            part = out[j * WIDE : (j + 1) * WIDE]
            total = (
                pltpu.roll(part[:, 0:128], WIDE - 1, 0)
                + part[:, 128:256]
                + pltpu.roll(part[:, 256:384], 1, 0)
            )
            out_ref[y + j] = total[0:128].astype(jnp.bfloat16)


def call(kernel, shapes, scratch, in_specs, args, out_specs=None, aliases={}):
    return pl.pallas_call(
        kernel,
        out_shape=shapes,
        in_specs=in_specs,
        out_specs=jax.tree.map(lambda _: VMEM, shapes) if out_specs is None else out_specs,
        scratch_shapes=scratch,
        input_output_aliases=aliases,
        compiler_params=pltpu.CompilerParams(vmem_limit_bytes=40 * 1024 * 1024),
    )(*args)


def shape(dims, dtype):
    return jax.ShapeDtypeStruct(dims, dtype)


def shards(
    hidden_in, conv_weight, conv_bias, proj_weight, ocean_depth, sea_mask,
    step_alpha, step_beta, surface_cotangent,
):
    wide, narrow = jnp.float32, jnp.bfloat16
    rows = hidden_in.shape[1]
    hidden = hidden_in[0]
    n_x = lax.axis_size("lon")
    n_lat = lax.axis_size(LAT)
    n_all = lax.axis_size(("lat_0", "lat_2", "lon"))
    n_z = lax.axis_size(("lat_1", "dp"))
    lat, me = lax.axis_index(LAT), lax.axis_index("lon")
    row_group = lax.axis_index(("lat_0", "lat_2"))
    at = jnp.stack(
        [lat % 2, lat, n_lat - 1 - lat, (me + n_x - 1) % n_x, (me + 1) % n_x, row_group]
    ).astype(jnp.int32)
    mask = sea_mask.astype(wide)
    cross, planes, sums = call(
        first_kernel,
        (
            shape((304, 128), narrow),
            shape((PLANES, rows, 128), wide),
            shape((2, 128), wide),
        ),
        [],
        [SMEM] + [VMEM] * 4,
        (
            at, hidden[:2], hidden[rows - 2 :], mask * surface_cotangent[0], mask * ocean_depth
        ),
    )
    odd = [(i, (i + 1) % n_lat) for i in range(1, n_lat, 2)]
    odd = odd + [(j, i) for i, j in odd]
    cross = lax.ppermute(cross, LAT, odd)
    pair, near = call(
        edges_kernel,
        (shape((304, 128), narrow), shape((2 * n_x, NEAR, 128), narrow)),
        [],
        [SMEM] + [VMEM] * 2,
        (at, hidden, planes),
    )
    pair = lax.ppermute(pair, "lat_2", [(0, 1), (1, 0)])
    near = lax.all_to_all(near, ("lat_2", "lon"), 0, 0, tiled=True)
    sent = call(
        second_kernel, shape((n_all, 16, 128), narrow), [], [SMEM] + [VMEM] * 2, (at, sums, cross)
    )
    got = lax.all_to_all(sent, ("lat_0", "lat_2", "lon"), 0, 0, tiled=True)
    early, preact, side = call(
        forward_kernel,
        (
            shape((rows + 4, WIDE, 128), narrow),
            shape((rows, SLIM, 128), wide),
            shape((4 * PACK + 16, 128), wide),
        ),
        [pltpu.VMEM((384, 384), narrow)],
        [SMEM] + [VMEM] * 7 + [SMEM] * 2,
        (
            at, hidden, planes, pair, near, conv_weight, conv_bias[None],
            proj_weight[None], step_alpha, step_beta,
        ),
    )
    grad, sent, _ = call(
        backward_kernel,
        (
            shape((rows + 2, WIDE, 128), narrow),
            shape((n_all, 40, 128), narrow),
            shape((rows + 4, WIDE, 128), narrow),
        ),
        [
            pltpu.VMEM((rows, WIDE, 384), narrow),
            pltpu.VMEM((9, 128, 128), wide),
            pltpu.VMEM((384, 384), narrow),
            pltpu.VMEM((2, SLIM, 128), wide),
        ],
        [SMEM] + [VMEM] * 6,
        (at, cross, got, conv_weight, side, preact, early),
        None,
        {6: 2},
    )
    got = lax.all_to_all(sent, ("lat_0", "lat_2", "lon"), 0, 0, tiled=True)
    sent = call(middle_kernel, shape((n_z, 24, 128), narrow), [], [VMEM], (got,))
    got = lax.all_to_all(sent, ("lat_1", "dp"), 0, 0, tiled=True)
    grad_hidden = call(
        input_kernel,
        shape((rows, 128, 128), narrow),
        [pltpu.VMEM((384, 384), narrow)],
        [VMEM] * 2,
        (grad, conv_weight),
    )
    cells = rows * 128 * lax.axis_size("dp") * n_lat * n_x
    own_weight, total_bias, total_proj = call(
        functools.partial(last_kernel, 1.0 / math.sqrt(cells)),
        (shape((3, 3, 2, 128), wide), shape((1, 128), wide), shape((1, 128), wide)),
        [],
        [VMEM],
        (got,),
    )
    return grad_hidden[None], own_weight.transpose(2, 0, 1, 3), total_bias[0], total_proj[0]


def solution(mesh):
    split = Mesh(
        mesh.devices.reshape(mesh.shape["dp"], 4, 2, 2, mesh.shape["lon"]),
        ("dp", "lat_0", "lat_1", "lat_2", "lon"),
    )
    placed = (
        P("dp", LAT, "lon", None),
        P(),
        P(),
        P(),
        P(LAT, "lon"),
        P(LAT, "lon"),
        P(),
        P(),
        P("dp", LAT, "lon"),
    )
    return jax.shard_map(
        shards,
        mesh=split,
        in_specs=placed,
        out_specs=(P("dp", LAT, "lon", None), P(LAT_LON, None, None, None), P(), P()),
        check_vma=False,
    )
```

```python
import functools
import math

import jax
import jax.numpy as jnp
from jax import lax
from jax.experimental import pallas as pl
from jax.experimental.pallas import tpu as pltpu
from jax.sharding import Mesh
from jax.sharding import PartitionSpec as P

ITERS = 6
LAT_LON = ("lat_0", "lat_1", "lat_2", "lon")
LAT = ("lat_0", "lat_1", "lat_2")
WIDE = 144
SLIM = 136
PACK = 32
PLANES = 5
NEAR = 48

helm_coef = 0.5
VMEM = pl.BlockSpec(memory_space=pltpu.VMEM)
SMEM = pl.BlockSpec(memory_space=pltpu.SMEM)
HBM = pl.BlockSpec(memory_space=pltpu.HBM)


def rounded(values):
    return values.astype(jnp.bfloat16).astype(jnp.float32)


def pieces_of(values, count):
    out = []
    for _ in range(count):
        piece = rounded(values)
        out.append(piece)
        values = values - piece
    return out


def full(value):
    return jnp.full((1, 128), value, jnp.float32)


def packed(planes, shift):
    rows = planes[0].shape[0]
    lane = lax.broadcasted_iota(jnp.int32, (rows, 128), 1) // 8
    out = jnp.zeros((rows, 128), jnp.float32)
    for k, plane in enumerate(planes):
        by = (8 * k + shift) % 128
        out = jnp.where(lane == k, pltpu.roll(plane, by, 1) if by else plane, out)
    return out


def edge_columns(load, rows):
    place = lax.broadcasted_iota(jnp.int32, (8, 128), 0)
    columns = [[jnp.zeros((8, 128), jnp.float32) for _ in range(rows // 8)] for _ in range(4)]
    for r in range(rows):
        head = load(r, 0).astype(jnp.float32)
        tail = load(r, 112).astype(jnp.float32)
        for k, row in enumerate((head[0:1], head[1:2], tail[14:15], tail[15:16])):
            columns[k][r // 8] = jnp.where(place == r % 8, row, columns[k][r // 8])
    return columns


def unpacked(beyond, before, k):
    near = lax.broadcasted_iota(jnp.int32, beyond.shape, 1)
    if k:
        beyond = pltpu.roll(beyond, 128 - 8 * k, 1)
    before = pltpu.roll(before, 120 - 8 * k, 1)
    return jnp.where(near < 8, beyond, jnp.where(near >= 120, before, 0.0))


def near_rows(planes, top):
    rows = planes[0].shape[0]
    return [jnp.where(top, p[0:8], p[rows - 8 : rows]) for p in planes]


def first_kernel(at_ref, hidden_ref, wet_ref, depth_ref, cross_ref, planes_ref, sums_ref):
    upper = at_ref[0] == 0
    wet, wet_depth = wet_ref[...], depth_ref[...]
    planes = pieces_of(wet, 3) + pieces_of(wet_depth, 2)
    summed = full(jnp.sum(wet))
    counted = full(jnp.sum(jnp.where(wet_depth > 0.0, 1.0, 0.0)))
    sums_ref[0:1] = summed
    sums_ref[1:2] = counted
    sums = pieces_of(summed, 3) + pieces_of(counted, 3)
    sums = jnp.concatenate(sums + [jnp.zeros((2, 128), jnp.float32)], axis=0)
    for k in range(PLANES):
        planes_ref[k] = planes[k]
    cross_ref[0:256] = hidden_ref[...].reshape(256, 128)
    near = near_rows(planes, upper) + [sums]
    for k in range(0, 6, 2):
        tile = jnp.concatenate(near[k : k + 2], axis=0)
        cross_ref[256 + k * 8 : 272 + k * 8] = tile.astype(jnp.bfloat16)


def edges_kernel(at_ref, hidden_ref, planes_ref, pair_ref, near_ref):
    rows = hidden_ref.shape[0]
    upper = at_ref[0] == 0
    planes = [planes_ref[k] for k in range(PLANES)]
    start = jnp.where(upper, rows - 2, 0)
    pair_ref[0:256] = hidden_ref[pl.ds(start, 2)].reshape(256, 128)
    near = near_rows(planes + planes[:1], jnp.logical_not(upper))
    for k in range(0, 6, 2):
        tile = jnp.concatenate(near[k : k + 2], axis=0)
        pair_ref[256 + k * 8 : 272 + k * 8] = tile.astype(jnp.bfloat16)
    columns = edge_columns(lambda r, at: hidden_ref[r, at : at + 16], rows)
    head = jnp.concatenate(columns[0] + columns[1] + [packed(planes, 0)], axis=0)
    tail = jnp.concatenate(columns[2] + columns[3] + [packed(planes, 8)], axis=0)
    n_x = near_ref.shape[0] // 2
    for peer in range(n_x):
        chosen = jnp.where(at_ref[4] == peer, tail, head).astype(jnp.bfloat16)
        near_ref[peer] = chosen
        near_ref[n_x + peer] = chosen


def second_kernel(at_ref, sums_ref, cross_ref, sent_ref):
    tiles = [cross_ref[256 + k * 16 : 272 + k * 16].astype(jnp.float32) for k in range(3)]
    planes = [tiles[k // 2][k % 2 * 8 : k % 2 * 8 + 8] for k in range(PLANES)]
    got = tiles[2][8:16]
    summed = sums_ref[0:1] + got[0:1] + got[1:2] + got[2:3]
    counted = sums_ref[1:2] + got[3:4] + got[4:5] + got[5:6]
    lane = lax.broadcasted_iota(jnp.int32, (1, 128), 1)
    sums = pieces_of(jnp.where(lane < 64, summed, counted), 3)
    place = lax.broadcasted_iota(jnp.int32, (8, 128), 0)
    blocks = []
    for side in range(2):
        corner = jnp.zeros((8, 128), jnp.float32)
        for r in range(2):
            start = r * 128 + 112 * side
            tile = cross_ref[start : start + 16].astype(jnp.float32)
            for k in range(2):
                at = 14 * side + k
                corner = jnp.where(place == 2 * r + k, tile[at : at + 1], corner)
        for k in range(3):
            corner = jnp.where(place == 4 + k, sums[k], corner)
        blocks.append(jnp.concatenate([corner, packed(planes, 8 * side)], axis=0))
    n_x = 4
    for peer in range(n_x):
        chosen = jnp.where(at_ref[4] == peer, blocks[1], blocks[0]).astype(jnp.bfloat16)
        for group in range(sent_ref.shape[0] // n_x):
            sent_ref[group * n_x + peer] = chosen


def sides_of(at_ref):
    return (
        at_ref[0] == 0,
        jnp.where(at_ref[1] == 0, 0.0, 1.0),
        jnp.where(at_ref[2] == 0, 0.0, 1.0),
    )


def fill(rhs_ref, weight_ref):
    for a in range(3):
        for c in range(3):
            rhs_ref[a * 128 : a * 128 + 128, c * 128 : c * 128 + 128] = weight_ref[a, c]


def convolved(ext_ref, rhs_ref, bias, start, group):
    lhs = jnp.concatenate(
        [ext_ref[pl.ds(start + a, group)].reshape(group * WIDE, 128) for a in range(3)], axis=1
    )
    out = jnp.dot(lhs, rhs_ref[...], preferred_element_type=jnp.float32)
    rows = []
    for j in range(group):
        part = out[j * WIDE : (j + 1) * WIDE]
        rows.append(
            pltpu.roll(part[:, 0:128], 1, 0)
            + part[:, 128:256]
            + pltpu.roll(part[:, 256:384], WIDE - 1, 0)
            + bias
        )
    return rows


def slimmed(row):
    place = lax.broadcasted_iota(jnp.int32, (8, 128), 0)
    edge = jnp.where(place < 4, row[128:136], row[136:144])
    return jnp.concatenate([0.5 * row[0:128], 0.5 * edge], axis=0)


def forward_kernel(
    at_ref, hidden_ref, planes_ref, pair_ref, near_ref, weight_ref, bias_ref, proj_ref,
    alpha_ref, beta_ref,
    ext_ref, preact_ref, side_ref, rhs_ref,
):
    rows = hidden_ref.shape[0]
    n_x = near_ref.shape[0] // 2
    core, left, right = at_ref[0], at_ref[3], at_ref[4]
    upper, keep_above, keep_below = sides_of(at_ref)
    zero = jnp.zeros((), jnp.bfloat16)
    paired = jnp.where(upper, rows + 2, 0)
    keep = jnp.where(upper, keep_below, keep_above) > 0.0
    for k in range(2):
        pair = pair_ref[k * 128 : k * 128 + 128]
        ext_ref[paired + k, 0:128] = jnp.where(keep, pair, zero)
    ext_ref[2 : rows + 2, 0:128] = hidden_ref[...]
    place = lax.broadcasted_iota(jnp.int32, (WIDE - 128, 128), 0)
    tiles = [jnp.zeros((WIDE - 128, 128), jnp.float32) for _ in range(rows + 4)]
    second = []
    for side, base in ((right, 0), (left, WIDE - 130)):
        own = near_ref[core * n_x + side].astype(jnp.float32)
        other = near_ref[(1 - core) * n_x + side].astype(jnp.float32)
        for k in range(2):
            for r in range(rows + 4):
                at = r - 2
                if r < 2:
                    at = k * 16 + rows - 2 + r
                    row = other[at : at + 1] * keep_above
                elif r >= rows + 2:
                    at = k * 16 + r - rows - 2
                    row = other[at : at + 1] * keep_below
                else:
                    row = own[k * 16 + at : k * 16 + at + 1]
                tiles[r] = jnp.where(place == base + k, row, tiles[r])
        above = jnp.where(upper, 0.0, other[40:48] * keep_above)
        below = jnp.where(upper, other[32:40] * keep_below, 0.0)
        second.append(jnp.concatenate([above, own[32:48], below], axis=0))
    for r in range(rows + 4):
        ext_ref[r, 128:WIDE] = tiles[r].astype(jnp.bfloat16)
    pair = pair_ref[256:304].astype(jnp.float32)
    above = jnp.where(upper, 0.0, pair * keep_above)
    below = jnp.where(upper, pair * keep_below, 0.0)
    planes = []
    for k in range(PLANES):
        at = k * 8
        tile = unpacked(second[0], second[1], k)
        planes.append(
            jnp.concatenate(
                [above[at : at + 8], planes_ref[k], below[at : at + 8], tile], axis=0
            )
        )
    side_ref[0 : 2 * PACK] = planes[0] + planes[1] + planes[2]
    side_ref[2 * PACK : 4 * PACK] = planes[3] + planes[4]
    fill(rhs_ref, weight_ref)
    bias = bias_ref[...]
    steps = [full(ref[k]) for ref in (alpha_ref, beta_ref) for k in range(ITERS)]
    params = [bias, proj_ref[...], *steps, full(0.0), full(0.0)]
    side_ref[4 * PACK : 4 * PACK + 16] = jnp.concatenate(params, axis=0)
    group = 4
    shift = jnp.where(upper, 2, 0)
    for g in range(0, rows, group):
        for j, row in enumerate(convolved(ext_ref, rhs_ref, bias, g + shift, group)):
            preact_ref[g + j] = slimmed(row)


def backward_kernel(
    at_ref, cross_ref, got_ref, kernel_ref, side_ref, preact_ref, early_ref,
    grad_ref, sent_ref, ext_ref,
    moved_ref, weight_ref, rhs_ref, fixed_ref,
):
    rows = grad_ref.shape[0] - 2
    n_x = 4
    fields = side_ref[0 : 4 * PACK]
    fields = (fields[0 : 2 * PACK], fields[2 * PACK : 4 * PACK])
    params = side_ref[4 * PACK : 4 * PACK + 16]
    left, right = at_ref[3], at_ref[4]
    upper, keep_above, keep_below = sides_of(at_ref)
    keep_cross = jnp.where(upper, keep_above, keep_below)
    place = lax.broadcasted_iota(jnp.int32, (WIDE - 128, 128), 0)
    tiles = [jnp.zeros((WIDE - 128, 128), jnp.float32) for _ in range(2)]
    second = []
    for side, base in ((right, 0), (left, WIDE - 130)):
        corner = got_ref[at_ref[5] * n_x + side].astype(jnp.float32) * keep_cross
        for r in range(2):
            for k in range(2):
                row = corner[2 * r + k : 2 * r + k + 1]
                tiles[r] = jnp.where(place == base + k, row, tiles[r])
        second.append(corner[8:16])
    crossed = jnp.where(upper, 0, rows + 2)
    for r in range(2):
        facing = cross_ref[r * 128 : r * 128 + 128]
        facing = jnp.where(keep_cross > 0.0, facing, jnp.zeros((), jnp.bfloat16))
        ext_ref[crossed + r, 0:128] = facing
        ext_ref[crossed + r, 128:WIDE] = tiles[r].astype(jnp.bfloat16)
    fill(rhs_ref, kernel_ref)
    again = jnp.where(upper, 0, rows)
    for g, row in enumerate(convolved(ext_ref, rhs_ref, params[0:1], again, 2)):
        fixed_ref[g] = slimmed(row)
    corner = [unpacked(second[0], second[1], k) for k in range(PLANES)]
    corner = (corner[0] + corner[1] + corner[2], corner[3] + corner[4])
    facing = cross_ref[256:304].astype(jnp.float32) * keep_cross
    facing = (facing[0:8] + facing[8:16] + facing[16:24], facing[24:32] + facing[32:40])
    start, wet_depth = [
        jnp.concatenate(
            [
                fields[k][0:8] + jnp.where(upper, facing[k], 0.0),
                fields[k][8 : PACK - 8],
                fields[k][PACK - 8 : PACK] + jnp.where(upper, 0.0, facing[k]),
                fields[k][PACK : PACK + 8] + jnp.where(upper, corner[k], 0.0),
                fields[k][PACK + 8 : 2 * PACK - 8],
                fields[k][2 * PACK - 8 : 2 * PACK] + jnp.where(upper, 0.0, corner[k]),
            ],
            axis=0,
        )
        for k in range(2)
    ]
    lane = lax.broadcasted_iota(jnp.int32, (2 * PACK, 128), 1)
    mask = jnp.where(wet_depth > 0.0, 1.0, 0.0)

    def other_half(field):
        parts = [field[k * PACK : (k + 1) * PACK] for k in range(field.shape[0] // PACK)]
        swapped = []
        for k in range(0, len(parts), 2):
            swapped += [parts[k + 1], parts[k]]
        return jnp.concatenate(swapped, axis=0)

    def beside(field):
        count = field.shape[0]
        lanes = lane if count == 2 * PACK else jnp.concatenate([lane, lane], axis=0)
        up = pltpu.roll(field, 1, 0)
        down = pltpu.roll(field, count - 1, 0)
        from_left = pltpu.roll(field, 1, 1)
        from_left = jnp.where(lanes == 0, other_half(from_left), from_left)
        from_right = pltpu.roll(field, 127, 1)
        from_right = jnp.where(lanes == 127, other_half(from_right), from_right)
        return up, down, from_left, from_right

    weights = [
        0.5 * (near_mask * wet_depth + mask * near_depth)
        for near_mask, near_depth in zip(beside(mask), beside(wet_depth))
    ]
    diagonal = helm_coef * mask + weights[0] + weights[1] + weights[2] + weights[3]
    weights = [jnp.concatenate([w, w], axis=0) for w in weights]
    diagonal = jnp.concatenate([diagonal, diagonal], axis=0)
    residual = jnp.concatenate([start, mask], axis=0)
    direction = residual
    result = jnp.zeros_like(residual)
    for k in range(ITERS):
        result = result + params[2 + k : 3 + k] * direction
        if k + 1 < ITERS:
            applied = diagonal * direction
            for w, near in zip(weights, beside(direction)):
                applied = applied - w * near
            residual = residual - params[2 + k : 3 + k] * applied
            direction = residual + params[8 + k : 9 + k] * direction
    result = result * jnp.concatenate([mask, mask], axis=0)
    sums = jnp.sum(got_ref[...].astype(jnp.float32)[:, 0:8], axis=0)
    sums = sums[4:5] + sums[5:6] + sums[6:7]
    mean = jnp.broadcast_to(sums[:, 0:1], (1, 128)) / jnp.broadcast_to(sums[:, 127:128], (1, 128))
    force = result.T
    force = force - mean * pltpu.roll(force, 64, 1)
    proj = 0.5 * params[1:2]
    shift = jnp.where(upper, 2, 0)
    sublane = lax.broadcasted_iota(jnp.int32, (8, 1), 0)
    sum_bias = jnp.zeros((8, 128), jnp.float32)
    sum_proj = jnp.zeros((8, 128), jnp.float32)
    for g in range(rows + 2):
        at = g + 7
        edge = jnp.where(
            sublane < 4,
            force[0:8, PACK + at : PACK + at + 1],
            force[120:128, PACK + at : PACK + at + 1],
        )
        for q, size in ((0, 48), (48, 48), (96, 32), (128, 8)):
            column = edge if q == 128 else force[q : q + size, at : at + 1]
            column = jnp.broadcast_to(column, (size, 128))
            if g < 2:
                preact = jnp.where(upper, fixed_ref[g, q : q + size], preact_ref[g, q : q + size])
            elif g >= rows:
                preact = jnp.where(
                    upper, preact_ref[g - 2, q : q + size], fixed_ref[g - rows, q : q + size]
                )
            else:
                preact = preact_ref[g - shift, q : q + size]
            turn = jnp.tanh(preact)
            bent = preact * turn
            active = preact + bent
            slope_act = (1.0 + turn) * ((1.0 + preact) - bent)
            grad = column * proj * slope_act
            if q == 128:
                grad_ref[g, 128:WIDE] = jnp.concatenate([grad, grad], axis=0).astype(jnp.bfloat16)
                continue
            grad = grad.astype(jnp.bfloat16)
            grad_ref[g, q : q + size] = grad
            if 1 <= g <= rows:
                own = grad.astype(jnp.float32)
                drawn = active * column
                for k in range(size // 8):
                    sum_bias = sum_bias + own[k * 8 : k * 8 + 8]
                    sum_proj = sum_proj + drawn[k * 8 : k * 8 + 8]
    for g in range(1, rows + 1):
        own = grad_ref[g, 0:128].astype(jnp.float32)
        own = jnp.concatenate([own, jnp.zeros((WIDE - 128, 128), jnp.float32)], axis=0)
        moved_ref[g - 1, :, 0:128] = pltpu.roll(own, WIDE - 1, 0).astype(jnp.bfloat16)
        moved_ref[g - 1, :, 128:256] = own.astype(jnp.bfloat16)
        moved_ref[g - 1, :, 256:384] = pltpu.roll(own, 1, 0).astype(jnp.bfloat16)
    to = lax.broadcasted_iota(jnp.int32, (128, 128), 0)
    of = lax.broadcasted_iota(jnp.int32, (128, 128), 1)
    source = (
        to // 32 * 32 + to // 2 % 2 * 16 + to // 16 % 2 * 8 + to // 4 % 4 * 2 + to % 2
    )
    order = jnp.where(of == source, 1.0, 0.0).astype(jnp.bfloat16)
    moved = moved_ref[...].reshape(rows * WIDE, 384)
    cells = jnp.concatenate(
        [ext_ref[a + 1 : a + 1 + rows].reshape(rows * WIDE, 128) for a in range(3)], axis=1
    )
    whole = lax.dot_general(
        cells, moved, (((0,), (0,)), ((), ())), preferred_element_type=jnp.float32
    )
    for a in range(3):
        out = whole[a * 128 : a * 128 + 128]
        out = jnp.dot(
            order, out.astype(jnp.bfloat16), preferred_element_type=jnp.float32
        )
        for c in range(3):
            weight_ref[a * 3 + c] = out[:, c * 128 : c * 128 + 128]
    vectors = jnp.concatenate(
        [jnp.sum(sum_bias, axis=0, keepdims=True), jnp.sum(sum_proj, axis=0, keepdims=True)], axis=0
    )
    vectors = jnp.concatenate(pieces_of(vectors, 2) + [jnp.zeros((4, 128), jnp.float32)], axis=0)
    vectors = pltpu.roll(vectors, 4, 0)
    low = lax.broadcasted_iota(jnp.int32, (8, 128), 0) < 4

    for t in range(16):
        start = t * 8
        blocks = ([], [])
        for k in range(0, 9, 2):
            one = weight_ref[k, start : start + 8]
            two = weight_ref[k + 1, start : start + 8] if k < 8 else vectors
            two_low = pltpu.roll(two, 4, 0) if k < 8 else vectors
            blocks[0].append(jnp.where(low, one, two_low))
            blocks[1].append(jnp.where(low, pltpu.roll(one, 4, 0), two))
        for x in range(2):
            sent_ref[t * 2 + x] = jnp.concatenate(blocks[x], axis=0).astype(jnp.bfloat16)


def middle_kernel(got_ref, sent_ref):
    total = jnp.sum(got_ref[...].astype(jnp.float32), axis=0)
    vectors = total[36:38] + total[38:40]
    vectors = jnp.concatenate(pieces_of(vectors, 2) + [jnp.zeros((2, 128), jnp.float32)], axis=0)
    peers = sent_ref.shape[0] // 2
    for z in range(2):
        block = [total[4 * k + 2 * z : 4 * k + 2 * z + 2] for k in range(9)]
        block = jnp.concatenate(block + [vectors], axis=0)
        block = block.astype(jnp.bfloat16)
        for d in range(peers):
            sent_ref[z * peers + d] = block


def last_kernel(scale, got_ref, weight_ref, bias_ref, proj_ref):
    total = jnp.sum(got_ref[...].astype(jnp.float32), axis=0) * scale
    for k in range(9):
        weight_ref[k // 3, k % 3] = total[k * 2 : k * 2 + 2]
    bias_ref[...] = total[18:19] + total[20:21]
    proj_ref[...] = total[19:20] + total[21:22]


def input_kernel(grad_ref, weight_ref, out_ref, rhs_ref):
    rows = out_ref.shape[0]
    for a in range(3):
        for c in range(3):
            rhs_ref[c * 128 : c * 128 + 128, a * 128 : a * 128 + 128] = weight_ref[a, c]
    group = 4
    for y in range(0, rows, group):
        lhs = jnp.concatenate(
            [
                grad_ref[y - a + 2 : y - a + 2 + group].reshape(group * WIDE, 128)
                for a in range(3)
            ],
            axis=1,
        )
        out = lax.dot_general(
            lhs, rhs_ref[...], (((1,), (1,)), ((), ())), preferred_element_type=jnp.float32
        )
        for j in range(group):
            part = out[j * WIDE : (j + 1) * WIDE]
            total = (
                pltpu.roll(part[:, 0:128], WIDE - 1, 0)
                + part[:, 128:256]
                + pltpu.roll(part[:, 256:384], 1, 0)
            )
            out_ref[y + j] = total[0:128].astype(jnp.bfloat16)


def call(kernel, shapes, scratch, in_specs, args, out_specs=None, aliases={}):
    return pl.pallas_call(
        kernel,
        out_shape=shapes,
        in_specs=in_specs,
        out_specs=jax.tree.map(lambda _: VMEM, shapes) if out_specs is None else out_specs,
        scratch_shapes=scratch,
        input_output_aliases=aliases,
        compiler_params=pltpu.CompilerParams(vmem_limit_bytes=40 * 1024 * 1024),
    )(*args)


def shape(dims, dtype):
    return jax.ShapeDtypeStruct(dims, dtype)


def shards(
    hidden_in, conv_weight, conv_bias, proj_weight, ocean_depth, sea_mask,
    step_alpha, step_beta, surface_cotangent,
):
    wide, narrow = jnp.float32, jnp.bfloat16
    rows = hidden_in.shape[1]
    hidden = hidden_in[0]
    n_x = lax.axis_size("lon")
    n_lat = lax.axis_size(LAT)
    n_all = lax.axis_size(("lat_0", "lat_2", "lon"))
    n_z = lax.axis_size(("lat_1", "dp"))
    lat, me = lax.axis_index(LAT), lax.axis_index("lon")
    row_group = lax.axis_index(("lat_0", "lat_2"))
    at = jnp.stack(
        [lat % 2, lat, n_lat - 1 - lat, (me + n_x - 1) % n_x, (me + 1) % n_x, row_group]
    ).astype(jnp.int32)
    mask = sea_mask.astype(wide)
    facing = lax.dynamic_slice_in_dim(
        hidden, jnp.where(lax.axis_index("lat_2") == 0, 0, rows - 2), 2, axis=0
    )
    cross, planes, sums = call(
        first_kernel,
        (
            shape((304, 128), narrow),
            shape((PLANES, rows, 128), wide),
            shape((2, 128), wide),
        ),
        [],
        [SMEM] + [VMEM] * 3,
        (at, facing, mask * surface_cotangent[0], mask * ocean_depth),
    )
    odd = [(i, (i + 1) % n_lat) for i in range(1, n_lat, 2)]
    odd = odd + [(j, i) for i, j in odd]
    cross = lax.ppermute(cross, LAT, odd)
    pair, near = call(
        edges_kernel,
        (shape((304, 128), narrow), shape((2 * n_x, NEAR, 128), narrow)),
        [],
        [SMEM] + [VMEM] * 2,
        (at, hidden, planes),
    )
    pair = lax.ppermute(pair, "lat_2", [(0, 1), (1, 0)])
    near = lax.all_to_all(near, ("lat_2", "lon"), 0, 0, tiled=True)
    sent = call(
        second_kernel, shape((n_all, 16, 128), narrow), [], [SMEM] + [VMEM] * 2, (at, sums, cross)
    )
    got = lax.all_to_all(sent, ("lat_0", "lat_2", "lon"), 0, 0, tiled=True)
    early, preact, side = call(
        forward_kernel,
        (
            shape((rows + 4, WIDE, 128), narrow),
            shape((rows, SLIM, 128), wide),
            shape((4 * PACK + 16, 128), wide),
        ),
        [pltpu.VMEM((384, 384), narrow)],
        [SMEM] + [VMEM] * 7 + [SMEM] * 2,
        (
            at, hidden, planes, pair, near, conv_weight, conv_bias[None],
            proj_weight[None], step_alpha, step_beta,
        ),
    )
    grad, sent, _ = call(
        backward_kernel,
        (
            shape((rows + 2, WIDE, 128), narrow),
            shape((n_all, 40, 128), narrow),
            shape((rows + 4, WIDE, 128), narrow),
        ),
        [
            pltpu.VMEM((rows, WIDE, 384), narrow),
            pltpu.VMEM((9, 128, 128), wide),
            pltpu.VMEM((384, 384), narrow),
            pltpu.VMEM((2, SLIM, 128), wide),
        ],
        [SMEM] + [VMEM] * 6,
        (at, cross, got, conv_weight, side, preact, early),
        None,
        {6: 2},
    )
    got = lax.all_to_all(sent, ("lat_0", "lat_2", "lon"), 0, 0, tiled=True)
    sent = call(middle_kernel, shape((n_z, 24, 128), narrow), [], [VMEM], (got,))
    got = lax.all_to_all(sent, ("lat_1", "dp"), 0, 0, tiled=True)
    grad_hidden = call(
        input_kernel,
        shape((rows, 128, 128), narrow),
        [pltpu.VMEM((384, 384), narrow)],
        [VMEM] * 2,
        (grad, conv_weight),
    )
    cells = rows * 128 * lax.axis_size("dp") * n_lat * n_x
    own_weight, total_bias, total_proj = call(
        functools.partial(last_kernel, 1.0 / math.sqrt(cells)),
        (shape((3, 3, 2, 128), wide), shape((1, 128), wide), shape((1, 128), wide)),
        [],
        [VMEM],
        (got,),
    )
    return grad_hidden[None], own_weight.transpose(2, 0, 1, 3), total_bias[0], total_proj[0]


def solution(mesh):
    split = Mesh(
        mesh.devices.reshape(mesh.shape["dp"], 4, 2, 2, mesh.shape["lon"]),
        ("dp", "lat_0", "lat_1", "lat_2", "lon"),
    )
    placed = (
        P("dp", LAT, "lon", None),
        P(),
        P(),
        P(),
        P(LAT, "lon"),
        P(LAT, "lon"),
        P(),
        P(),
        P("dp", LAT, "lon"),
    )
    return jax.shard_map(
        shards,
        mesh=split,
        in_specs=placed,
        out_specs=(P("dp", LAT, "lon", None), P(LAT_LON, None, None, None), P(), P()),
        check_vma=False,
    )
```
